256 devices in a mesh: patch: 64 (over y, z, core), sub: 4 (over x).
Axes of the slice: x: 4, y: 4, z: 8, core: 2. Of those that a mesh axis runs over, the one named last changes fastest.
Arguments:
- state: float32 [64, 4, 1, 27, 729], P('patch', 'sub'), may hold values from -6 to 6
- stiff_weight: float32 [64, 96, 9216], P('patch'), may hold values from 0.3 to 3
- volume_weight: float32 [64, 96, 9216], P('patch'), may hold values from 0.5 to 2
- lagrange: float32 [256, 4, 1, 729], P('patch', 'sub'), may hold values from -6 to 6
- mortar: float32 [256, 2, 2, 27, 27], P('patch'), may hold values from -1.25 to 1.25
- links: int32 [256, 6], replicated, may hold values from 0 to 63, as said below
Outputs:
- residual: float32 [64, 4, 1, 27, 729], P('patch', 'sub')
- constraint: float32 [256, 4, 1, 729], P('patch', 'sub')
The draws below stay inside these ranges and needn't reach their ends.
Inputs may be any that keep to these rules, and one draw needn't show every extreme that they name: `links`: row o * 4 + s is slot s of owner o along patch. Live slots of an owner come first and have both counts in 12 to 27; empty slots are all zero. 2 * 64 slots are live. A live interface joins face 2d + 1 of its first patch to face 2d of its second patch, d being 0 or 1; faces 0 to 3 of every patch lie on exactly one live interface each; the live interfaces of one owner all have the same d. At most 2 faces of one patch lie on live interfaces of one owner; in every draw some owner has 4 live slots and 2 faces of one patch.
All inputs are finite; a program needn't handle non-finite values.
Results may differ from the reference program's by a relative error of at most 0.0001.
Values sent between devices are 32-bit elements; how exact they have to be, the bound alone decides.
A program may use at most 128 MiB of HBM per device.

```python
import math
import jax
import jax.numpy as jnp
import numpy as np
from jax import lax

ELEMS = 24
DEGREE = 3
FIELDS = 4
VECS = 1
SLOTS = 4
BASIS = 27
QUAD = 96
QLO = 12
PATCHES = 64


def draw_links(key, part):
    count = PATCHES
    streams = jax.random.split(jax.random.fold_in(key, 17), 5)
    cycles = jnp.stack([jax.random.permutation(streams[0], count), jax.random.permutation(streams[1], count)])
    owner_order = jax.random.permutation(streams[2], count)
    shifts = jax.random.randint(streams[3], (count // 2,), -2, 3).at[0].set(2)
    pair_loads = jnp.stack([2 + shifts, 2 - shifts], axis=1).reshape(count)
    order_starts = jnp.cumsum(pair_loads) - pair_loads
    position = jnp.argsort(owner_order)
    loads = pair_loads[position]
    starts = order_starts[position]
    slot_ids = jnp.arange(SLOTS)
    edges = starts[:, None] + slot_ids[None, :]
    alive = (slot_ids[None, :] < loads[:, None]).astype(jnp.int32)
    direction = jnp.minimum(edges // count, 1)
    along = edges % count
    first_patch = cycles[direction, along]
    second_patch = cycles[direction, (along + 1) % count]
    extents = jax.random.randint(streams[4], (count, SLOTS, 2), QLO, BASIS + 1)
    table = jnp.stack([first_patch, second_patch, 2 * direction + 1, 2 * direction, extents[:, :, 0], extents[:, :, 1]], axis=-1)
    return (table * alive[:, :, None]).reshape(count * SLOTS, 6).astype(jnp.int32)


def block_levels(key, extent, shards, smallest, largest):
    level = 1.0
    for dim, parts in shards:
        steps = jax.random.uniform(jax.random.fold_in(jax.random.fold_in(key, 6), dim), (parts,), jnp.float32, smallest / len(shards), largest / len(shards))
        level = level * jnp.repeat(jnp.exp(steps), extent[dim] // parts).reshape((-1,) + (1,) * (len(extent) - 1 - dim))
    return level


def bell_draw(stream_key, extent, width, most, cuts=(), dtype=jnp.bfloat16):
    values = jax.random.normal(stream_key, extent, jnp.float32) * width
    if len(cuts) > 0:
        values = block_levels(stream_key, extent, cuts, -0.22, 0.18) * values
    return jnp.clip(values, min=-most, max=most).astype(dtype)


def setup_inputs(seed: int = 0) -> dict:
    splits = jax.random.split(jax.random.key(seed), 7)
    return {
        "state": bell_draw(splits[0], (PATCHES, FIELDS, VECS, BASIS, BASIS * BASIS), 1.0, 6.0, ((0, 64), (1, 4)), jnp.float32),
        "stiff_weight": jnp.clip(jnp.exp(math.log(3.0) - 2.3025851 * jax.random.uniform(splits[1], (PATCHES, QUAD, QUAD * QUAD), jnp.float32) ** block_levels(splits[1], (PATCHES, QUAD, QUAD * QUAD), ((0, 64),), -0.2, 0.2)), 0.3, 3.0),
        "volume_weight": jnp.clip(jnp.exp(math.log(2.0) - 1.3862944 * jax.random.uniform(splits[2], (PATCHES, QUAD, QUAD * QUAD), jnp.float32) ** block_levels(splits[2], (PATCHES, QUAD, QUAD * QUAD), ((0, 64),), -0.2, 0.2)), 0.5, 2.0),
        "lagrange": bell_draw(splits[3], (PATCHES * SLOTS, FIELDS, VECS, BASIS * BASIS), 1.0, 6.0, ((0, 64), (1, 4)), jnp.float32),
        "mortar": bell_draw(splits[4], (PATCHES * SLOTS, 2, 2, BASIS, BASIS), BASIS ** -0.5, 1.25, ((0, 64),), jnp.float32),
        "links": draw_links(jax.random.fold_in(splits[6], 71), 0),
    }


stabilize = 0.25
highest = lax.Precision.HIGHEST
gauss_points_four = [-0.8611363115940526, -0.3399810435848563, 0.3399810435848563, 0.8611363115940526]
gauss_weights_four = [0.3478548451374538, 0.6521451548625461, 0.6521451548625461, 0.3478548451374538]


def spline_tables(elements, degree):
    knot_list = np.concatenate([np.zeros(degree), np.arange(elements + 1.0), np.full(degree, float(elements))])
    gauss_nodes = np.array(gauss_points_four)
    gauss_weights = np.array(gauss_weights_four)
    points = (np.arange(elements)[:, None] + (gauss_nodes[None, :] + 1.0) / 2.0).reshape(-1)
    point_weights = np.tile(gauss_weights / 2.0, elements)
    current = np.where((knot_list[None, :-1] <= points[:, None]) & (points[:, None] < knot_list[None, 1:]), 1.0, 0.0)
    previous = current
    for order_k in range(1, degree + 1):
        previous = current
        amount = len(knot_list) - 1 - order_k
        current = np.zeros((points.shape[0], amount))
        for column in range(amount):
            left_span = knot_list[column + order_k] - knot_list[column]
            right_span = knot_list[column + order_k + 1] - knot_list[column + 1]
            if left_span > 0:
                current[:, column] += (points - knot_list[column]) / left_span * previous[:, column]
            if right_span > 0:
                current[:, column] += (knot_list[column + order_k + 1] - points) / right_span * previous[:, column + 1]
    slope_part = np.zeros(current.shape)
    for column in range(current.shape[1]):
        left_span = knot_list[column + degree] - knot_list[column]
        right_span = knot_list[column + degree + 1] - knot_list[column + 1]
        if left_span > 0:
            slope_part[:, column] += degree / left_span * previous[:, column]
        if right_span > 0:
            slope_part[:, column] -= degree / right_span * previous[:, column + 1]
    return (jnp.asarray(current, jnp.float32), jnp.asarray(slope_part, jnp.float32),
            jnp.asarray(current * point_weights[:, None], jnp.float32),
            jnp.asarray(slope_part * point_weights[:, None], jnp.float32))


def forward(coefficients, outer_matrix, middle_matrix, inner_matrix):
    size_n = outer_matrix.shape[1]
    partial_value = coefficients.reshape(size_n, size_n, size_n)
    partial_value = jnp.einsum('ck,ijk->ijc', inner_matrix, partial_value, precision=highest)
    partial_value = jnp.einsum('bj,ijc->ibc', middle_matrix, partial_value, precision=highest)
    return jnp.dot(outer_matrix, partial_value.reshape(size_n, -1), precision=highest, preferred_element_type=jnp.float32)


def backward(values, outer_matrix, middle_matrix, inner_matrix):
    size_n = outer_matrix.shape[1]
    points = outer_matrix.shape[0]
    partial_value = jnp.dot(outer_matrix.T, values, precision=highest, preferred_element_type=jnp.float32)
    partial_value = partial_value.reshape(size_n, points, points)
    partial_value = jnp.einsum('bj,ibc->ijc', middle_matrix, partial_value, precision=highest)
    partial_value = jnp.einsum('ck,ijc->ijk', inner_matrix, partial_value, precision=highest)
    return partial_value.reshape(size_n, size_n * size_n)


def reference(state, stiff_weight, volume_weight, lagrange, mortar, links):
    value_table, slope_table, value_weighted, slope_weighted = spline_tables(ELEMS, DEGREE)
    size_n = BASIS
    slopes = [(slope_table, value_table, value_table), (value_table, slope_table, value_table),
              (value_table, value_table, slope_table)]
    weighted = [(slope_weighted, value_weighted, value_weighted), (value_weighted, slope_weighted, value_weighted),
                (value_weighted, value_weighted, slope_weighted)]

    def one_patch(packed):
        fields, stiffness, volume = packed

        def one_vector(group):
            pvalue = forward(group[3], value_table, value_table, value_table)
            outputs = []
            for comp in range(3):
                total = jnp.zeros((size_n, size_n * size_n), jnp.float32)
                for axis_d in range(3):
                    flux = stiffness * forward(group[comp], slopes[axis_d][0], slopes[axis_d][1], slopes[axis_d][2])
                    if axis_d == comp:
                        flux = flux - volume * pvalue
                    total = total + backward(flux, weighted[axis_d][0], weighted[axis_d][1], weighted[axis_d][2])
                outputs.append(total)
            pressure_total = jnp.zeros((size_n, size_n * size_n), jnp.float32)
            for axis_d in range(3):
                flux = -stabilize * stiffness * forward(group[3], slopes[axis_d][0], slopes[axis_d][1], slopes[axis_d][2])
                pressure_total = pressure_total + backward(flux, weighted[axis_d][0], weighted[axis_d][1], weighted[axis_d][2])
            for comp in range(3):
                flux = volume * forward(group[comp], slopes[comp][0], slopes[comp][1], slopes[comp][2])
                pressure_total = pressure_total - backward(flux, value_weighted, value_weighted, value_weighted)
            outputs.append(pressure_total)
            return jnp.stack(outputs)

        return jnp.moveaxis(lax.map(one_vector, jnp.moveaxis(fields, 1, 0)), 0, 1)

    volume_part = lax.map(one_patch, (state, stiff_weight, volume_weight))
    patches = state.shape[0]
    vectors = state.shape[2]
    cube = state.reshape(patches, FIELDS, vectors, size_n, size_n, size_n)
    faces = jnp.stack([cube[:, :, :, 0], cube[:, :, :, -1], cube[:, :, :, :, 0], cube[:, :, :, :, -1]], axis=1)
    item_patch = links[:, 0:2]
    item_face = links[:, 2:4]
    item_traces = faces[item_patch, item_face]
    rank_grid = jnp.arange(size_n).astype(jnp.int32)
    row_mask = (rank_grid[None, :] < links[:, 4:5]).astype(jnp.float32)
    col_mask = (rank_grid[None, :] < links[:, 5:6]).astype(jnp.float32)
    left = mortar[:, :, 0] * row_mask[:, None, :, None]
    right = mortar[:, :, 1] * col_mask[:, None, :, None]
    projected = jnp.einsum('rsai,rsfvij,rsbj->rsfvab', left, item_traces, right, precision=highest)
    link_rows = links.shape[0]
    constraint = (projected[:, 0] - projected[:, 1]).reshape(link_rows, FIELDS, vectors, size_n * size_n)
    multipliers = lagrange.reshape(link_rows, FIELDS, vectors, size_n, size_n)
    signs = jnp.array([1.0, -1.0], jnp.float32)
    correction = jnp.einsum('rsai,rfvab,rsbj->rsfvij', left, multipliers, right, precision=highest)
    correction = correction * signs[None, :, None, None, None, None]
    segment_ids = (item_patch * 4 + item_face).reshape(-1).astype(jnp.int32)
    face_total = jax.ops.segment_sum(correction.reshape(link_rows * 2, FIELDS, vectors, size_n, size_n),
                                     segment_ids, num_segments=patches * 4)
    face_total = face_total.reshape(patches, 4, FIELDS, vectors, size_n, size_n)
    result = volume_part.reshape(patches, FIELDS, vectors, size_n, size_n, size_n)
    result = result.at[:, :, :, 0].add(face_total[:, 0])
    result = result.at[:, :, :, -1].add(face_total[:, 1])
    result = result.at[:, :, :, :, 0].add(face_total[:, 2])
    result = result.at[:, :, :, :, -1].add(face_total[:, 3])
    return result.reshape(patches, FIELDS, vectors, size_n, size_n * size_n), constraint
```

```python
import jax
import jax.numpy as jnp
import numpy as np
from jax import lax
from jax.experimental import pallas as pl
from jax.experimental.pallas import tpu as pltpu
from jax.sharding import PartitionSpec as P

ELEMS = 24
DEGREE = 3
FIELDS = 4
BASIS = 27
QUAD = 96
SUBS = 4
SLAB = QUAD // SUBS
LAYERS = SLAB // 4 + DEGREE
STEPS = 12
MESH = pl.DeviceIdType.MESH

stabilize = 0.25
highest = lax.Precision.HIGHEST
gauss_points_four = [
    -0.8611363115940526,
    -0.3399810435848563,
    0.3399810435848563,
    0.8611363115940526,
]
gauss_weights_four = [
    0.3478548451374538,
    0.6521451548625461,
    0.6521451548625461,
    0.3478548451374538,
]


def in_order(tiles, dim):
    dims = list(tiles.shape[1:])
    dims[dim] *= tiles.shape[0]
    return jnp.moveaxis(tiles, 0, dim).reshape(dims)


def from_everyone(value, axis):
    peers = lax.axis_size(axis)
    return lax.all_to_all(
        jnp.broadcast_to(value[None], (peers, *value.shape)), axis, 0, 0, tiled=True
    )


def gathered_copies(value, axis, dim):
    return in_order(from_everyone(value, axis), dim)


def spline_tables(elements, degree):
    knot_list = np.concatenate(
        [np.zeros(degree), np.arange(elements + 1.0), np.full(degree, float(elements))]
    )
    gauss_nodes = np.array(gauss_points_four)
    gauss_weights = np.array(gauss_weights_four)
    points = (np.arange(elements)[:, None] + (gauss_nodes[None, :] + 1.0) / 2.0).reshape(-1)
    point_weights = np.tile(gauss_weights / 2.0, elements)
    current = np.where(
        (knot_list[None, :-1] <= points[:, None]) & (points[:, None] < knot_list[None, 1:]),
        1.0,
        0.0,
    )
    previous = current
    for order_k in range(1, degree + 1):
        previous = current
        amount = len(knot_list) - 1 - order_k
        current = np.zeros((points.shape[0], amount))
        for column in range(amount):
            left_span = knot_list[column + order_k] - knot_list[column]
            right_span = knot_list[column + order_k + 1] - knot_list[column + 1]
            if left_span > 0:
                current[:, column] += (points - knot_list[column]) / left_span * previous[:, column]
            if right_span > 0:
                current[:, column] += (
                    (knot_list[column + order_k + 1] - points)
                    / right_span
                    * previous[:, column + 1]
                )
    slope_part = np.zeros(current.shape)
    for column in range(current.shape[1]):
        left_span = knot_list[column + degree] - knot_list[column]
        right_span = knot_list[column + degree + 1] - knot_list[column + 1]
        if left_span > 0:
            slope_part[:, column] += degree / left_span * previous[:, column]
        if right_span > 0:
            slope_part[:, column] -= degree / right_span * previous[:, column + 1]
    return (
        current.astype(np.float32),
        slope_part.astype(np.float32),
        (current * point_weights[:, None]).astype(np.float32),
        (slope_part * point_weights[:, None]).astype(np.float32),
    )


def halves(table):
    high = table.astype(jnp.bfloat16).astype(np.float32)
    low = (table - high).astype(jnp.bfloat16).astype(np.float32)
    return high, low


def constant_tables():
    value, slope, value_w, slope_w = spline_tables(ELEMS, DEGREE)
    first = np.zeros((SUBS, 2 * SLAB, 16), np.float32)
    last = np.zeros((SUBS, 16, 2 * SLAB), np.float32)
    for q in range(SUBS):
        rows = slice(SLAB * q, SLAB * (q + 1))
        cols = slice(6 * q, 6 * q + LAYERS)
        first[q, :SLAB, :LAYERS] = value[rows, cols]
        first[q, SLAB:, :LAYERS] = slope[rows, cols]
        last[q, :LAYERS, :SLAB] = slope_w[rows, cols].T
        last[q, :LAYERS, SLAB:] = value_w[rows, cols].T
    high, low = halves(first)
    first = np.concatenate([high, high, low], axis=2)
    high, low = halves(last)
    last = np.concatenate([high, high, low], axis=2)

    def pair_tables(table):
        high, low = halves(table)
        even = np.zeros((256, 256), np.float32)
        odd = np.zeros((256, 256), np.float32)
        for s in range(2):
            cols = slice(128 * s, 128 * s + QUAD)
            even[32 * s:32 * s + BASIS, cols] = high.T
            even[128 + 32 * s:128 + 32 * s + BASIS, cols] = high.T
            even[192 + 32 * s:192 + 32 * s + BASIS, cols] = low.T
            odd[64 + 32 * s:64 + 32 * s + BASIS, cols] = high.T
            odd[128 + 32 * s:128 + 32 * s + BASIS, cols] = low.T
            odd[192 + 32 * s:192 + 32 * s + BASIS, cols] = high.T
        return even, odd

    value_even, value_odd = pair_tables(value)
    slope_even, slope_odd = pair_tables(slope)
    inner = np.stack([value_even, value_odd, slope_even, slope_odd])
    plain = value_odd[:, 128:]

    def adjoint_table(table):
        high, low = halves(table)
        out = np.zeros((512, 256), np.float32)
        for f in range(FIELDS):
            scale = -stabilize if f == FIELDS - 1 else 1.0
            rows = slice(128 * f, 128 * f + QUAD)
            out[rows, 32 * f:32 * f + BASIS] = scale * high
            out[rows, 128 + 32 * f:128 + 32 * f + BASIS] = scale * low
        return out

    high, low = halves(value_w)
    div = np.zeros((128, 256), np.float32)
    div[:QUAD, 96:96 + BASIS] = -high
    div[:QUAD, 224:224 + BASIS] = -low
    adjoint_value = adjoint_table(value_w)
    adjoint_slope = np.concatenate([adjoint_table(slope_w), div])
    middle = np.zeros((STEPS, 128), np.float32)
    for t in range(STEPS):
        for bb in range(8):
            point = 8 * t + bb
            for m in range(4):
                col = 2 * t + bb // 4 + m
                for n, table in enumerate((value, slope, value_w, slope_w)):
                    middle[t, 32 * n + 4 * bb + m] = table[point, col]
    half = lambda x: jnp.asarray(x, jnp.bfloat16)
    return (half(first), half(last), half(inner), half(plain), half(adjoint_value), half(adjoint_slope),
            jnp.asarray(middle, jnp.float32))


def split(x):
    high = x.astype(jnp.bfloat16)
    return high, (x - high.astype(jnp.float32)).astype(jnp.bfloat16)


def product(left, right):
    return jnp.dot(left, right, preferred_element_type=jnp.float32)


def lanes_of(rows):
    return lax.broadcasted_iota(jnp.int32, (rows, 128), 1)


def volume_kernel(x_ref, stiff_hbm, volume_hbm, first_ref, last_ref, inner_ref, plain_ref, adj_value_ref,
                  adj_slope_ref, middle_ref, out_ref, stiff, volume, sent, got, back, home, outer, total,
                  load_sem, send_sem, recv_sem, back_send_sem, back_recv_sem):
    me = lax.axis_index("sub")
    rows = pl.ds(pl.multiple_of(me * SLAB, 8), SLAB)
    load_stiff = pltpu.make_async_copy(stiff_hbm.at[rows], stiff, load_sem.at[0])
    load_volume = pltpu.make_async_copy(volume_hbm.at[rows], volume, load_sem.at[1])
    load_stiff.start()
    load_volume.start()
    peers = [lax.rem(me + d, SUBS) for d in range(SUBS)]
    origins = [lax.rem(me + SUBS - d, SUBS) for d in range(SUBS)]
    barrier = pltpu.get_barrier_semaphore()
    for d in range(1, SUBS):
        pl.semaphore_signal(barrier, inc=1, device_id={"sub": peers[d]}, device_id_type=MESH)
    sent[...] = jnp.zeros_like(sent)
    for q in range(SUBS):
        sent[q, 0:LAYERS, 0:729] = x_ref[6 * q:6 * q + LAYERS, :]
    pl.semaphore_wait(barrier, SUBS - 1)
    going = [None]
    for d in range(1, SUBS):
        copy = pltpu.make_async_remote_copy(
            src_ref=sent.at[peers[d]], dst_ref=got.at[me], send_sem=send_sem.at[d], recv_sem=recv_sem.at[d],
            device_id={"sub": peers[d]}, device_id_type=MESH)
        copy.start()
        going.append(copy)
    got[me] = sent[me]
    total[...] = jnp.zeros_like(total)
    for d in range(1, SUBS):
        going[d].wait_send()
        pltpu.make_async_remote_copy(
            src_ref=sent.at[peers[d]], dst_ref=got.at[origins[d]], send_sem=send_sem.at[d],
            recv_sem=recv_sem.at[d], device_id={"sub": peers[d]}, device_id_type=MESH).wait_recv()

    first = first_ref[me]
    spread = []
    for f in range(FIELDS):
        high, low = split(got[f])
        spread.append(product(first, jnp.concatenate([high, low, high], axis=0)))
    lane = lanes_of(2 * SLAB)
    for j in range(BASIS):
        tile, shift = divmod(BASIS * j, 128)
        merged = None
        for f in range(FIELDS):
            piece = spread[f][:, 128 * tile:128 * tile + 128]
            if shift + BASIS > 128:
                piece = jnp.where(lane >= shift, piece, spread[f][:, 128 * tile + 128:128 * tile + 256])
            turn = (32 * f - shift) % 128
            piece = pltpu.roll(piece, turn, 1) if turn else piece
            merged = piece if f == 0 else jnp.where(lane >= 32 * f, piece, merged)
        outer[j] = merged
    load_stiff.wait()
    load_volume.wait()

    def step(t, carry):
        def scalar(table, bb, m):
            return middle_ref[t, 32 * table + 4 * bb + m]

        window = [outer[2 * t + m] for m in range(5)]
        values = [w[0:SLAB] for w in window]
        slopes = [w[SLAB:2 * SLAB] for w in window]

        def middle_sum(table, parts, bb):
            e = bb // 4
            out = scalar(table, bb, 0) * parts[e]
            for m in range(1, 4):
                out = out + scalar(table, bb, m) * parts[e + m]
            return out

        across = [middle_sum(0, slopes, bb) for bb in range(8)] + [middle_sum(1, values, bb) for bb in range(8)]
        along = [middle_sum(0, values, bb) for bb in range(8)]

        def pair_sides(x):
            lane = lanes_of(x.shape[0])
            high = x.astype(jnp.bfloat16)
            wide = high.astype(jnp.float32)
            low = x - wide
            turned = pltpu.roll(wide, 64, 1)
            even = jnp.where(lane < 64, low, turned).astype(jnp.bfloat16)
            odd = jnp.where(lane < 64, turned, low).astype(jnp.bfloat16)
            return jnp.concatenate([high, even], axis=1), jnp.concatenate([high, odd], axis=1)

        even, odd = pair_sides(jnp.concatenate(across, axis=0))
        across_even = product(even, inner_ref[0])
        across_odd = product(odd, inner_ref[1])
        even, odd = pair_sides(jnp.concatenate(along, axis=0))
        along_even = product(even, inner_ref[2])
        along_odd = product(odd, inner_ref[3])
        pvalue = product(odd, plain_ref[...])

        def weights(ref):
            lane = lanes_of(SLAB)
            tiles = [ref[:, pl.ds(pl.multiple_of(768 * t + 128 * n, 128), 128)] for n in range(6)]
            parts = []
            for bb in range(8):
                tile, shift = divmod(QUAD * bb, 128)
                part = tiles[tile]
                if shift + QUAD > 128:
                    part = jnp.where(lane >= shift, part, tiles[tile + 1])
                parts.append(pltpu.roll(part, 128 - shift, 1) if shift else part)
            return jnp.concatenate(parts, axis=0)

        s = weights(stiff)
        w = weights(volume)
        half = 8 * SLAB
        pressed = w * pvalue
        grads = [
            [across_even[0:half, 0:128], across_even[0:half, 128:256], across_odd[0:half, 0:128],
             across_odd[0:half, 128:256]],
            [across_even[half:, 0:128], across_even[half:, 128:256], across_odd[half:, 0:128],
             across_odd[half:, 128:256]],
            [along_even[:, 0:128], along_even[:, 128:256], along_odd[:, 0:128], along_odd[:, 128:256]],
        ]
        fluxes = []
        for d in range(3):
            fluxes.append([s * grads[d][f] - pressed if f == d else s * grads[d][f] for f in range(FIELDS)])
        spill = w * (grads[0][0] + grads[1][1] + grads[2][2])

        def adjoint(parts, table):
            pairs = [split(p) for p in parts]
            wide = product(jnp.concatenate([p[0] for p in pairs], axis=1), table[...])
            low = product(jnp.concatenate([p[1] for p in pairs], axis=1), table[:, 0:128])
            return wide[:, 0:128] + wide[:, 128:256] + low

        heads = [adjoint(fluxes[0], adj_value_ref), adjoint(fluxes[1], adj_value_ref),
                 adjoint(fluxes[2] + [spill], adj_slope_ref)]
        heads = [[h[SLAB * bb:SLAB * bb + SLAB] for bb in range(8)] for h in heads]
        sums = [[None, None] for _ in range(5)]
        for bb in range(8):
            for m in range(4):
                at = bb // 4 + m
                v = scalar(2, bb, m)
                terms = [v * heads[0][bb], scalar(3, bb, m) * heads[1][bb] + v * heads[2][bb]]
                sums[at] = [a if b is None else b + a for a, b in zip(terms, sums[at])]
        for m in range(5):
            total[2 * t + m] += jnp.concatenate(sums[m], axis=0)
        return carry

    lax.fori_loop(0, STEPS, step, 0)

    last = last_ref[me]
    lane = lanes_of(16)
    packed = [[jnp.zeros((16, 128), jnp.float32) for _ in range(6)] for _ in range(FIELDS)]
    for j0 in range(0, BASIS, 2):
        some = list(range(j0, min(j0 + 2, BASIS)))
        columns = []
        for j in some:
            high, low = split(total[j])
            columns.append(jnp.concatenate([high, low, high], axis=0))
        result = product(last, jnp.concatenate(columns, axis=1))
        for n, j in enumerate(some):
            piece = result[:, 128 * n:128 * n + 128]
            tile, shift = divmod(BASIS * j, 128)
            for f in range(FIELDS):
                turn = (shift - 32 * f) % 128
                turned = pltpu.roll(piece, turn, 1) if turn else piece
                end = shift + BASIS
                mask = (lane >= shift) & (lane < end)
                packed[f][tile] = jnp.where(mask, turned, packed[f][tile])
                if end > 128:
                    packed[f][tile + 1] = jnp.where(lane < end - 128, turned, packed[f][tile + 1])
    for f in range(FIELDS):
        back[f] = jnp.concatenate(packed[f], axis=1)
    going = [None]
    for d in range(1, SUBS):
        copy = pltpu.make_async_remote_copy(
            src_ref=back.at[peers[d]], dst_ref=home.at[me], send_sem=back_send_sem.at[d],
            recv_sem=back_recv_sem.at[d], device_id={"sub": peers[d]}, device_id_type=MESH)
        copy.start()
        going.append(copy)
    home[me] = back[me]
    for d in range(1, SUBS):
        going[d].wait_send()
        pltpu.make_async_remote_copy(
            src_ref=back.at[peers[d]], dst_ref=home.at[origins[d]], send_sem=back_send_sem.at[d],
            recv_sem=back_recv_sem.at[d], device_id={"sub": peers[d]}, device_id_type=MESH).wait_recv()
    out_ref[...] = jnp.zeros_like(out_ref)
    for q in range(SUBS):
        out_ref[6 * q:6 * q + LAYERS, :] += home[q, 0:LAYERS, 0:729]


def volume_residual(coefficients, stiffness, volume):
    constants = constant_tables()
    vmem = pl.BlockSpec(memory_space=pltpu.VMEM)
    anywhere = pl.BlockSpec(memory_space=pl.ANY)
    smem = pl.BlockSpec(memory_space=pltpu.SMEM)
    return pl.pallas_call(
        volume_kernel,
        name="volume",
        out_shape=jax.ShapeDtypeStruct((BASIS, BASIS * BASIS), jnp.float32),
        in_specs=[vmem, anywhere, anywhere] + [vmem] * 6 + [smem],
        out_specs=vmem,
        scratch_shapes=[
            pltpu.VMEM((SLAB, QUAD * QUAD), jnp.float32),
            pltpu.VMEM((SLAB, QUAD * QUAD), jnp.float32),
            pltpu.VMEM((SUBS, 16, 768), jnp.float32),
            pltpu.VMEM((SUBS, 16, 768), jnp.float32),
            pltpu.VMEM((SUBS, 16, 768), jnp.float32),
            pltpu.VMEM((SUBS, 16, 768), jnp.float32),
            pltpu.VMEM((BASIS, 2 * SLAB, 128), jnp.float32),
            pltpu.VMEM((BASIS, 2 * SLAB, 128), jnp.float32),
            pltpu.SemaphoreType.DMA((2,)),
            pltpu.SemaphoreType.DMA((SUBS,)),
            pltpu.SemaphoreType.DMA((SUBS,)),
            pltpu.SemaphoreType.DMA((SUBS,)),
            pltpu.SemaphoreType.DMA((SUBS,)),
        ],
        compiler_params=pltpu.CompilerParams(collective_id=0, has_side_effects=True),
        cost_estimate=pl.CostEstimate(flops=10**10, bytes_accessed=4 * 10**6, transcendentals=0),
    )(coefficients, stiffness, volume, *constants)


def per_device(state, stiff_weight, volume_weight, lagrange, mortar, links):
    patches = lax.axis_size("patch")
    device = lax.axis_index("patch")
    vectors = state.shape[2]
    size_n = state.shape[3]
    slot_count = mortar.shape[0]
    coefficients = state[0, 0]
    stiffness = stiff_weight[0]
    volume = volume_weight[0]
    residual = volume_residual(coefficients.reshape(size_n, size_n * size_n), stiffness, volume)
    field_cube = coefficients.reshape(vectors, size_n, size_n, size_n)
    faces = jnp.stack(
        [field_cube[:, 0], field_cube[:, -1], field_cube[:, :, 0], field_cube[:, :, -1]]
    )
    faces = faces.reshape(4, vectors, size_n * size_n)
    item_count = 2 * slot_count
    item_patch = links[:, 0:2].reshape(patches, item_count)
    item_face = links[:, 2:4].reshape(patches, item_count)
    is_live = jnp.repeat(links[:, 4] > 0, 2).reshape(patches, item_count)
    own_patch = lax.dynamic_index_in_dim(item_patch, device, 0, keepdims=False)
    own_face = lax.dynamic_index_in_dim(item_face, device, 0, keepdims=False)
    own_live = lax.dynamic_index_in_dim(is_live, device, 0, keepdims=False)
    own_rows = lax.dynamic_slice_in_dim(links, device * slot_count, slot_count, 0)
    face_grid = jnp.arange(4)
    gathered = gathered_copies(faces[None], "patch", 0)
    picked = jnp.take(
        gathered.reshape(patches * 4, vectors, size_n * size_n), own_patch * 4 + own_face, axis=0
    )
    picked = picked * own_live.astype(jnp.float32)[:, None, None]
    rank_grid = jnp.arange(size_n)
    row_mask = (rank_grid[None, :] < own_rows[:, 4:5]).astype(jnp.float32)
    col_mask = (rank_grid[None, :] < own_rows[:, 5:6]).astype(jnp.float32)
    left = mortar[:, :, 0] * row_mask[:, None, :, None]
    right = mortar[:, :, 1] * col_mask[:, None, :, None]
    traces_here = picked.reshape(slot_count, 2, vectors, size_n, size_n)
    projected = jnp.einsum("sgai,sgvij,sgbj->sgvab", left, traces_here, right, precision=highest)
    constraint = (projected[:, 0] - projected[:, 1]).reshape(
        slot_count, 1, vectors, size_n * size_n
    )
    multipliers = lagrange[:, 0].reshape(slot_count, vectors, size_n, size_n)
    signs = jnp.array([1.0, -1.0], jnp.float32)
    correction = jnp.einsum("sgai,svab,sgbj->sgvij", left, multipliers, right, precision=highest)
    correction = (correction * signs[None, :, None, None, None]).reshape(
        item_count, vectors, size_n * size_n
    )
    all_blocks = lax.all_gather(correction, "patch", axis=0, tiled=True)
    face_match = (
        (is_live & (item_patch == device)).reshape(-1)[None, :]
        & (item_face.reshape(-1)[None, :] == face_grid[:, None])
    ).astype(jnp.float32)
    face_total = jnp.einsum("ft,tvx->fvx", face_match, all_blocks, precision=highest)
    pieces = face_total.reshape(4, vectors, size_n, size_n)
    result_cube = residual.reshape(vectors, size_n, size_n, size_n)
    result_cube = result_cube.at[:, 0].add(pieces[0])
    result_cube = result_cube.at[:, -1].add(pieces[1])
    result_cube = result_cube.at[:, :, 0].add(pieces[2])
    result_cube = result_cube.at[:, :, -1].add(pieces[3])
    return (result_cube.reshape(1, 1, vectors, size_n, size_n * size_n), constraint)


def solution(mesh):
    return jax.shard_map(
        per_device,
        mesh=mesh,
        in_specs=(
            P("patch", "sub", None, None, None),
            P("patch", None, None),
            P("patch", None, None),
            P("patch", "sub", None, None),
            P("patch", None, None, None, None),
            P(),
        ),
        out_specs=(P("patch", "sub", None, None, None), P("patch", "sub", None, None)),
        check_vma=False,
    )
```

```python
import jax
import jax.numpy as jnp
import numpy as np
from jax import lax
from jax.experimental import pallas as pl
from jax.experimental.pallas import tpu as pltpu
from jax.sharding import PartitionSpec as P

ELEMS = 24
DEGREE = 3
FIELDS = 4
BASIS = 27
QUAD = 96
SUBS = 4
SLAB = QUAD // SUBS
LAYERS = SLAB // 4 + DEGREE
STEPS = 12
MESH = pl.DeviceIdType.MESH

stabilize = 0.25
highest = lax.Precision.HIGHEST
gauss_points_four = [
    -0.8611363115940526,
    -0.3399810435848563,
    0.3399810435848563,
    0.8611363115940526,
]
gauss_weights_four = [
    0.3478548451374538,
    0.6521451548625461,
    0.6521451548625461,
    0.3478548451374538,
]


def spline_tables(elements, degree):
    knot_list = np.concatenate(
        [np.zeros(degree), np.arange(elements + 1.0), np.full(degree, float(elements))]
    )
    gauss_nodes = np.array(gauss_points_four)
    gauss_weights = np.array(gauss_weights_four)
    points = (np.arange(elements)[:, None] + (gauss_nodes[None, :] + 1.0) / 2.0).reshape(-1)
    point_weights = np.tile(gauss_weights / 2.0, elements)
    current = np.where(
        (knot_list[None, :-1] <= points[:, None]) & (points[:, None] < knot_list[None, 1:]),
        1.0,
        0.0,
    )
    previous = current
    for order_k in range(1, degree + 1):
        previous = current
        amount = len(knot_list) - 1 - order_k
        current = np.zeros((points.shape[0], amount))
        for column in range(amount):
            left_span = knot_list[column + order_k] - knot_list[column]
            right_span = knot_list[column + order_k + 1] - knot_list[column + 1]
            if left_span > 0:
                current[:, column] += (points - knot_list[column]) / left_span * previous[:, column]
            if right_span > 0:
                current[:, column] += (
                    (knot_list[column + order_k + 1] - points)
                    / right_span
                    * previous[:, column + 1]
                )
    slope_part = np.zeros(current.shape)
    for column in range(current.shape[1]):
        left_span = knot_list[column + degree] - knot_list[column]
        right_span = knot_list[column + degree + 1] - knot_list[column + 1]
        if left_span > 0:
            slope_part[:, column] += degree / left_span * previous[:, column]
        if right_span > 0:
            slope_part[:, column] -= degree / right_span * previous[:, column + 1]
    return (
        current.astype(np.float32),
        slope_part.astype(np.float32),
        (current * point_weights[:, None]).astype(np.float32),
        (slope_part * point_weights[:, None]).astype(np.float32),
    )


def halves(table):
    high = table.astype(jnp.bfloat16).astype(np.float32)
    low = (table - high).astype(jnp.bfloat16).astype(np.float32)
    return high, low


def constant_tables():
    value, slope, value_w, slope_w = spline_tables(ELEMS, DEGREE)
    first = np.zeros((SUBS, 2 * SLAB, 16), np.float32)
    last = np.zeros((SUBS, 16, 2 * SLAB), np.float32)
    for q in range(SUBS):
        rows = slice(SLAB * q, SLAB * (q + 1))
        cols = slice(6 * q, 6 * q + LAYERS)
        first[q, :SLAB, :LAYERS] = value[rows, cols]
        first[q, SLAB:, :LAYERS] = slope[rows, cols]
        last[q, :LAYERS, :SLAB] = slope_w[rows, cols].T
        last[q, :LAYERS, SLAB:] = value_w[rows, cols].T
    high, low = halves(first)
    first = np.concatenate([high, high, low], axis=2)
    high, low = halves(last)
    last = np.concatenate([high, high, low], axis=2)

    def pair_tables(table):
        high, low = halves(table)
        even = np.zeros((256, 256), np.float32)
        odd = np.zeros((256, 256), np.float32)
        for s in range(2):
            cols = slice(128 * s, 128 * s + QUAD)
            even[32 * s:32 * s + BASIS, cols] = high.T
            even[128 + 32 * s:128 + 32 * s + BASIS, cols] = high.T
            even[192 + 32 * s:192 + 32 * s + BASIS, cols] = low.T
            odd[64 + 32 * s:64 + 32 * s + BASIS, cols] = high.T
            odd[128 + 32 * s:128 + 32 * s + BASIS, cols] = low.T
            odd[192 + 32 * s:192 + 32 * s + BASIS, cols] = high.T
        return even, odd

    value_even, value_odd = pair_tables(value)
    slope_even, slope_odd = pair_tables(slope)
    inner = np.stack([value_even, value_odd, slope_even, slope_odd])
    plain = value_odd[:, 128:]

    def adjoint_table(table):
        high, low = halves(table)
        out = np.zeros((512, 256), np.float32)
        for f in range(FIELDS):
            scale = -stabilize if f == FIELDS - 1 else 1.0
            rows = slice(128 * f, 128 * f + QUAD)
            out[rows, 32 * f:32 * f + BASIS] = scale * high
            out[rows, 128 + 32 * f:128 + 32 * f + BASIS] = scale * low
        return out

    high, low = halves(value_w)
    div = np.zeros((128, 256), np.float32)
    div[:QUAD, 96:96 + BASIS] = -high
    div[:QUAD, 224:224 + BASIS] = -low
    adjoint_value = adjoint_table(value_w)
    adjoint_slope = np.concatenate([adjoint_table(slope_w), div])
    middle = np.zeros((STEPS, 128), np.float32)
    for t in range(STEPS):
        for bb in range(8):
            point = 8 * t + bb
            for m in range(4):
                col = 2 * t + bb // 4 + m
                for n, table in enumerate((value, slope, value_w, slope_w)):
                    middle[t, 32 * n + 4 * bb + m] = table[point, col]
    half = lambda x: jnp.asarray(x, jnp.bfloat16)
    return (half(first), half(last), half(inner), half(plain), half(adjoint_value), half(adjoint_slope),
            jnp.asarray(middle, jnp.float32))


def split(x):
    high = x.astype(jnp.bfloat16)
    return high, (x - high.astype(jnp.float32)).astype(jnp.bfloat16)


def product(left, right):
    return jnp.dot(left, right, preferred_element_type=jnp.float32)


def lanes_of(rows):
    return lax.broadcasted_iota(jnp.int32, (rows, 128), 1)


def exact(left, right, dims):
    return lax.dot_general(left, right, (dims, ((), ())), precision=highest, preferred_element_type=jnp.float32)


def to_matrices(tiles, grid):
    for i in range(BASIS):
        tile, shift = divmod(BASIS * i, 128)
        piece = tiles[tile]
        if shift + BASIS > 128:
            piece = jnp.where(lanes_of(piece.shape[0]) >= shift, piece, tiles[tile + 1])
        grid[8 * i:8 * i + piece.shape[0], :] = pltpu.roll(piece, 128 - shift, 1) if shift else piece


def to_rows(row_of, count):
    lane = lanes_of(count)
    tiles = [jnp.zeros((count, 128), jnp.float32) for _ in range(6)]
    for i in range(BASIS):
        tile, shift = divmod(BASIS * i, 128)
        piece = row_of(i)
        piece = pltpu.roll(piece, shift, 1) if shift else piece
        end = shift + BASIS
        tiles[tile] = jnp.where((lane >= shift) & (lane < end), piece, tiles[tile])
        if end > 128:
            tiles[tile + 1] = jnp.where(lane < end - 128, piece, tiles[tile + 1])
    return tiles


def routing(links_ref, y, z, core):
    low_half = lanes_of(32) < 64
    table = jnp.concatenate(
        [links_ref[pl.ds(pl.multiple_of(64 * row + 8 * z, 8), 8), :] for row in range(4)], axis=0
    ).astype(jnp.float32)
    live = table[:, 4:5] > 0.0
    sides = []
    for s in range(2):
        patch = jnp.where(live, table[:, s:s + 1], -1.0)
        sides.append(jnp.where(low_half, patch, table[:, 2 + s:3 + s]))
    natural = jnp.concatenate(sides, axis=0).astype(jnp.bfloat16)
    row = lax.broadcasted_iota(jnp.int32, (128, 64), 0)
    col = lax.broadcasted_iota(jnp.int32, (128, 64), 1)
    source = ((row // 4) % 2) * 32 + (row // 16) * 4 + row % 4
    order = jnp.where(col == source, 1.0, 0.0).astype(jnp.bfloat16)
    keys = product(order, natural)
    faces = pltpu.roll(keys, 64, 1)
    lane = lanes_of(128)
    row = lax.broadcasted_iota(jnp.int32, (128, 128), 0)
    wanted = (16 * y + 2 * (lane // 8) + core).astype(jnp.float32)
    same = (keys == wanted) & (faces == (lane % 4).astype(jnp.float32))
    same = same & ((lane // 4) % 2 == (row // 8) % 2) & (lane < 64)
    return jnp.where(same, 1.0, 0.0)


def operator_kernel(x_ref, stiff_hbm, volume_hbm, lagrange_ref, mortar_ref, links_ref, counts_ref, first_ref,
                    last_ref, inner_ref, plain_ref, adj_value_ref, adj_slope_ref, middle_ref, out_ref,
                    jump_ref, stiff, volume, sent, got, back, home, outer, total, grid, trace_own, trace_all,
                    trace_out, trace_in, fix_own, fix_all, fix_out, fix_in, load_sem, send_sem, recv_sem,
                    back_send_sem, back_recv_sem, face_send_sem, face_recv_sem):
    me = lax.axis_index("sub")
    patch = lax.axis_index("patch")
    y, z, core = patch // 16, (patch // 2) % 8, patch % 2
    group = 2 * y + core
    line = [lax.rem(z + d, 8) for d in range(8)]
    line_from = [lax.rem(z + 8 - d, 8) for d in range(8)]
    plane = [lax.rem(group + d, 8) for d in range(8)]
    plane_from = [lax.rem(group + 8 - d, 8) for d in range(8)]
    line_ids = [{"patch": 16 * y + 2 * at + core} for at in line]
    plane_ids = [{"patch": 16 * (at // 2) + 2 * z + at % 2} for at in plane]

    def exchange(n, source, target, slot, slots_from, ids):
        def one(d, at):
            return pltpu.make_async_remote_copy(
                src_ref=source(d), dst_ref=target.at[at], send_sem=face_send_sem.at[n, d],
                recv_sem=face_recv_sem.at[n, d], device_id=ids[d], device_id_type=MESH)

        def start():
            for d in range(1, 8):
                one(d, slot).start()

        def finish():
            for d in range(1, 8):
                one(d, slot).wait_send()
                one(d, slots_from[d]).wait_recv()

        return start, finish

    rows = pl.ds(pl.multiple_of(me * SLAB, 8), SLAB)
    load_stiff = pltpu.make_async_copy(stiff_hbm.at[0, rows], stiff, load_sem.at[0])
    load_volume = pltpu.make_async_copy(volume_hbm.at[0, rows], volume, load_sem.at[1])
    load_stiff.start()
    load_volume.start()
    peers = [lax.rem(me + d, SUBS) for d in range(SUBS)]
    origins = [lax.rem(me + SUBS - d, SUBS) for d in range(SUBS)]
    barrier = pltpu.get_barrier_semaphore()
    for d in range(1, SUBS):
        pl.semaphore_signal(barrier, inc=1, device_id={"sub": peers[d]}, device_id_type=MESH)
    for d in range(1, 8):
        for ids in (line_ids, plane_ids):
            pl.semaphore_signal(barrier, inc=1, device_id=ids[d], device_id_type=MESH)
    sent[...] = jnp.zeros_like(sent)
    for q in range(SUBS):
        sent[q, 0:LAYERS, 0:729] = x_ref[0, 0, 0, 6 * q:6 * q + LAYERS, :]
    trace_rows = [[x_ref[0, 0, 0, 26 * s:26 * s + 1, 128 * n:min(128 * n + 128, 729)] for n in range(6)] for s in range(2)]
    for s in range(2):
        tail = jnp.zeros((1, 768 - 729), jnp.float32)
        trace_rows[s][5] = jnp.concatenate([trace_rows[s][5], tail], axis=1)
    edge = x_ref[0, 0, 0, :, 0:128]
    trace_rows.append(to_rows(lambda i: edge[i:i + 1, :], 1))
    edge = jnp.concatenate([x_ref[0, 0, 0, :, 640:729], jnp.zeros((BASIS, 39), jnp.float32)], axis=1)
    edge = pltpu.roll(edge, 128 - 62, 1)
    trace_rows.append(to_rows(lambda i: edge[i:i + 1, :], 1))
    for h in range(2):
        for f in range(4):
            for n in range(3):
                trace_own[4 * h + f:4 * h + f + 1, 128 * n:128 * n + 128] = trace_rows[f][3 * h + n]
    start_traces, finish_traces = exchange(0, lambda d: trace_own, trace_all, z, line_from, line_ids)
    start_picked, finish_picked = exchange(1, lambda d: trace_out.at[plane[d]], trace_in, group, plane_from, plane_ids)
    start_fixes, finish_fixes = exchange(2, lambda d: fix_own, fix_all, group, plane_from, plane_ids)
    start_sums, finish_sums = exchange(3, lambda d: fix_out.at[line[d]], fix_in, z, line_from, line_ids)
    pl.semaphore_wait(barrier, SUBS - 1 + 14)
    going = [None]
    for d in range(1, SUBS):
        copy = pltpu.make_async_remote_copy(
            src_ref=sent.at[peers[d]], dst_ref=got.at[me], send_sem=send_sem.at[d], recv_sem=recv_sem.at[d],
            device_id={"sub": peers[d]}, device_id_type=MESH)
        copy.start()
        going.append(copy)
    start_traces()
    trace_all[z] = trace_own[...]
    got[me] = sent[me]
    row = lax.broadcasted_iota(jnp.int32, (BASIS, BASIS), 0)
    lefts, rights = [], []
    for s in range(2):
        for slot in range(4):
            at = 4 * patch + slot
            lefts.append(jnp.where(row < counts_ref[at, 4], mortar_ref[slot, s, 0], 0.0))
            rights.append(jnp.where(row < counts_ref[at, 5], mortar_ref[slot, s, 1], 0.0))
    multipliers = jnp.concatenate([lagrange_ref[slot, 0] for slot in range(4)], axis=0)
    multipliers = jnp.concatenate([multipliers, jnp.zeros((4, 768 - 729), jnp.float32)], axis=1)
    to_matrices([multipliers[:, 128 * n:128 * n + 128] for n in range(6)], grid)
    given = [grid[pl.ds(slot, BASIS, stride=8), :][:, 0:BASIS] for slot in range(4)]
    for k in range(8):
        fix = exact(given[k % 4], rights[k], ((1,), (0,)))
        fix = exact(lefts[k], fix, ((0,), (0,)))
        fix = fix if k < 4 else -fix
        grid[pl.ds(k, BASIS, stride=8), :] = jnp.concatenate(
            [fix, jnp.zeros((BASIS, 128 - BASIS), jnp.float32)], axis=1)
    fix_rows = to_rows(lambda i: grid[8 * i:8 * i + 8, :], 8)
    for h in range(2):
        for n in range(3):
            fix_own[8 * h:8 * h + 8, 128 * n:128 * n + 128] = fix_rows[3 * h + n]
    start_fixes()
    fix_all[group] = fix_own[...]
    route = routing(links_ref, y, z, core)
    total[...] = jnp.zeros_like(total)
    for d in range(1, SUBS):
        going[d].wait_send()
        pltpu.make_async_remote_copy(
            src_ref=sent.at[peers[d]], dst_ref=got.at[origins[d]], send_sem=send_sem.at[d],
            recv_sem=recv_sem.at[d], device_id={"sub": peers[d]}, device_id_type=MESH).wait_recv()

    first = first_ref[me]
    spread = []
    for f in range(FIELDS):
        high, low = split(got[f])
        spread.append(product(first, jnp.concatenate([high, low, high], axis=0)))
    lane = lanes_of(2 * SLAB)
    for j in range(BASIS):
        tile, shift = divmod(BASIS * j, 128)
        merged = None
        for f in range(FIELDS):
            piece = spread[f][:, 128 * tile:128 * tile + 128]
            if shift + BASIS > 128:
                piece = jnp.where(lane >= shift, piece, spread[f][:, 128 * tile + 128:128 * tile + 256])
            turn = (32 * f - shift) % 128
            piece = pltpu.roll(piece, turn, 1) if turn else piece
            merged = piece if f == 0 else jnp.where(lane >= 32 * f, piece, merged)
        outer[j] = merged
    load_stiff.wait()
    load_volume.wait()

    def step(t, carry):
        def scalar(table, bb, m):
            return middle_ref[t, 32 * table + 4 * bb + m]

        window = [outer[2 * t + m] for m in range(5)]
        values = [w[0:SLAB] for w in window]
        slopes = [w[SLAB:2 * SLAB] for w in window]

        def middle_sum(table, parts, bb):
            e = bb // 4
            out = scalar(table, bb, 0) * parts[e]
            for m in range(1, 4):
                out = out + scalar(table, bb, m) * parts[e + m]
            return out

        across = [middle_sum(0, slopes, bb) for bb in range(8)] + [middle_sum(1, values, bb) for bb in range(8)]
        along = [middle_sum(0, values, bb) for bb in range(8)]

        def pair_sides(x):
            lane = lanes_of(x.shape[0])
            high = x.astype(jnp.bfloat16)
            wide = high.astype(jnp.float32)
            low = x - wide
            turned = pltpu.roll(wide, 64, 1)
            even = jnp.where(lane < 64, low, turned).astype(jnp.bfloat16)
            odd = jnp.where(lane < 64, turned, low).astype(jnp.bfloat16)
            return jnp.concatenate([high, even], axis=1), jnp.concatenate([high, odd], axis=1)

        even, odd = pair_sides(jnp.concatenate(across, axis=0))
        across_even = product(even, inner_ref[0])
        across_odd = product(odd, inner_ref[1])
        even, odd = pair_sides(jnp.concatenate(along, axis=0))
        along_even = product(even, inner_ref[2])
        along_odd = product(odd, inner_ref[3])
        pvalue = product(odd, plain_ref[...])

        def weights(ref):
            lane = lanes_of(SLAB)
            tiles = [ref[:, pl.ds(pl.multiple_of(768 * t + 128 * n, 128), 128)] for n in range(6)]
            parts = []
            for bb in range(8):
                tile, shift = divmod(QUAD * bb, 128)
                part = tiles[tile]
                if shift + QUAD > 128:
                    part = jnp.where(lane >= shift, part, tiles[tile + 1])
                parts.append(pltpu.roll(part, 128 - shift, 1) if shift else part)
            return jnp.concatenate(parts, axis=0)

        s = weights(stiff)
        w = weights(volume)
        half = 8 * SLAB
        pressed = w * pvalue
        grads = [
            [across_even[0:half, 0:128], across_even[0:half, 128:256], across_odd[0:half, 0:128],
             across_odd[0:half, 128:256]],
            [across_even[half:, 0:128], across_even[half:, 128:256], across_odd[half:, 0:128],
             across_odd[half:, 128:256]],
            [along_even[:, 0:128], along_even[:, 128:256], along_odd[:, 0:128], along_odd[:, 128:256]],
        ]
        fluxes = []
        for d in range(3):
            fluxes.append([s * grads[d][f] - pressed if f == d else s * grads[d][f] for f in range(FIELDS)])
        spill = w * (grads[0][0] + grads[1][1] + grads[2][2])

        def adjoint(parts, table):
            pairs = [split(p) for p in parts]
            wide = product(jnp.concatenate([p[0] for p in pairs], axis=1), table[...])
            low = product(jnp.concatenate([p[1] for p in pairs], axis=1), table[:, 0:128])
            return wide[:, 0:128] + wide[:, 128:256] + low

        heads = [adjoint(fluxes[0], adj_value_ref), adjoint(fluxes[1], adj_value_ref),
                 adjoint(fluxes[2] + [spill], adj_slope_ref)]
        heads = [[h[SLAB * bb:SLAB * bb + SLAB] for bb in range(8)] for h in heads]
        sums = [[None, None] for _ in range(5)]
        for bb in range(8):
            for m in range(4):
                at = bb // 4 + m
                v = scalar(2, bb, m)
                terms = [v * heads[0][bb], scalar(3, bb, m) * heads[1][bb] + v * heads[2][bb]]
                sums[at] = [a if b is None else b + a for a, b in zip(terms, sums[at])]
        for m in range(5):
            total[2 * t + m] += jnp.concatenate(sums[m], axis=0)
        return carry

    lax.fori_loop(0, STEPS // 2, step, 0)
    finish_traces()
    high, low = split(trace_all[...].reshape(64, 384))
    both = (route + pltpu.roll(route, 64, 1)).astype(jnp.bfloat16)
    trace_out[...] = product(both, jnp.concatenate([high, low], axis=0)).reshape(8, 16, 384)
    start_picked()
    trace_in[group] = trace_out[group]
    finish_fixes()
    high, low = split(fix_all[...].reshape(128, 384))
    flipped = route.T.astype(jnp.bfloat16)[0:64]
    fix_out[...] = product(jnp.concatenate([flipped, flipped], axis=1),
                           jnp.concatenate([high, low], axis=0)).reshape(8, 8, 384)
    start_sums()
    fix_in[z] = fix_out[z]
    lax.fori_loop(STEPS // 2, STEPS, step, 0)

    last = last_ref[me]
    lane = lanes_of(16)
    packed = [[jnp.zeros((16, 128), jnp.float32) for _ in range(6)] for _ in range(FIELDS)]
    for j0 in range(0, BASIS, 2):
        some = list(range(j0, min(j0 + 2, BASIS)))
        columns = []
        for j in some:
            high, low = split(total[j])
            columns.append(jnp.concatenate([high, low, high], axis=0))
        result = product(last, jnp.concatenate(columns, axis=1))
        for n, j in enumerate(some):
            piece = result[:, 128 * n:128 * n + 128]
            tile, shift = divmod(BASIS * j, 128)
            for f in range(FIELDS):
                turn = (shift - 32 * f) % 128
                turned = pltpu.roll(piece, turn, 1) if turn else piece
                end = shift + BASIS
                mask = (lane >= shift) & (lane < end)
                packed[f][tile] = jnp.where(mask, turned, packed[f][tile])
                if end > 128:
                    packed[f][tile + 1] = jnp.where(lane < end - 128, turned, packed[f][tile + 1])
    for f in range(FIELDS):
        back[f] = jnp.concatenate(packed[f], axis=1)
    going = [None]
    for d in range(1, SUBS):
        copy = pltpu.make_async_remote_copy(
            src_ref=back.at[peers[d]], dst_ref=home.at[me], send_sem=back_send_sem.at[d],
            recv_sem=back_recv_sem.at[d], device_id={"sub": peers[d]}, device_id_type=MESH)
        copy.start()
        going.append(copy)
    home[me] = back[me]
    finish_picked()
    picked = trace_in[0]
    for at in range(1, 8):
        picked = picked + trace_in[at]
    to_matrices([picked[8 * h:8 * h + 8, 128 * n:128 * n + 128] for h in range(2) for n in range(3)], grid)
    jumps = []
    for k in range(8):
        jump = exact(grid[pl.ds(k, BASIS, stride=8), :][:, 0:BASIS], rights[k], ((1,), (1,)))
        jumps.append(exact(lefts[k], jump, ((1,), (0,))))
    for slot in range(4):
        grid[pl.ds(slot, BASIS, stride=8), :] = jnp.concatenate(
            [jumps[slot] - jumps[4 + slot], jnp.zeros((BASIS, 128 - BASIS), jnp.float32)], axis=1)
    jump_rows = jnp.concatenate(to_rows(lambda i: grid[8 * i:8 * i + 8, :], 8), axis=1)
    for slot in range(4):
        jump_ref[slot, 0] = jump_rows[slot:slot + 1, 0:729]
    finish_sums()
    sums = fix_in[0]
    for at in range(1, 8):
        sums = sums + fix_in[at]
    sums = [sums[4 * h:4 * h + 4, 128 * n:128 * n + 128] for h in range(2) for n in range(3)]
    to_matrices(sums, grid)
    lane = lanes_of(BASIS)
    inside = lane < BASIS
    near = jnp.where(inside, grid[pl.ds(2, BASIS, stride=8), :], 0.0)
    far = jnp.where(inside, grid[pl.ds(3, BASIS, stride=8), :], 0.0)
    far = pltpu.roll(far, 62, 1)
    ends = jnp.concatenate(sums, axis=1)
    for d in range(1, SUBS):
        going[d].wait_send()
        pltpu.make_async_remote_copy(
            src_ref=back.at[peers[d]], dst_ref=home.at[origins[d]], send_sem=back_send_sem.at[d],
            recv_sem=back_recv_sem.at[d], device_id={"sub": peers[d]}, device_id_type=MESH).wait_recv()
    out_ref[0, 0, 0] = jnp.zeros((BASIS, BASIS * BASIS), jnp.float32)
    for q in range(SUBS):
        out_ref[0, 0, 0, 6 * q:6 * q + LAYERS, :] += home[q, 0:LAYERS, 0:729]
    for s in range(2):
        out_ref[0, 0, 0, 26 * s:26 * s + 1, :] += ends[s:s + 1, 0:729]
    out_ref[0, 0, 0, :, 0:128] += near
    out_ref[0, 0, 0, :, 640:729] += far[:, 0:89]


def per_device(state, stiff_weight, volume_weight, lagrange, mortar, links):
    vmem = pl.BlockSpec(memory_space=pltpu.VMEM)
    anywhere = pl.BlockSpec(memory_space=pl.ANY)
    smem = pl.BlockSpec(memory_space=pltpu.SMEM)
    return pl.pallas_call(
        operator_kernel,
        name="operator",
        out_shape=(jax.ShapeDtypeStruct(state.shape, jnp.float32), jax.ShapeDtypeStruct(lagrange.shape, jnp.float32)),
        in_specs=[vmem, anywhere, anywhere, vmem, vmem, vmem, smem] + [vmem] * 6 + [smem],
        out_specs=(vmem, vmem),
        scratch_shapes=[
            pltpu.VMEM((SLAB, QUAD * QUAD), jnp.float32),
            pltpu.VMEM((SLAB, QUAD * QUAD), jnp.float32),
            pltpu.VMEM((SUBS, 16, 768), jnp.float32),
            pltpu.VMEM((SUBS, 16, 768), jnp.float32),
            pltpu.VMEM((SUBS, 16, 768), jnp.float32),
            pltpu.VMEM((SUBS, 16, 768), jnp.float32),
            pltpu.VMEM((BASIS, 2 * SLAB, 128), jnp.float32),
            pltpu.VMEM((BASIS, 2 * SLAB, 128), jnp.float32),
            pltpu.VMEM((BASIS * 8, 128), jnp.float32),
            pltpu.VMEM((8, 384), jnp.float32),
            pltpu.VMEM((8, 8, 384), jnp.float32),
            pltpu.VMEM((8, 16, 384), jnp.float32),
            pltpu.VMEM((8, 16, 384), jnp.float32),
            pltpu.VMEM((16, 384), jnp.float32),
            pltpu.VMEM((8, 16, 384), jnp.float32),
            pltpu.VMEM((8, 8, 384), jnp.float32),
            pltpu.VMEM((8, 8, 384), jnp.float32),
            pltpu.SemaphoreType.DMA((2,)),
            pltpu.SemaphoreType.DMA((SUBS,)),
            pltpu.SemaphoreType.DMA((SUBS,)),
            pltpu.SemaphoreType.DMA((SUBS,)),
            pltpu.SemaphoreType.DMA((SUBS,)),
            pltpu.SemaphoreType.DMA((4, 8)),
            pltpu.SemaphoreType.DMA((4, 8)),
        ],
        compiler_params=pltpu.CompilerParams(collective_id=0, has_side_effects=True),
        cost_estimate=pl.CostEstimate(flops=10**10, bytes_accessed=4 * 10**6, transcendentals=0),
    )(state, stiff_weight, volume_weight, lagrange, mortar, links, links, *constant_tables())


def solution(mesh):
    return jax.shard_map(
        per_device,
        mesh=mesh,
        in_specs=(
            P("patch", "sub", None, None, None),
            P("patch", None, None),
            P("patch", None, None),
            P("patch", "sub", None, None),
            P("patch", None, None, None, None),
            P(),
        ),
        out_specs=(P("patch", "sub", None, None, None), P("patch", "sub", None, None)),
        check_vma=False,
    )
```

```python
import jax
import jax.numpy as jnp
import numpy as np
from jax import lax
from jax.experimental import pallas as pl
from jax.experimental.pallas import tpu as pltpu
from jax.sharding import PartitionSpec as P

ELEMS = 24
DEGREE = 3
FIELDS = 4
BASIS = 27
QUAD = 96
SUBS = 4
SLAB = QUAD // SUBS
LAYERS = SLAB // 4 + DEGREE
STEPS = 12
MESH = pl.DeviceIdType.MESH

stabilize = 0.25
highest = lax.Precision.HIGHEST
gauss_points_four = [
    -0.8611363115940526,
    -0.3399810435848563,
    0.3399810435848563,
    0.8611363115940526,
]
gauss_weights_four = [
    0.3478548451374538,
    0.6521451548625461,
    0.6521451548625461,
    0.3478548451374538,
]


def spline_tables(elements, degree):
    knot_list = np.concatenate(
        [np.zeros(degree), np.arange(elements + 1.0), np.full(degree, float(elements))]
    )
    gauss_nodes = np.array(gauss_points_four)
    gauss_weights = np.array(gauss_weights_four)
    points = (np.arange(elements)[:, None] + (gauss_nodes[None, :] + 1.0) / 2.0).reshape(-1)
    point_weights = np.tile(gauss_weights / 2.0, elements)
    current = np.where(
        (knot_list[None, :-1] <= points[:, None]) & (points[:, None] < knot_list[None, 1:]),
        1.0,
        0.0,
    )
    previous = current
    for order_k in range(1, degree + 1):
        previous = current
        amount = len(knot_list) - 1 - order_k
        current = np.zeros((points.shape[0], amount))
        for column in range(amount):
            left_span = knot_list[column + order_k] - knot_list[column]
            right_span = knot_list[column + order_k + 1] - knot_list[column + 1]
            if left_span > 0:
                current[:, column] += (points - knot_list[column]) / left_span * previous[:, column]
            if right_span > 0:
                current[:, column] += (
                    (knot_list[column + order_k + 1] - points)
                    / right_span
                    * previous[:, column + 1]
                )
    slope_part = np.zeros(current.shape)
    for column in range(current.shape[1]):
        left_span = knot_list[column + degree] - knot_list[column]
        right_span = knot_list[column + degree + 1] - knot_list[column + 1]
        if left_span > 0:
            slope_part[:, column] += degree / left_span * previous[:, column]
        if right_span > 0:
            slope_part[:, column] -= degree / right_span * previous[:, column + 1]
    return (
        current.astype(np.float32),
        slope_part.astype(np.float32),
        (current * point_weights[:, None]).astype(np.float32),
        (slope_part * point_weights[:, None]).astype(np.float32),
    )


def halves(table):
    high = table.astype(jnp.bfloat16).astype(np.float32)
    low = (table - high).astype(jnp.bfloat16).astype(np.float32)
    return high, low


def constant_tables():
    value, slope, value_w, slope_w = spline_tables(ELEMS, DEGREE)
    first = np.zeros((SUBS, 2 * SLAB, 16), np.float32)
    last = np.zeros((SUBS, 16, 2 * SLAB), np.float32)
    for q in range(SUBS):
        rows = slice(SLAB * q, SLAB * (q + 1))
        cols = slice(6 * q, 6 * q + LAYERS)
        first[q, :SLAB, :LAYERS] = value[rows, cols]
        first[q, SLAB:, :LAYERS] = slope[rows, cols]
        last[q, :LAYERS, :SLAB] = slope_w[rows, cols].T
        last[q, :LAYERS, SLAB:] = value_w[rows, cols].T
    high, low = halves(first)
    first = np.concatenate([high, high, low], axis=2)
    high, low = halves(last)
    last = np.concatenate([high, high, low], axis=2)

    def pair_tables(table):
        high, low = halves(table)
        even = np.zeros((256, 256), np.float32)
        odd = np.zeros((256, 256), np.float32)
        for s in range(2):
            cols = slice(128 * s, 128 * s + QUAD)
            even[32 * s:32 * s + BASIS, cols] = high.T
            even[128 + 32 * s:128 + 32 * s + BASIS, cols] = high.T
            even[192 + 32 * s:192 + 32 * s + BASIS, cols] = low.T
            odd[64 + 32 * s:64 + 32 * s + BASIS, cols] = high.T
            odd[128 + 32 * s:128 + 32 * s + BASIS, cols] = low.T
            odd[192 + 32 * s:192 + 32 * s + BASIS, cols] = high.T
        return even, odd

    value_even, value_odd = pair_tables(value)
    slope_even, slope_odd = pair_tables(slope)
    inner = np.stack([value_even, value_odd, slope_even, slope_odd])
    plain = value_odd[:, 128:]

    def adjoint_table(table):
        high, low = halves(table)
        out = np.zeros((512, 256), np.float32)
        for f in range(FIELDS):
            scale = -stabilize if f == FIELDS - 1 else 1.0
            rows = slice(128 * f, 128 * f + QUAD)
            out[rows, 32 * f:32 * f + BASIS] = scale * high
            out[rows, 128 + 32 * f:128 + 32 * f + BASIS] = scale * low
        return out

    high, low = halves(value_w)
    div = np.zeros((128, 256), np.float32)
    div[:QUAD, 96:96 + BASIS] = -high
    div[:QUAD, 224:224 + BASIS] = -low
    adjoint_value = adjoint_table(value_w)
    adjoint_slope = np.concatenate([adjoint_table(slope_w), div])
    middle = np.zeros((STEPS, 128), np.float32)
    for t in range(STEPS):
        for bb in range(8):
            point = 8 * t + bb
            for m in range(4):
                col = 2 * t + bb // 4 + m
                for n, table in enumerate((value, slope, value_w, slope_w)):
                    middle[t, 32 * n + 4 * bb + m] = table[point, col]
    half = lambda x: jnp.asarray(x, jnp.bfloat16)
    return (half(first), half(last), half(inner), half(plain), half(adjoint_value), half(adjoint_slope),
            jnp.asarray(middle, jnp.float32))


def split(x):
    high = x.astype(jnp.bfloat16)
    return high, (x - high.astype(jnp.float32)).astype(jnp.bfloat16)


def product(left, right):
    return jnp.dot(left, right, preferred_element_type=jnp.float32)


def lanes_of(rows):
    return lax.broadcasted_iota(jnp.int32, (rows, 128), 1)


def exact(left, right, dims):
    return lax.dot_general(left, right, (dims, ((), ())), precision=highest, preferred_element_type=jnp.float32)


def to_matrices(tiles, grid):
    for i in range(BASIS):
        tile, shift = divmod(BASIS * i, 128)
        piece = tiles[tile]
        if shift + BASIS > 128:
            piece = jnp.where(lanes_of(piece.shape[0]) >= shift, piece, tiles[tile + 1])
        grid[8 * i:8 * i + piece.shape[0], :] = pltpu.roll(piece, 128 - shift, 1) if shift else piece


def to_rows(row_of, count):
    lane = lanes_of(count)
    tiles = [jnp.zeros((count, 128), jnp.float32) for _ in range(6)]
    for i in range(BASIS):
        tile, shift = divmod(BASIS * i, 128)
        piece = row_of(i)
        piece = pltpu.roll(piece, shift, 1) if shift else piece
        end = shift + BASIS
        tiles[tile] = jnp.where((lane >= shift) & (lane < end), piece, tiles[tile])
        if end > 128:
            tiles[tile + 1] = jnp.where(lane < end - 128, piece, tiles[tile + 1])
    return tiles


def ninth_layer(ref, at):
    first = lax.broadcasted_iota(jnp.int32, (8, 768), 0) == 0
    line = jnp.concatenate([ref[at, n:n + 1, 768:896] for n in range(6)], axis=1)
    return jnp.where(first, line, 0.0)


def routing(links_ref, y, z, core):
    row = lax.broadcasted_iota(jnp.int32, (128, 256), 0)
    col = lax.broadcasted_iota(jnp.int32, (128, 256), 1)
    source = ((row // 32) * 16 + 2 * z + (row // 16) % 2) * 4 + row % 4
    order = jnp.where(col == source, 1.0, 0.0).astype(jnp.bfloat16)
    table = links_ref[...].astype(jnp.float32).astype(jnp.bfloat16)
    found = lax.dot_general(order, table, (((1,), (1,)), ((), ())), preferred_element_type=jnp.float32)
    row = lax.broadcasted_iota(jnp.int32, (128, 1), 0)
    second = (row // 4) % 2 == 1
    patch = jnp.where(second, found[:, 1:2], found[:, 0:1])
    face = jnp.where(second, found[:, 3:4], found[:, 2:3])
    patch = jnp.where(found[:, 4:5] > 0.0, patch, -1.0)
    lane = lanes_of(128)
    row = lax.broadcasted_iota(jnp.int32, (128, 128), 0)
    wanted = (16 * y + 2 * (lane // 8) + core).astype(jnp.float32)
    same = (patch == wanted) & (face == (lane % 4).astype(jnp.float32))
    same = same & ((lane // 4) % 2 == (row // 8) % 2) & (lane < 64)
    return jnp.where(same, 1.0, 0.0)


def operator_kernel(x_hbm, stiff_hbm, volume_hbm, lagrange_hbm, mortar_hbm, links_hbm, first_hbm, last_hbm,
                    inner_hbm, plain_hbm, adj_value_hbm, adj_slope_hbm, middle_hbm, out_ref, jump_ref,
                    x_ref, lagrange_ref, mortar_ref, links_ref, counts_ref, first_ref, last_ref, inner_ref,
                    plain_ref, adj_value_ref, adj_slope_ref, middle_ref, stiff, volume, sent, got, back, home, outer, total, grid, trace_own, trace_all,
                    trace_out, trace_in, fix_own, fix_all, fix_out, fix_in, load_sem, send_sem, recv_sem,
                    back_send_sem, back_recv_sem, face_send_sem, face_recv_sem):
    me = lax.axis_index("sub")
    patch = lax.axis_index("patch")
    y, z, core = patch // 16, (patch // 2) % 8, patch % 2
    group = 2 * y + core
    line = [lax.rem(z + d, 8) for d in range(8)]
    line_from = [lax.rem(z + 8 - d, 8) for d in range(8)]
    plane = [lax.rem(group + d, 8) for d in range(8)]
    plane_from = [lax.rem(group + 8 - d, 8) for d in range(8)]
    line_ids = [{"patch": 16 * y + 2 * at + core} for at in line]
    plane_ids = [{"patch": 16 * (at // 2) + 2 * z + at % 2} for at in plane]

    def exchange(n, source, target, slot, slots_from, ids):
        def one(d, at):
            return pltpu.make_async_remote_copy(
                src_ref=source(d), dst_ref=target.at[at], send_sem=face_send_sem.at[n, d],
                recv_sem=face_recv_sem.at[n, d], device_id=ids[d], device_id_type=MESH)

        def start():
            for d in range(1, 8):
                one(d, slot).start()

        def finish():
            for d in range(1, 8):
                one(d, slot).wait_send()
                one(d, slots_from[d]).wait_recv()

        return start, finish

    rows = pl.ds(pl.multiple_of(me * SLAB, 8), SLAB)
    pairs = [(slot, s, n) for slot in range(4) for s in range(2) for n in range(2)]
    loads = [
        [(x_hbm.at[0, 0, :, 0, :], x_ref)],
        [(links_hbm, links_ref)],
        [(links_hbm, counts_ref)],
        [(lagrange_hbm, lagrange_ref)],
        [(mortar_hbm.at[slot, s, :, n, :], mortar_ref.at[slot, s, n]) for slot, s, n in pairs],
        [(first_hbm.at[me], first_ref)],
        [(middle_hbm, middle_ref)],
        [(inner_hbm, inner_ref), (plain_hbm, plain_ref)],
        [(stiff_hbm.at[0, rows], stiff), (volume_hbm.at[0, rows], volume)],
        [(adj_value_hbm, adj_value_ref), (adj_slope_hbm, adj_slope_ref)],
        [(last_hbm.at[me], last_ref)],
    ]
    loads = [[pltpu.make_async_copy(a, b, load_sem.at[n]) for a, b in some] for n, some in enumerate(loads)]
    for some in loads:
        for copy in some:
            copy.start()

    def loaded(*which):
        for n in which:
            for copy in loads[n]:
                copy.wait()

    peers = [lax.rem(me + d, SUBS) for d in range(SUBS)]
    origins = [lax.rem(me + SUBS - d, SUBS) for d in range(SUBS)]
    barrier = pltpu.get_barrier_semaphore()
    for d in range(1, SUBS):
        pl.semaphore_signal(barrier, inc=1, device_id={"sub": peers[d]}, device_id_type=MESH)
    for d in range(1, 8):
        for ids in (line_ids, plane_ids):
            pl.semaphore_signal(barrier, inc=1, device_id=ids[d], device_id_type=MESH)
    loaded(0)
    sent[...] = jnp.zeros_like(sent)
    for q in range(SUBS):
        sent[q, :, 0:729] = x_ref[6 * q:6 * q + 8, :]
        for n in range(6):
            width = min(128, 729 - 128 * n)
            sent[q, n:n + 1, 768:768 + width] = x_ref[6 * q + 8:6 * q + 9, 128 * n:128 * n + width]
    trace_rows = [[x_ref[26 * s:26 * s + 1, 128 * n:min(128 * n + 128, 729)] for n in range(6)] for s in range(2)]
    for s in range(2):
        tail = jnp.zeros((1, 768 - 729), jnp.float32)
        trace_rows[s][5] = jnp.concatenate([trace_rows[s][5], tail], axis=1)
    edge = x_ref[:, 0:128]
    trace_rows.append(to_rows(lambda i: edge[i:i + 1, :], 1))
    edge = jnp.concatenate([x_ref[:, 640:729], jnp.zeros((BASIS, 39), jnp.float32)], axis=1)
    edge = pltpu.roll(edge, 128 - 62, 1)
    trace_rows.append(to_rows(lambda i: edge[i:i + 1, :], 1))
    for h in range(2):
        for f in range(4):
            for n in range(3):
                trace_own[4 * h + f:4 * h + f + 1, 128 * n:128 * n + 128] = trace_rows[f][3 * h + n]
    start_traces, finish_traces = exchange(0, lambda d: trace_own, trace_all, z, line_from, line_ids)
    start_picked, finish_picked = exchange(1, lambda d: trace_out.at[plane[d]], trace_in, group, plane_from, plane_ids)
    start_fixes, finish_fixes = exchange(2, lambda d: fix_own, fix_all, group, plane_from, plane_ids)
    start_sums, finish_sums = exchange(3, lambda d: fix_out.at[line[d]], fix_in, z, line_from, line_ids)
    pl.semaphore_wait(barrier, SUBS - 1 + 14)
    going = [None]
    for d in range(1, SUBS):
        copy = pltpu.make_async_remote_copy(
            src_ref=sent.at[peers[d]], dst_ref=got.at[me], send_sem=send_sem.at[d], recv_sem=recv_sem.at[d],
            device_id={"sub": peers[d]}, device_id_type=MESH)
        copy.start()
        going.append(copy)
    start_traces()
    trace_all[z] = trace_own[...]
    got[me] = sent[me]
    loaded(1, 2, 3, 4)
    row = lax.broadcasted_iota(jnp.int32, (BASIS, BASIS), 0)
    lefts, rights = [], []
    for s in range(2):
        for slot in range(4):
            at = 4 * patch + slot
            lefts.append(jnp.where(row < counts_ref[4, at], mortar_ref[slot, s, 0], 0.0))
            rights.append(jnp.where(row < counts_ref[5, at], mortar_ref[slot, s, 1], 0.0))
    multipliers = jnp.concatenate([lagrange_ref[slot, 0] for slot in range(4)], axis=0)
    multipliers = jnp.concatenate([multipliers, jnp.zeros((4, 768 - 729), jnp.float32)], axis=1)
    to_matrices([multipliers[:, 128 * n:128 * n + 128] for n in range(6)], grid)
    given = [grid[pl.ds(slot, BASIS, stride=8), :][:, 0:BASIS] for slot in range(4)]
    for k in range(8):
        fix = exact(given[k % 4], rights[k], ((1,), (0,)))
        fix = exact(lefts[k], fix, ((0,), (0,)))
        fix = fix if k < 4 else -fix
        grid[pl.ds(k, BASIS, stride=8), :] = jnp.concatenate(
            [fix, jnp.zeros((BASIS, 128 - BASIS), jnp.float32)], axis=1)
    fix_rows = to_rows(lambda i: grid[8 * i:8 * i + 8, :], 8)
    for h in range(2):
        for n in range(3):
            fix_own[8 * h:8 * h + 8, 128 * n:128 * n + 128] = fix_rows[3 * h + n]
    start_fixes()
    fix_all[group] = fix_own[...]
    route = routing(links_ref, y, z, core)
    total[...] = jnp.zeros_like(total)
    for d in range(1, SUBS):
        going[d].wait_send()
        pltpu.make_async_remote_copy(
            src_ref=sent.at[peers[d]], dst_ref=got.at[origins[d]], send_sem=send_sem.at[d],
            recv_sem=recv_sem.at[d], device_id={"sub": peers[d]}, device_id_type=MESH).wait_recv()

    loaded(5)
    first = first_ref[...]
    spread = []
    for f in range(FIELDS):
        high, low = split(jnp.concatenate([got[f, :, 0:768], ninth_layer(got, f)], axis=0))
        spread.append(product(first, jnp.concatenate([high, low, high], axis=0)))
    lane = lanes_of(2 * SLAB)
    for j in range(BASIS):
        tile, shift = divmod(BASIS * j, 128)
        merged = None
        for f in range(FIELDS):
            piece = spread[f][:, 128 * tile:128 * tile + 128]
            if shift + BASIS > 128:
                piece = jnp.where(lane >= shift, piece, spread[f][:, 128 * tile + 128:128 * tile + 256])
            turn = (32 * f - shift) % 128
            piece = pltpu.roll(piece, turn, 1) if turn else piece
            merged = piece if f == 0 else jnp.where(lane >= 32 * f, piece, merged)
        outer[j] = merged
    loaded(6, 7, 8, 9, 10)

    def step(t, carry):
        def scalar(table, bb, m):
            return middle_ref[t, 32 * table + 4 * bb + m]

        window = [outer[2 * t + m] for m in range(5)]
        values = [w[0:SLAB] for w in window]
        slopes = [w[SLAB:2 * SLAB] for w in window]

        def middle_sum(table, parts, bb):
            e = bb // 4
            out = scalar(table, bb, 0) * parts[e]
            for m in range(1, 4):
                out = out + scalar(table, bb, m) * parts[e + m]
            return out

        across = [middle_sum(0, slopes, bb) for bb in range(8)] + [middle_sum(1, values, bb) for bb in range(8)]
        along = [middle_sum(0, values, bb) for bb in range(8)]

        def pair_sides(x):
            lane = lanes_of(x.shape[0])
            high = x.astype(jnp.bfloat16)
            wide = high.astype(jnp.float32)
            low = x - wide
            turned = pltpu.roll(wide, 64, 1)
            even = jnp.where(lane < 64, low, turned).astype(jnp.bfloat16)
            odd = jnp.where(lane < 64, turned, low).astype(jnp.bfloat16)
            return jnp.concatenate([high, even], axis=1), jnp.concatenate([high, odd], axis=1)

        even, odd = pair_sides(jnp.concatenate(across, axis=0))
        across_even = product(even, inner_ref[0])
        across_odd = product(odd, inner_ref[1])
        even, odd = pair_sides(jnp.concatenate(along, axis=0))
        along_even = product(even, inner_ref[2])
        along_odd = product(odd, inner_ref[3])
        pvalue = product(odd, plain_ref[...])

        def weights(ref):
            lane = lanes_of(SLAB)
            tiles = [ref[:, pl.ds(pl.multiple_of(768 * t + 128 * n, 128), 128)] for n in range(6)]
            parts = []
            for bb in range(8):
                tile, shift = divmod(QUAD * bb, 128)
                part = tiles[tile]
                if shift + QUAD > 128:
                    part = jnp.where(lane >= shift, part, tiles[tile + 1])
                parts.append(pltpu.roll(part, 128 - shift, 1) if shift else part)
            return jnp.concatenate(parts, axis=0)

        s = weights(stiff)
        w = weights(volume)
        half = 8 * SLAB
        pressed = w * pvalue
        grads = [
            [across_even[0:half, 0:128], across_even[0:half, 128:256], across_odd[0:half, 0:128],
             across_odd[0:half, 128:256]],
            [across_even[half:, 0:128], across_even[half:, 128:256], across_odd[half:, 0:128],
             across_odd[half:, 128:256]],
            [along_even[:, 0:128], along_even[:, 128:256], along_odd[:, 0:128], along_odd[:, 128:256]],
        ]
        fluxes = []
        for d in range(3):
            fluxes.append([s * grads[d][f] - pressed if f == d else s * grads[d][f] for f in range(FIELDS)])
        spill = w * (grads[0][0] + grads[1][1] + grads[2][2])

        def adjoint(parts, table):
            pairs = [split(p) for p in parts]
            wide = product(jnp.concatenate([p[0] for p in pairs], axis=1), table[...])
            low = product(jnp.concatenate([p[1] for p in pairs], axis=1), table[:, 0:128])
            return wide[:, 0:128] + wide[:, 128:256] + low

        heads = [adjoint(fluxes[0], adj_value_ref), adjoint(fluxes[1], adj_value_ref),
                 adjoint(fluxes[2] + [spill], adj_slope_ref)]
        heads = [[h[SLAB * bb:SLAB * bb + SLAB] for bb in range(8)] for h in heads]
        sums = [[None, None] for _ in range(5)]
        for bb in range(8):
            for m in range(4):
                at = bb // 4 + m
                v = scalar(2, bb, m)
                terms = [v * heads[0][bb], scalar(3, bb, m) * heads[1][bb] + v * heads[2][bb]]
                sums[at] = [a if b is None else b + a for a, b in zip(terms, sums[at])]
        for m in range(5):
            total[2 * t + m] += jnp.concatenate(sums[m], axis=0)
        return carry

    lax.fori_loop(0, STEPS // 2, step, 0)
    finish_traces()
    high, low = split(trace_all[...].reshape(64, 384))
    both = (route + pltpu.roll(route, 64, 1)).astype(jnp.bfloat16)
    trace_out[...] = product(both, jnp.concatenate([high, low], axis=0)).reshape(8, 16, 384)
    start_picked()
    trace_in[group] = trace_out[group]
    finish_fixes()
    high, low = split(fix_all[...].reshape(128, 384))
    flipped = route.T.astype(jnp.bfloat16)[0:64]
    fix_out[...] = product(jnp.concatenate([flipped, flipped], axis=1),
                           jnp.concatenate([high, low], axis=0)).reshape(8, 8, 384)
    start_sums()
    fix_in[z] = fix_out[z]
    lax.fori_loop(STEPS // 2, STEPS, step, 0)

    last = last_ref[...]
    lane = lanes_of(16)
    packed = [[jnp.zeros((16, 128), jnp.float32) for _ in range(6)] for _ in range(FIELDS)]
    for j0 in range(0, BASIS, 2):
        some = list(range(j0, min(j0 + 2, BASIS)))
        columns = []
        for j in some:
            high, low = split(total[j])
            columns.append(jnp.concatenate([high, low, high], axis=0))
        result = product(last, jnp.concatenate(columns, axis=1))
        for n, j in enumerate(some):
            piece = result[:, 128 * n:128 * n + 128]
            tile, shift = divmod(BASIS * j, 128)
            for f in range(FIELDS):
                turn = (shift - 32 * f) % 128
                turned = pltpu.roll(piece, turn, 1) if turn else piece
                end = shift + BASIS
                mask = (lane >= shift) & (lane < end)
                packed[f][tile] = jnp.where(mask, turned, packed[f][tile])
                if end > 128:
                    packed[f][tile + 1] = jnp.where(lane < end - 128, turned, packed[f][tile + 1])
    for f in range(FIELDS):
        for n in range(6):
            back[f, :, 128 * n:128 * n + 128] = packed[f][n][0:8]
            back[f, n:n + 1, 768:896] = packed[f][n][8:9]
    going = [None]
    for d in range(1, SUBS):
        copy = pltpu.make_async_remote_copy(
            src_ref=back.at[peers[d]], dst_ref=home.at[me], send_sem=back_send_sem.at[d],
            recv_sem=back_recv_sem.at[d], device_id={"sub": peers[d]}, device_id_type=MESH)
        copy.start()
        going.append(copy)
    home[me] = back[me]
    finish_picked()
    picked = trace_in[0]
    for at in range(1, 8):
        picked = picked + trace_in[at]
    to_matrices([picked[8 * h:8 * h + 8, 128 * n:128 * n + 128] for h in range(2) for n in range(3)], grid)
    jumps = []
    for k in range(8):
        jump = exact(grid[pl.ds(k, BASIS, stride=8), :][:, 0:BASIS], rights[k], ((1,), (1,)))
        jumps.append(exact(lefts[k], jump, ((1,), (0,))))
    for slot in range(4):
        grid[pl.ds(slot, BASIS, stride=8), :] = jnp.concatenate(
            [jumps[slot] - jumps[4 + slot], jnp.zeros((BASIS, 128 - BASIS), jnp.float32)], axis=1)
    jump_rows = jnp.concatenate(to_rows(lambda i: grid[8 * i:8 * i + 8, :], 8), axis=1)
    for slot in range(4):
        jump_ref[slot, 0] = jump_rows[slot:slot + 1, 0:729]
    finish_sums()
    sums = fix_in[0]
    for at in range(1, 8):
        sums = sums + fix_in[at]
    sums = [sums[4 * h:4 * h + 4, 128 * n:128 * n + 128] for h in range(2) for n in range(3)]
    to_matrices(sums, grid)
    lane = lanes_of(BASIS)
    inside = lane < BASIS
    near = jnp.where(inside, grid[pl.ds(2, BASIS, stride=8), :], 0.0)
    far = jnp.where(inside, grid[pl.ds(3, BASIS, stride=8), :], 0.0)
    far = pltpu.roll(far, 62, 1)
    ends = jnp.concatenate(sums, axis=1)
    for d in range(1, SUBS):
        going[d].wait_send()
        pltpu.make_async_remote_copy(
            src_ref=back.at[peers[d]], dst_ref=home.at[origins[d]], send_sem=back_send_sem.at[d],
            recv_sem=back_recv_sem.at[d], device_id={"sub": peers[d]}, device_id_type=MESH).wait_recv()
    x_ref[...] = jnp.zeros((BASIS, BASIS * BASIS), jnp.float32)
    for q in range(SUBS):
        x_ref[6 * q:6 * q + 8, :] += home[q, :, 0:729]
        x_ref[6 * q + 8:6 * q + 9, :] += ninth_layer(home, q)[0:1, 0:729]
    for s in range(2):
        x_ref[26 * s:26 * s + 1, :] += ends[s:s + 1, 0:729]
    x_ref[:, 0:128] += near
    x_ref[:, 640:729] += far[:, 0:89]
    out_ref[0, 0, :, 0, :] = x_ref[...]


def per_device(state, stiff_weight, volume_weight, lagrange, mortar, links):
    vmem = pl.BlockSpec(memory_space=pltpu.VMEM)
    anywhere = pl.BlockSpec(memory_space=pl.ANY)
    constants = constant_tables()
    local = [x.shape[1:] if n < 2 else x.shape for n, x in enumerate(constants)]
    result, jumps = pl.pallas_call(
        operator_kernel,
        name="operator",
        out_shape=(jax.ShapeDtypeStruct((1, 1, BASIS, 1, BASIS * BASIS), jnp.float32),
                   jax.ShapeDtypeStruct(lagrange.shape, jnp.float32)),
        in_specs=[anywhere] * 13,
        out_specs=(vmem, vmem),
        scratch_shapes=[
            pltpu.VMEM((BASIS, BASIS * BASIS), jnp.float32),
            pltpu.VMEM(lagrange.shape, jnp.float32),
            pltpu.VMEM(mortar.shape, jnp.float32),
            pltpu.VMEM((6, 256), jnp.int32),
            pltpu.SMEM((6, 256), jnp.int32),
            *[pltpu.VMEM(shape, jnp.bfloat16) for shape in local[:-1]],
            pltpu.SMEM(local[-1], jnp.float32),
            pltpu.VMEM((SLAB, QUAD * QUAD), jnp.float32),
            pltpu.VMEM((SLAB, QUAD * QUAD), jnp.float32),
            pltpu.VMEM((SUBS, 8, 896), jnp.float32),
            pltpu.VMEM((SUBS, 8, 896), jnp.float32),
            pltpu.VMEM((SUBS, 8, 896), jnp.float32),
            pltpu.VMEM((SUBS, 8, 896), jnp.float32),
            pltpu.VMEM((BASIS, 2 * SLAB, 128), jnp.float32),
            pltpu.VMEM((BASIS, 2 * SLAB, 128), jnp.float32),
            pltpu.VMEM((BASIS * 8, 128), jnp.float32),
            pltpu.VMEM((8, 384), jnp.float32),
            pltpu.VMEM((8, 8, 384), jnp.float32),
            pltpu.VMEM((8, 16, 384), jnp.float32),
            pltpu.VMEM((8, 16, 384), jnp.float32),
            pltpu.VMEM((16, 384), jnp.float32),
            pltpu.VMEM((8, 16, 384), jnp.float32),
            pltpu.VMEM((8, 8, 384), jnp.float32),
            pltpu.VMEM((8, 8, 384), jnp.float32),
            pltpu.SemaphoreType.DMA((11,)),
            pltpu.SemaphoreType.DMA((SUBS,)),
            pltpu.SemaphoreType.DMA((SUBS,)),
            pltpu.SemaphoreType.DMA((SUBS,)),
            pltpu.SemaphoreType.DMA((SUBS,)),
            pltpu.SemaphoreType.DMA((4, 8)),
            pltpu.SemaphoreType.DMA((4, 8)),
        ],
        compiler_params=pltpu.CompilerParams(collective_id=0, has_side_effects=True),
        cost_estimate=pl.CostEstimate(flops=10**10, bytes_accessed=4 * 10**6, transcendentals=0),
    )(jnp.transpose(state, (0, 1, 3, 2, 4)), stiff_weight, volume_weight, lagrange,
      jnp.transpose(mortar, (0, 1, 3, 2, 4)), links.T, *constants)
    return jnp.transpose(result, (0, 1, 3, 2, 4)), jumps


def solution(mesh):
    return jax.shard_map(
        per_device,
        mesh=mesh,
        in_specs=(
            P("patch", "sub", None, None, None),
            P("patch", None, None),
            P("patch", None, None),
            P("patch", "sub", None, None),
            P("patch", None, None, None, None),
            P(),
        ),
        out_specs=(P("patch", "sub", None, None, None), P("patch", "sub", None, None)),
        check_vma=False,
    )
```

```python
import jax
import jax.numpy as jnp
import numpy as np
from jax import lax
from jax.experimental import pallas as pl
from jax.experimental.pallas import tpu as pltpu
from jax.sharding import PartitionSpec as P

ELEMS = 24
DEGREE = 3
FIELDS = 4
BASIS = 27
QUAD = 96
SUBS = 4
SLAB = QUAD // SUBS
LAYERS = SLAB // 4 + DEGREE
STEPS = 12
MESH = pl.DeviceIdType.MESH

stabilize = 0.25
highest = lax.Precision.HIGHEST
gauss_points_four = [
    -0.8611363115940526,
    -0.3399810435848563,
    0.3399810435848563,
    0.8611363115940526,
]
gauss_weights_four = [
    0.3478548451374538,
    0.6521451548625461,
    0.6521451548625461,
    0.3478548451374538,
]


def spline_tables(elements, degree):
    knot_list = np.concatenate(
        [np.zeros(degree), np.arange(elements + 1.0), np.full(degree, float(elements))]
    )
    gauss_nodes = np.array(gauss_points_four)
    gauss_weights = np.array(gauss_weights_four)
    points = (np.arange(elements)[:, None] + (gauss_nodes[None, :] + 1.0) / 2.0).reshape(-1)
    point_weights = np.tile(gauss_weights / 2.0, elements)
    current = np.where(
        (knot_list[None, :-1] <= points[:, None]) & (points[:, None] < knot_list[None, 1:]),
        1.0,
        0.0,
    )
    previous = current
    for order_k in range(1, degree + 1):
        previous = current
        amount = len(knot_list) - 1 - order_k
        current = np.zeros((points.shape[0], amount))
        for column in range(amount):
            left_span = knot_list[column + order_k] - knot_list[column]
            right_span = knot_list[column + order_k + 1] - knot_list[column + 1]
            if left_span > 0:
                current[:, column] += (points - knot_list[column]) / left_span * previous[:, column]
            if right_span > 0:
                current[:, column] += (
                    (knot_list[column + order_k + 1] - points)
                    / right_span
                    * previous[:, column + 1]
                )
    slope_part = np.zeros(current.shape)
    for column in range(current.shape[1]):
        left_span = knot_list[column + degree] - knot_list[column]
        right_span = knot_list[column + degree + 1] - knot_list[column + 1]
        if left_span > 0:
            slope_part[:, column] += degree / left_span * previous[:, column]
        if right_span > 0:
            slope_part[:, column] -= degree / right_span * previous[:, column + 1]
    return (
        current.astype(np.float32),
        slope_part.astype(np.float32),
        (current * point_weights[:, None]).astype(np.float32),
        (slope_part * point_weights[:, None]).astype(np.float32),
    )


def halves(table):
    high = table.astype(jnp.bfloat16).astype(np.float32)
    low = (table - high).astype(jnp.bfloat16).astype(np.float32)
    return high, low


def constant_tables():
    value, slope, value_w, slope_w = spline_tables(ELEMS, DEGREE)
    first = np.zeros((SUBS, 2 * SLAB, 16), np.float32)
    last = np.zeros((SUBS, 16, 2 * SLAB), np.float32)
    for q in range(SUBS):
        rows = slice(SLAB * q, SLAB * (q + 1))
        cols = slice(6 * q, 6 * q + LAYERS)
        first[q, :SLAB, :LAYERS] = value[rows, cols]
        first[q, SLAB:, :LAYERS] = slope[rows, cols]
        last[q, :LAYERS, :SLAB] = slope_w[rows, cols].T
        last[q, :LAYERS, SLAB:] = value_w[rows, cols].T
    high, low = halves(first)
    first = np.concatenate([high, high, low], axis=2)
    high, low = halves(last)
    last = np.concatenate([high, high, low], axis=2)

    def pair_tables(table):
        high, low = halves(table)
        even = np.zeros((256, 256), np.float32)
        odd = np.zeros((256, 256), np.float32)
        for s in range(2):
            cols = slice(128 * s, 128 * s + QUAD)
            even[32 * s:32 * s + BASIS, cols] = high.T
            even[128 + 32 * s:128 + 32 * s + BASIS, cols] = high.T
            even[192 + 32 * s:192 + 32 * s + BASIS, cols] = low.T
            odd[64 + 32 * s:64 + 32 * s + BASIS, cols] = high.T
            odd[128 + 32 * s:128 + 32 * s + BASIS, cols] = low.T
            odd[192 + 32 * s:192 + 32 * s + BASIS, cols] = high.T
        return even, odd

    value_even, value_odd = pair_tables(value)
    slope_even, slope_odd = pair_tables(slope)
    inner = np.stack([value_even, value_odd, slope_even, slope_odd])
    plain = value_odd[:, 128:]

    def adjoint_table(table, spilled=None):
        high, low = halves(table)
        out = np.zeros((1024, 256), np.float32)
        for f in range(FIELDS):
            scale = -stabilize if f == FIELDS - 1 else 1.0
            rows = slice(128 * f, 128 * f + QUAD)
            out[rows, 32 * f:32 * f + BASIS] = scale * high
            out[rows, 128 + 32 * f:128 + 32 * f + BASIS] = scale * low
            out[512 + 128 * f:512 + 128 * f + QUAD, 32 * f:32 * f + BASIS] = scale * high
        if spilled is None:
            return out
        high, low = halves(spilled)
        more = np.zeros((256, 256), np.float32)
        more[:QUAD, 96:96 + BASIS] = -high
        more[:QUAD, 224:224 + BASIS] = -low
        more[128:128 + QUAD, 96:96 + BASIS] = -high
        return np.concatenate([out, more])

    adjoint_value = adjoint_table(value_w)
    adjoint_slope = adjoint_table(slope_w, value_w)
    middle = np.zeros((STEPS, 128), np.float32)
    for t in range(STEPS):
        for bb in range(8):
            point = 8 * t + bb
            for m in range(4):
                col = 2 * t + bb // 4 + m
                for n, table in enumerate((value, slope, value_w, slope_w)):
                    middle[t, 32 * n + 4 * bb + m] = table[point, col]
    half = lambda x: jnp.asarray(x, jnp.bfloat16)
    return (half(first), half(last), half(inner), half(plain), half(adjoint_value), half(adjoint_slope),
            jnp.asarray(middle, jnp.float32))


def split(x):
    high = x.astype(jnp.bfloat16)
    return high, (x - high.astype(jnp.float32)).astype(jnp.bfloat16)


def product(left, right):
    return jnp.dot(left, right, preferred_element_type=jnp.float32)


def lanes_of(rows):
    return lax.broadcasted_iota(jnp.int32, (rows, 128), 1)


def exact(left, right, dims):
    return lax.dot_general(left, right, (dims, ((), ())), precision=highest, preferred_element_type=jnp.float32)


def to_matrices(tiles, grid):
    for i in range(BASIS):
        tile, shift = divmod(BASIS * i, 128)
        piece = tiles[tile]
        if shift + BASIS > 128:
            piece = jnp.where(lanes_of(piece.shape[0]) >= shift, piece, tiles[tile + 1])
        grid[8 * i:8 * i + piece.shape[0], :] = pltpu.roll(piece, 128 - shift, 1) if shift else piece


def to_rows(row_of, count):
    lane = lanes_of(count)
    tiles = [jnp.zeros((count, 128), jnp.float32) for _ in range(6)]
    for i in range(BASIS):
        tile, shift = divmod(BASIS * i, 128)
        piece = row_of(i)
        piece = pltpu.roll(piece, shift, 1) if shift else piece
        end = shift + BASIS
        tiles[tile] = jnp.where((lane >= shift) & (lane < end), piece, tiles[tile])
        if end > 128:
            tiles[tile + 1] = jnp.where(lane < end - 128, piece, tiles[tile + 1])
    return tiles


def ninth_layer(ref, at):
    first = lax.broadcasted_iota(jnp.int32, (8, 768), 0) == 0
    line = jnp.concatenate([ref[at, n:n + 1, 768:896] for n in range(6)], axis=1)
    return jnp.where(first, line, 0.0)


def routing(links_ref, y, z, core):
    row = lax.broadcasted_iota(jnp.int32, (128, 256), 0)
    col = lax.broadcasted_iota(jnp.int32, (128, 256), 1)
    source = ((row // 32) * 16 + 2 * z + (row // 16) % 2) * 4 + row % 4
    order = jnp.where(col == source, 1.0, 0.0).astype(jnp.bfloat16)
    table = links_ref[...].astype(jnp.float32).astype(jnp.bfloat16)
    found = lax.dot_general(order, table, (((1,), (1,)), ((), ())), preferred_element_type=jnp.float32)
    row = lax.broadcasted_iota(jnp.int32, (128, 1), 0)
    second = (row // 4) % 2 == 1
    patch = jnp.where(second, found[:, 1:2], found[:, 0:1])
    face = jnp.where(second, found[:, 3:4], found[:, 2:3])
    patch = jnp.where(found[:, 4:5] > 0.0, patch, -1.0)
    lane = lanes_of(128)
    row = lax.broadcasted_iota(jnp.int32, (128, 128), 0)
    wanted = (16 * y + 2 * (lane // 8) + core).astype(jnp.float32)
    same = (patch == wanted) & (face == (lane % 4).astype(jnp.float32))
    same = same & ((lane // 4) % 2 == (row // 8) % 2) & (lane < 64)
    return jnp.where(same, 1.0, 0.0)


def masked_mortar(mortar_ref, counts_ref, patch):
    row = lax.broadcasted_iota(jnp.int32, (BASIS, BASIS), 0)
    lefts, rights = [], []
    for s in range(2):
        for slot in range(4):
            at = 4 * patch + slot
            lefts.append(jnp.where(row < counts_ref[4, at], mortar_ref[slot, s, :, 0, :], 0.0))
            rights.append(jnp.where(row < counts_ref[5, at], mortar_ref[slot, s, :, 1, :], 0.0))
    return lefts, rights


def spread_kernel(x_in, lagrange_ref, mortar_ref, links_ref, counts_ref, stiff_hbm, volume_hbm, got_out, trace_own,
                  fix_own, route_out, stiff, volume, x_ref, sent, got, grid, load_sem, send_sem, recv_sem):
    me = lax.axis_index("sub")
    rows = pl.ds(pl.multiple_of(me * SLAB, 8), SLAB)
    patch = lax.axis_index("patch")
    y, z, core = patch // 16, (patch // 2) % 8, patch % 2
    peers = [lax.rem(me + d, SUBS) for d in range(SUBS)]
    origins = [lax.rem(me + SUBS - d, SUBS) for d in range(SUBS)]
    barrier = pltpu.get_barrier_semaphore()
    for d in range(1, SUBS):
        pl.semaphore_signal(barrier, inc=1, device_id={"sub": peers[d]}, device_id_type=MESH)
    loads = [pltpu.make_async_copy(stiff_hbm.at[0, rows], stiff, load_sem.at[0]),
             pltpu.make_async_copy(volume_hbm.at[0, rows], volume, load_sem.at[1])]
    for copy in loads:
        copy.start()
    x_ref[...] = x_in[0, 0, :, 0, :]
    sent[...] = jnp.zeros_like(sent)
    for q in range(SUBS):
        sent[q, :, 0:729] = x_ref[6 * q:6 * q + 8, :]
        for n in range(6):
            width = min(128, 729 - 128 * n)
            sent[q, n:n + 1, 768:768 + width] = x_ref[6 * q + 8:6 * q + 9, 128 * n:128 * n + width]
    pl.semaphore_wait(barrier, SUBS - 1)
    going = [None]
    for d in range(1, SUBS):
        copy = pltpu.make_async_remote_copy(
            src_ref=sent.at[peers[d]], dst_ref=got.at[me], send_sem=send_sem.at[d], recv_sem=recv_sem.at[d],
            device_id={"sub": peers[d]}, device_id_type=MESH)
        copy.start()
        going.append(copy)
    got[me] = sent[me]
    trace_rows = [[x_ref[26 * s:26 * s + 1, 128 * n:min(128 * n + 128, 729)] for n in range(6)] for s in range(2)]
    for s in range(2):
        tail = jnp.zeros((1, 768 - 729), jnp.float32)
        trace_rows[s][5] = jnp.concatenate([trace_rows[s][5], tail], axis=1)
    edge = x_ref[:, 0:128]
    trace_rows.append(to_rows(lambda i: edge[i:i + 1, :], 1))
    edge = jnp.concatenate([x_ref[:, 640:729], jnp.zeros((BASIS, 39), jnp.float32)], axis=1)
    edge = pltpu.roll(edge, 128 - 62, 1)
    trace_rows.append(to_rows(lambda i: edge[i:i + 1, :], 1))
    for h in range(2):
        for f in range(4):
            for n in range(3):
                trace_own[4 * h + f:4 * h + f + 1, 128 * n:128 * n + 128] = trace_rows[f][3 * h + n]
    lefts, rights = masked_mortar(mortar_ref, counts_ref, patch)
    multipliers = jnp.concatenate([lagrange_ref[slot, 0] for slot in range(4)], axis=0)
    multipliers = jnp.concatenate([multipliers, jnp.zeros((4, 768 - 729), jnp.float32)], axis=1)
    to_matrices([multipliers[:, 128 * n:128 * n + 128] for n in range(6)], grid)
    given = [grid[pl.ds(slot, BASIS, stride=8), :][:, 0:BASIS] for slot in range(4)]
    for k in range(8):
        fix = exact(given[k % 4], rights[k], ((1,), (0,)))
        fix = exact(lefts[k], fix, ((0,), (0,)))
        fix = fix if k < 4 else -fix
        grid[pl.ds(k, BASIS, stride=8), :] = jnp.concatenate(
            [fix, jnp.zeros((BASIS, 128 - BASIS), jnp.float32)], axis=1)
    fix_rows = to_rows(lambda i: grid[8 * i:8 * i + 8, :], 8)
    for h in range(2):
        for n in range(3):
            fix_own[8 * h:8 * h + 8, 128 * n:128 * n + 128] = fix_rows[3 * h + n]
    route_out[...] = routing(links_ref, y, z, core)
    for d in range(1, SUBS):
        going[d].wait_send()
        pltpu.make_async_remote_copy(
            src_ref=sent.at[peers[d]], dst_ref=got.at[origins[d]], send_sem=send_sem.at[d],
            recv_sem=recv_sem.at[d], device_id={"sub": peers[d]}, device_id_type=MESH).wait_recv()

    got_out[...] = got[...]
    for copy in loads:
        copy.wait()


def operator_kernel(got, stiff, volume, mortar_ref, counts_ref, trace_own, fix_own, route_ref, first_ref, last_ref,
                    inner_ref, plain_ref, adj_value_ref, adj_slope_ref, middle_hbm, out_ref, jump_ref, x_ref,
                    middle_ref, back, home, outer, total, grid, trace_all, trace_out, trace_in, fix_all, fix_out,
                    fix_in, load_sem, back_send_sem, back_recv_sem, face_send_sem, face_recv_sem):
    load_middle = pltpu.make_async_copy(middle_hbm, middle_ref, load_sem)
    load_middle.start()
    me = lax.axis_index("sub")
    patch = lax.axis_index("patch")
    y, z, core = patch // 16, (patch // 2) % 8, patch % 2
    group = 2 * y + core
    line = [lax.rem(z + d, 8) for d in range(8)]
    line_from = [lax.rem(z + 8 - d, 8) for d in range(8)]
    plane = [lax.rem(group + d, 8) for d in range(8)]
    plane_from = [lax.rem(group + 8 - d, 8) for d in range(8)]
    line_ids = [{"patch": 16 * y + 2 * at + core} for at in line]
    plane_ids = [{"patch": 16 * (at // 2) + 2 * z + at % 2} for at in plane]

    def exchange(n, source, target, slot, slots_from, ids):
        def one(d, at):
            return pltpu.make_async_remote_copy(
                src_ref=source(d), dst_ref=target.at[at], send_sem=face_send_sem.at[n, d],
                recv_sem=face_recv_sem.at[n, d], device_id=ids[d], device_id_type=MESH)

        def start():
            for d in range(1, 8):
                one(d, slot).start()

        def finish():
            for d in range(1, 8):
                one(d, slot).wait_send()
                one(d, slots_from[d]).wait_recv()

        return start, finish

    peers = [lax.rem(me + d, SUBS) for d in range(SUBS)]
    origins = [lax.rem(me + SUBS - d, SUBS) for d in range(SUBS)]
    barrier = pltpu.get_barrier_semaphore()
    for d in range(1, SUBS):
        pl.semaphore_signal(barrier, inc=1, device_id={"sub": peers[d]}, device_id_type=MESH)
    for d in range(1, 8):
        for ids in (line_ids, plane_ids):
            pl.semaphore_signal(barrier, inc=1, device_id=ids[d], device_id_type=MESH)
    start_traces, finish_traces = exchange(0, lambda d: trace_own, trace_all, z, line_from, line_ids)
    start_picked, finish_picked = exchange(1, lambda d: trace_out.at[plane[d]], trace_in, group, plane_from, plane_ids)
    start_fixes, finish_fixes = exchange(2, lambda d: fix_own, fix_all, group, plane_from, plane_ids)
    start_sums, finish_sums = exchange(3, lambda d: fix_out.at[line[d]], fix_in, z, line_from, line_ids)
    total[...] = jnp.zeros_like(total)
    first = first_ref[me]
    slabs = [jnp.concatenate([got[f, :, 0:768], ninth_layer(got, f)], axis=0) for f in range(FIELDS)]
    lane = lanes_of(16)
    columns = []
    for j in range(BASIS):
        tile, shift = divmod(BASIS * j, 128)
        merged = None
        for f in range(FIELDS):
            piece = slabs[f][:, 128 * tile:128 * tile + 128]
            if shift + BASIS > 128:
                piece = jnp.where(lane >= shift, piece, slabs[f][:, 128 * tile + 128:128 * tile + 256])
            turn = (32 * f - shift) % 128
            piece = pltpu.roll(piece, turn, 1) if turn else piece
            merged = piece if f == 0 else jnp.where(lane >= 32 * f, piece, merged)
        high, low = split(merged)
        columns.append(jnp.concatenate([high, low, high], axis=0))
    for j in range(0, BASIS, 2):
        result = product(first, jnp.concatenate(columns[j:j + 2], axis=1))
        for n in range(min(2, BASIS - j)):
            outer[j + n] = result[:, 128 * n:128 * n + 128]
    load_middle.wait()

    def step(t, carry):
        def scalar(table, bb, m):
            return middle_ref[t, 32 * table + 4 * bb + m]

        window = [outer[2 * t + m] for m in range(5)]
        values = [w[0:SLAB] for w in window]
        slopes = [w[SLAB:2 * SLAB] for w in window]

        def middle_sum(table, parts, bb):
            e = bb // 4
            out = scalar(table, bb, 0) * parts[e]
            for m in range(1, 4):
                out = out + scalar(table, bb, m) * parts[e + m]
            return out

        def pair_sides(x):
            lane = lanes_of(x.shape[0])
            high = x.astype(jnp.bfloat16)
            wide = high.astype(jnp.float32)
            low = x - wide
            turned = pltpu.roll(wide, 64, 1)
            even = jnp.where(lane < 64, low, turned).astype(jnp.bfloat16)
            odd = jnp.where(lane < 64, turned, low).astype(jnp.bfloat16)
            return jnp.concatenate([high, even], axis=1), jnp.concatenate([high, odd], axis=1)

        def weights(ref):
            lane = lanes_of(SLAB)
            tiles = [ref[:, pl.ds(pl.multiple_of(768 * t + 128 * n, 128), 128)] for n in range(6)]
            parts = []
            for bb in range(8):
                tile, shift = divmod(QUAD * bb, 128)
                part = tiles[tile]
                if shift + QUAD > 128:
                    part = jnp.where(lane >= shift, part, tiles[tile + 1])
                parts.append(pltpu.roll(part, 128 - shift, 1) if shift else part)
            return jnp.concatenate(parts, axis=0)

        s = weights(stiff)
        w = weights(volume)
        def adjoint(parts, table):
            pairs = [split(p) for p in parts]
            sides = [p[0] for p in pairs[:FIELDS]] + [p[1] for p in pairs[:FIELDS]]
            for pair in pairs[FIELDS:]:
                sides.extend(pair)
            wide = product(jnp.concatenate(sides, axis=1), table[...])
            return wide[:, 0:128] + wide[:, 128:256]

        def gradient(table, parts, at):
            even, odd = pair_sides(jnp.concatenate([middle_sum(table, parts, bb) for bb in range(8)], axis=0))
            first, second = product(even, inner_ref[at]), product(odd, inner_ref[at + 1])
            return [first[:, 0:128], first[:, 128:256], second[:, 0:128], second[:, 128:256]], odd

        along, odd = gradient(0, values, 2)
        pressed = w * product(odd, plain_ref[...])
        spill = along[2]
        heads = [None] * 3
        for d in range(2):
            grads, _ = gradient(d, values if d else slopes, 0)
            spill = spill + grads[d]
            heads[d] = adjoint([s * g - pressed if f == d else s * g for f, g in enumerate(grads)], adj_value_ref)
        heads[2] = adjoint([s * g - pressed if f == 2 else s * g for f, g in enumerate(along)] + [w * spill],
                           adj_slope_ref)
        heads = [[h[SLAB * bb:SLAB * bb + SLAB] for bb in range(8)] for h in heads]
        sums = [[None, None] for _ in range(5)]
        for bb in range(8):
            for m in range(4):
                at = bb // 4 + m
                v = scalar(2, bb, m)
                terms = [v * heads[0][bb], scalar(3, bb, m) * heads[1][bb] + v * heads[2][bb]]
                sums[at] = [a if b is None else b + a for a, b in zip(terms, sums[at])]
        for m in range(5):
            total[2 * t + m] += jnp.concatenate(sums[m], axis=0)
        return carry

    lax.fori_loop(0, STEPS // 2, step, 0, unroll=2)
    pl.semaphore_wait(barrier, SUBS - 1 + 14)
    start_traces()
    trace_all[z] = trace_own[...]
    start_fixes()
    fix_all[group] = fix_own[...]
    lax.fori_loop(STEPS // 2, STEPS - 2, step, 0, unroll=2)
    finish_traces()
    high, low = split(trace_all[...].reshape(64, 384))
    both = (route_ref[...] + pltpu.roll(route_ref[...], 64, 1)).astype(jnp.bfloat16)
    trace_out[...] = product(both, jnp.concatenate([high, low], axis=0)).reshape(8, 16, 384)
    start_picked()
    trace_in[group] = trace_out[group]
    finish_fixes()
    high, low = split(fix_all[...].reshape(128, 384))
    flipped = route_ref[...].T.astype(jnp.bfloat16)[0:64]
    fix_out[...] = product(jnp.concatenate([flipped, flipped], axis=1),
                           jnp.concatenate([high, low], axis=0)).reshape(8, 8, 384)
    start_sums()
    fix_in[z] = fix_out[z]
    lax.fori_loop(STEPS - 2, STEPS, step, 0, unroll=2)

    last = last_ref[me]
    lane = lanes_of(16)
    packed = [[jnp.zeros((16, 128), jnp.float32) for _ in range(6)] for _ in range(FIELDS)]
    for j0 in range(0, BASIS, 2):
        some = list(range(j0, min(j0 + 2, BASIS)))
        columns = []
        for j in some:
            high, low = split(total[j])
            columns.append(jnp.concatenate([high, low, high], axis=0))
        result = product(last, jnp.concatenate(columns, axis=1))
        for n, j in enumerate(some):
            piece = result[:, 128 * n:128 * n + 128]
            tile, shift = divmod(BASIS * j, 128)
            for f in range(FIELDS):
                turn = (shift - 32 * f) % 128
                turned = pltpu.roll(piece, turn, 1) if turn else piece
                end = shift + BASIS
                mask = (lane >= shift) & (lane < end)
                packed[f][tile] = jnp.where(mask, turned, packed[f][tile])
                if end > 128:
                    packed[f][tile + 1] = jnp.where(lane < end - 128, turned, packed[f][tile + 1])
    for f in range(FIELDS):
        for n in range(6):
            back[f, :, 128 * n:128 * n + 128] = packed[f][n][0:8]
            back[f, n:n + 1, 768:896] = packed[f][n][8:9]
    going = [None]
    for d in range(1, SUBS):
        copy = pltpu.make_async_remote_copy(
            src_ref=back.at[peers[d]], dst_ref=home.at[me], send_sem=back_send_sem.at[d],
            recv_sem=back_recv_sem.at[d], device_id={"sub": peers[d]}, device_id_type=MESH)
        copy.start()
        going.append(copy)
    home[me] = back[me]
    finish_picked()
    picked = trace_in[0]
    for at in range(1, 8):
        picked = picked + trace_in[at]
    to_matrices([picked[8 * h:8 * h + 8, 128 * n:128 * n + 128] for h in range(2) for n in range(3)], grid)
    lefts, rights = masked_mortar(mortar_ref, counts_ref, patch)
    jumps = []
    for k in range(8):
        jump = exact(grid[pl.ds(k, BASIS, stride=8), :][:, 0:BASIS], rights[k], ((1,), (1,)))
        jumps.append(exact(lefts[k], jump, ((1,), (0,))))
    for slot in range(4):
        grid[pl.ds(slot, BASIS, stride=8), :] = jnp.concatenate(
            [jumps[slot] - jumps[4 + slot], jnp.zeros((BASIS, 128 - BASIS), jnp.float32)], axis=1)
    jump_rows = jnp.concatenate(to_rows(lambda i: grid[8 * i:8 * i + 8, :], 8), axis=1)
    for slot in range(4):
        jump_ref[slot, 0] = jump_rows[slot:slot + 1, 0:729]
    finish_sums()
    sums = fix_in[0]
    for at in range(1, 8):
        sums = sums + fix_in[at]
    sums = [sums[4 * h:4 * h + 4, 128 * n:128 * n + 128] for h in range(2) for n in range(3)]
    to_matrices(sums, grid)
    lane = lanes_of(BASIS)
    inside = lane < BASIS
    near = jnp.where(inside, grid[pl.ds(2, BASIS, stride=8), :], 0.0)
    far = jnp.where(inside, grid[pl.ds(3, BASIS, stride=8), :], 0.0)
    far = pltpu.roll(far, 62, 1)
    ends = jnp.concatenate(sums, axis=1)
    for d in range(1, SUBS):
        going[d].wait_send()
        pltpu.make_async_remote_copy(
            src_ref=back.at[peers[d]], dst_ref=home.at[origins[d]], send_sem=back_send_sem.at[d],
            recv_sem=back_recv_sem.at[d], device_id={"sub": peers[d]}, device_id_type=MESH).wait_recv()
    x_ref[...] = jnp.zeros((BASIS, BASIS * BASIS), jnp.float32)
    for q in range(SUBS):
        x_ref[6 * q:6 * q + 8, :] += home[q, :, 0:729]
        x_ref[6 * q + 8:6 * q + 9, :] += ninth_layer(home, q)[0:1, 0:729]
    for s in range(2):
        x_ref[26 * s:26 * s + 1, :] += ends[s:s + 1, 0:729]
    x_ref[:, 0:128] += near
    x_ref[:, 640:729] += far[:, 0:89]
    out_ref[0, 0, :, 0, :] = x_ref[...]


def per_device(state, stiff_weight, volume_weight, lagrange, mortar, links):
    vmem = pl.BlockSpec(memory_space=pltpu.VMEM)
    anywhere = pl.BlockSpec(memory_space=pl.ANY)
    smem = pl.BlockSpec(memory_space=pltpu.SMEM)
    f32 = lambda *shape: jax.ShapeDtypeStruct(shape, jnp.float32)
    constants = constant_tables()
    mortar = jnp.transpose(mortar, (0, 1, 3, 2, 4))
    links = links.T
    spread = pl.pallas_call(
        spread_kernel,
        name="spread",
        out_shape=(f32(SUBS, 8, 896), f32(8, 384), f32(16, 384), f32(128, 128),
                   f32(SLAB, QUAD * QUAD), f32(SLAB, QUAD * QUAD)),
        in_specs=[vmem, vmem, vmem, vmem, smem, anywhere, anywhere],
        out_specs=(vmem,) * 6,
        scratch_shapes=[
            pltpu.VMEM((BASIS, BASIS * BASIS), jnp.float32),
            pltpu.VMEM((SUBS, 8, 896), jnp.float32),
            pltpu.VMEM((SUBS, 8, 896), jnp.float32),
            pltpu.VMEM((BASIS * 8, 128), jnp.float32),
            pltpu.SemaphoreType.DMA((2,)),
            pltpu.SemaphoreType.DMA((SUBS,)),
            pltpu.SemaphoreType.DMA((SUBS,)),
        ],
        compiler_params=pltpu.CompilerParams(collective_id=0, has_side_effects=True, vmem_limit_bytes=52 * 10**6),
        cost_estimate=pl.CostEstimate(flops=10**9, bytes_accessed=10**5, transcendentals=0),
    )(jnp.transpose(state, (0, 1, 3, 2, 4)), lagrange, mortar, links, links,
      stiff_weight, volume_weight)
    result, jumps = pl.pallas_call(
        operator_kernel,
        name="operator",
        out_shape=(f32(1, 1, BASIS, 1, BASIS * BASIS), f32(*lagrange.shape)),
        in_specs=[vmem] * 4 + [smem] + [vmem] * 9 + [anywhere],
        out_specs=(vmem, vmem),
        scratch_shapes=[
            pltpu.VMEM((BASIS, BASIS * BASIS), jnp.float32),
            pltpu.SMEM(constants[-1].shape, jnp.float32),
            pltpu.VMEM((SUBS, 8, 896), jnp.float32),
            pltpu.VMEM((SUBS, 8, 896), jnp.float32),
            pltpu.VMEM((BASIS, 2 * SLAB, 128), jnp.float32),
            pltpu.VMEM((BASIS, 2 * SLAB, 128), jnp.float32),
            pltpu.VMEM((BASIS * 8, 128), jnp.float32),
            pltpu.VMEM((8, 8, 384), jnp.float32),
            pltpu.VMEM((8, 16, 384), jnp.float32),
            pltpu.VMEM((8, 16, 384), jnp.float32),
            pltpu.VMEM((8, 16, 384), jnp.float32),
            pltpu.VMEM((8, 8, 384), jnp.float32),
            pltpu.VMEM((8, 8, 384), jnp.float32),
            pltpu.SemaphoreType.DMA,
            pltpu.SemaphoreType.DMA((SUBS,)),
            pltpu.SemaphoreType.DMA((SUBS,)),
            pltpu.SemaphoreType.DMA((4, 8)),
            pltpu.SemaphoreType.DMA((4, 8)),
        ],
        compiler_params=pltpu.CompilerParams(collective_id=1, has_side_effects=True, vmem_limit_bytes=52 * 10**6),
        cost_estimate=pl.CostEstimate(flops=10**10, bytes_accessed=4 * 10**6, transcendentals=0),
    )(spread[0], *spread[4:], mortar, links, *spread[1:4], *constants)
    return jnp.transpose(result, (0, 1, 3, 2, 4)), jumps


def solution(mesh):
    return jax.shard_map(
        per_device,
        mesh=mesh,
        in_specs=(
            P("patch", "sub", None, None, None),
            P("patch", None, None),
            P("patch", None, None),
            P("patch", "sub", None, None),
            P("patch", None, None, None, None),
            P(),
        ),
        out_specs=(P("patch", "sub", None, None, None), P("patch", "sub", None, None)),
        check_vma=False,
    )
```

```python
import jax
import jax.numpy as jnp
import numpy as np
from jax import lax
from jax.experimental import pallas as pl
from jax.experimental.pallas import tpu as pltpu
from jax.sharding import PartitionSpec as P

ELEMS = 24
DEGREE = 3
FIELDS = 4
BASIS = 27
QUAD = 96
SUBS = 4
SLAB = QUAD // SUBS
LAYERS = SLAB // 4 + DEGREE
STEPS = 12
MESH = pl.DeviceIdType.MESH

stabilize = 0.25
highest = lax.Precision.HIGHEST
gauss_points_four = [
    -0.8611363115940526,
    -0.3399810435848563,
    0.3399810435848563,
    0.8611363115940526,
]
gauss_weights_four = [
    0.3478548451374538,
    0.6521451548625461,
    0.6521451548625461,
    0.3478548451374538,
]


def spline_tables(elements, degree):
    knot_list = np.concatenate(
        [np.zeros(degree), np.arange(elements + 1.0), np.full(degree, float(elements))]
    )
    gauss_nodes = np.array(gauss_points_four)
    gauss_weights = np.array(gauss_weights_four)
    points = (np.arange(elements)[:, None] + (gauss_nodes[None, :] + 1.0) / 2.0).reshape(-1)
    point_weights = np.tile(gauss_weights / 2.0, elements)
    current = np.where(
        (knot_list[None, :-1] <= points[:, None]) & (points[:, None] < knot_list[None, 1:]),
        1.0,
        0.0,
    )
    previous = current
    for order_k in range(1, degree + 1):
        previous = current
        amount = len(knot_list) - 1 - order_k
        current = np.zeros((points.shape[0], amount))
        for column in range(amount):
            left_span = knot_list[column + order_k] - knot_list[column]
            right_span = knot_list[column + order_k + 1] - knot_list[column + 1]
            if left_span > 0:
                current[:, column] += (points - knot_list[column]) / left_span * previous[:, column]
            if right_span > 0:
                current[:, column] += (
                    (knot_list[column + order_k + 1] - points)
                    / right_span
                    * previous[:, column + 1]
                )
    slope_part = np.zeros(current.shape)
    for column in range(current.shape[1]):
        left_span = knot_list[column + degree] - knot_list[column]
        right_span = knot_list[column + degree + 1] - knot_list[column + 1]
        if left_span > 0:
            slope_part[:, column] += degree / left_span * previous[:, column]
        if right_span > 0:
            slope_part[:, column] -= degree / right_span * previous[:, column + 1]
    return (
        current.astype(np.float32),
        slope_part.astype(np.float32),
        (current * point_weights[:, None]).astype(np.float32),
        (slope_part * point_weights[:, None]).astype(np.float32),
    )


def halves(table):
    high = table.astype(jnp.bfloat16).astype(np.float32)
    low = (table - high).astype(jnp.bfloat16).astype(np.float32)
    return high, low


def constant_tables():
    value, slope, value_w, slope_w = spline_tables(ELEMS, DEGREE)
    first = np.zeros((SUBS, 2 * SLAB, 16), np.float32)
    last = np.zeros((SUBS, 16, 2 * SLAB), np.float32)
    for q in range(SUBS):
        rows = slice(SLAB * q, SLAB * (q + 1))
        cols = slice(6 * q, 6 * q + LAYERS)
        first[q, :SLAB, :LAYERS] = value[rows, cols]
        first[q, SLAB:, :LAYERS] = slope[rows, cols]
        last[q, :LAYERS, :SLAB] = slope_w[rows, cols].T
        last[q, :LAYERS, SLAB:] = value_w[rows, cols].T
    high, low = halves(first)
    first = np.concatenate([high, high, low], axis=2)
    high, low = halves(last)
    last = np.concatenate([high, high, low], axis=2)

    def pair_tables(table):
        high, low = halves(table)
        even = np.zeros((256, 256), np.float32)
        odd = np.zeros((256, 256), np.float32)
        for s in range(2):
            cols = slice(128 * s, 128 * s + QUAD)
            even[32 * s:32 * s + BASIS, cols] = high.T
            even[128 + 32 * s:128 + 32 * s + BASIS, cols] = high.T
            even[192 + 32 * s:192 + 32 * s + BASIS, cols] = low.T
            odd[64 + 32 * s:64 + 32 * s + BASIS, cols] = high.T
            odd[128 + 32 * s:128 + 32 * s + BASIS, cols] = low.T
            odd[192 + 32 * s:192 + 32 * s + BASIS, cols] = high.T
        return even, odd

    value_even, value_odd = pair_tables(value)
    slope_even, slope_odd = pair_tables(slope)
    inner = np.stack([value_even, value_odd, slope_even, slope_odd])
    plain = value_odd[:, 128:]

    def adjoint_table(table, spilled=None):
        high, low = halves(table)
        out = np.zeros((1024, 256), np.float32)
        for f in range(FIELDS):
            scale = -stabilize if f == FIELDS - 1 else 1.0
            rows = slice(128 * f, 128 * f + QUAD)
            out[rows, 32 * f:32 * f + BASIS] = scale * high
            out[rows, 128 + 32 * f:128 + 32 * f + BASIS] = scale * low
            out[512 + 128 * f:512 + 128 * f + QUAD, 32 * f:32 * f + BASIS] = scale * high
        if spilled is None:
            return out
        high, low = halves(spilled)
        more = np.zeros((256, 256), np.float32)
        more[:QUAD, 96:96 + BASIS] = -high
        more[:QUAD, 224:224 + BASIS] = -low
        more[128:128 + QUAD, 96:96 + BASIS] = -high
        return np.concatenate([out, more])

    adjoint_value = adjoint_table(value_w)
    adjoint_slope = adjoint_table(slope_w, value_w)
    middle = np.zeros((STEPS, 128), np.float32)
    for t in range(STEPS):
        for bb in range(8):
            point = 8 * t + bb
            for m in range(4):
                col = 2 * t + bb // 4 + m
                for n, table in enumerate((value, slope, value_w, slope_w)):
                    middle[t, 32 * n + 4 * bb + m] = table[point, col]
    half = lambda x: jnp.asarray(x, jnp.bfloat16)
    return (half(first), half(last), half(inner), half(plain), half(adjoint_value), half(adjoint_slope),
            jnp.asarray(middle, jnp.float32))


def split(x):
    high = x.astype(jnp.bfloat16)
    return high, (x - high.astype(jnp.float32)).astype(jnp.bfloat16)


def product(left, right):
    return jnp.dot(left, right, preferred_element_type=jnp.float32)


def lanes_of(rows):
    return lax.broadcasted_iota(jnp.int32, (rows, 128), 1)


def exact(left, right, dims):
    return lax.dot_general(left, right, (dims, ((), ())), precision=highest, preferred_element_type=jnp.float32)


def to_matrices(tiles, grid):
    for i in range(BASIS):
        tile, shift = divmod(BASIS * i, 128)
        piece = tiles[tile]
        if shift + BASIS > 128:
            piece = jnp.where(lanes_of(piece.shape[0]) >= shift, piece, tiles[tile + 1])
        grid[8 * i:8 * i + piece.shape[0], :] = pltpu.roll(piece, 128 - shift, 1) if shift else piece


def to_rows(row_of, count):
    lane = lanes_of(count)
    tiles = [jnp.zeros((count, 128), jnp.float32) for _ in range(6)]
    for i in range(BASIS):
        tile, shift = divmod(BASIS * i, 128)
        piece = row_of(i)
        piece = pltpu.roll(piece, shift, 1) if shift else piece
        end = shift + BASIS
        tiles[tile] = jnp.where((lane >= shift) & (lane < end), piece, tiles[tile])
        if end > 128:
            tiles[tile + 1] = jnp.where(lane < end - 128, piece, tiles[tile + 1])
    return tiles


def ninth_layer(ref, at):
    first = lax.broadcasted_iota(jnp.int32, (8, 768), 0) == 0
    line = jnp.concatenate([ref[at, n:n + 1, 768:896] for n in range(6)], axis=1)
    return jnp.where(first, line, 0.0)


def routing(links_ref, y, z, core):
    row = lax.broadcasted_iota(jnp.int32, (128, 256), 0)
    col = lax.broadcasted_iota(jnp.int32, (128, 256), 1)
    source = ((row // 32) * 16 + 2 * z + (row // 16) % 2) * 4 + row % 4
    order = jnp.where(col == source, 1.0, 0.0).astype(jnp.bfloat16)
    table = links_ref[...].astype(jnp.float32).astype(jnp.bfloat16)
    found = lax.dot_general(order, table, (((1,), (1,)), ((), ())), preferred_element_type=jnp.float32)
    row = lax.broadcasted_iota(jnp.int32, (128, 1), 0)
    second = (row // 4) % 2 == 1
    patch = jnp.where(second, found[:, 1:2], found[:, 0:1])
    face = jnp.where(second, found[:, 3:4], found[:, 2:3])
    patch = jnp.where(found[:, 4:5] > 0.0, patch, -1.0)
    lane = lanes_of(128)
    row = lax.broadcasted_iota(jnp.int32, (128, 128), 0)
    wanted = (16 * y + 2 * (lane // 8) + core).astype(jnp.float32)
    same = (patch == wanted) & (face == (lane % 4).astype(jnp.float32))
    same = same & ((lane // 4) % 2 == (row // 8) % 2) & (lane < 64)
    return jnp.where(same, 1.0, 0.0)


def operator_kernel(x_hbm, stiff_hbm, volume_hbm, lagrange_hbm, mortar_hbm, links_hbm, first_hbm, last_hbm,
                    inner_hbm, plain_hbm, adj_value_hbm, adj_slope_hbm, middle_hbm, out_ref, jump_ref,
                    x_ref, lagrange_ref, mortar_ref, links_ref, counts_ref, first_ref, last_ref, inner_ref,
                    plain_ref, adj_value_ref, adj_slope_ref, middle_ref, stiff, volume, sent, got, back, home, outer, total, grid, trace_own, trace_all,
                    trace_out, trace_in, fix_own, fix_all, fix_out, fix_in, load_sem, send_sem, recv_sem,
                    back_send_sem, back_recv_sem, face_send_sem, face_recv_sem):
    me = lax.axis_index("sub")
    patch = lax.axis_index("patch")
    y, z, core = patch // 16, (patch // 2) % 8, patch % 2
    group = 2 * y + core
    line = [lax.rem(z + d, 8) for d in range(8)]
    line_from = [lax.rem(z + 8 - d, 8) for d in range(8)]
    plane = [lax.rem(group + d, 8) for d in range(8)]
    plane_from = [lax.rem(group + 8 - d, 8) for d in range(8)]
    line_ids = [{"patch": 16 * y + 2 * at + core} for at in line]
    plane_ids = [{"patch": 16 * (at // 2) + 2 * z + at % 2} for at in plane]

    def exchange(n, source, target, slot, slots_from, ids):
        def one(d, at):
            return pltpu.make_async_remote_copy(
                src_ref=source(d), dst_ref=target.at[at], send_sem=face_send_sem.at[n, d],
                recv_sem=face_recv_sem.at[n, d], device_id=ids[d], device_id_type=MESH)

        def start():
            for d in range(1, 8):
                one(d, slot).start()

        def finish():
            for d in range(1, 8):
                one(d, slot).wait_send()
                one(d, slots_from[d]).wait_recv()

        return start, finish

    peers = [lax.rem(me + d, SUBS) for d in range(SUBS)]
    origins = [lax.rem(me + SUBS - d, SUBS) for d in range(SUBS)]
    barrier = pltpu.get_barrier_semaphore()
    for d in range(1, SUBS):
        pl.semaphore_signal(barrier, inc=1, device_id={"sub": peers[d]}, device_id_type=MESH)
    for d in range(1, 8):
        for ids in (line_ids, plane_ids):
            pl.semaphore_signal(barrier, inc=1, device_id=ids[d], device_id_type=MESH)
    rows = pl.ds(pl.multiple_of(me * SLAB, 8), SLAB)
    pairs = [(slot, s, n) for slot in range(4) for s in range(2) for n in range(2)]
    loads = [
        [(x_hbm.at[0, 0, :, 0, :], x_ref)],
        [(links_hbm, links_ref)],
        [(links_hbm, counts_ref)],
        [(lagrange_hbm, lagrange_ref)],
        [(mortar_hbm.at[slot, s, :, n, :], mortar_ref.at[slot, s, n]) for slot, s, n in pairs],
        [(first_hbm.at[me], first_ref)],
        [(middle_hbm, middle_ref)],
        [(inner_hbm, inner_ref), (plain_hbm, plain_ref)],
        [(stiff_hbm.at[0, rows], stiff), (volume_hbm.at[0, rows], volume)],
        [(adj_value_hbm, adj_value_ref), (adj_slope_hbm, adj_slope_ref)],
        [(last_hbm.at[me], last_ref)],
    ]
    loads = [[pltpu.make_async_copy(a, b, load_sem.at[n]) for a, b in some] for n, some in enumerate(loads)]
    for some in loads:
        for copy in some:
            copy.start()

    def loaded(*which):
        for n in which:
            for copy in loads[n]:
                copy.wait()

    loaded(0)
    sent[...] = jnp.zeros_like(sent)
    for q in range(SUBS):
        sent[q, :, 0:729] = x_ref[6 * q:6 * q + 8, :]
        for n in range(6):
            width = min(128, 729 - 128 * n)
            sent[q, n:n + 1, 768:768 + width] = x_ref[6 * q + 8:6 * q + 9, 128 * n:128 * n + width]
    trace_rows = [[x_ref[26 * s:26 * s + 1, 128 * n:min(128 * n + 128, 729)] for n in range(6)] for s in range(2)]
    for s in range(2):
        tail = jnp.zeros((1, 768 - 729), jnp.float32)
        trace_rows[s][5] = jnp.concatenate([trace_rows[s][5], tail], axis=1)
    edge = x_ref[:, 0:128]
    trace_rows.append(to_rows(lambda i: edge[i:i + 1, :], 1))
    edge = jnp.concatenate([x_ref[:, 640:729], jnp.zeros((BASIS, 39), jnp.float32)], axis=1)
    edge = pltpu.roll(edge, 128 - 62, 1)
    trace_rows.append(to_rows(lambda i: edge[i:i + 1, :], 1))
    for h in range(2):
        for f in range(4):
            for n in range(3):
                trace_own[4 * h + f:4 * h + f + 1, 128 * n:128 * n + 128] = trace_rows[f][3 * h + n]
    start_traces, finish_traces = exchange(0, lambda d: trace_own, trace_all, z, line_from, line_ids)
    start_picked, finish_picked = exchange(1, lambda d: trace_out.at[plane[d]], trace_in, group, plane_from, plane_ids)
    start_fixes, finish_fixes = exchange(2, lambda d: fix_own, fix_all, group, plane_from, plane_ids)
    start_sums, finish_sums = exchange(3, lambda d: fix_out.at[line[d]], fix_in, z, line_from, line_ids)
    pl.semaphore_wait(barrier, SUBS - 1 + 14)
    going = [None]
    for d in range(1, SUBS):
        copy = pltpu.make_async_remote_copy(
            src_ref=sent.at[peers[d]], dst_ref=got.at[me], send_sem=send_sem.at[d], recv_sem=recv_sem.at[d],
            device_id={"sub": peers[d]}, device_id_type=MESH)
        copy.start()
        going.append(copy)
    start_traces()
    trace_all[z] = trace_own[...]
    got[me] = sent[me]
    loaded(1, 2, 3, 4)
    row = lax.broadcasted_iota(jnp.int32, (BASIS, BASIS), 0)
    lefts, rights = [], []
    for s in range(2):
        for slot in range(4):
            at = 4 * patch + slot
            lefts.append(jnp.where(row < counts_ref[4, at], mortar_ref[slot, s, 0], 0.0))
            rights.append(jnp.where(row < counts_ref[5, at], mortar_ref[slot, s, 1], 0.0))
    multipliers = jnp.concatenate([lagrange_ref[slot, 0] for slot in range(4)], axis=0)
    multipliers = jnp.concatenate([multipliers, jnp.zeros((4, 768 - 729), jnp.float32)], axis=1)
    to_matrices([multipliers[:, 128 * n:128 * n + 128] for n in range(6)], grid)
    given = [grid[pl.ds(slot, BASIS, stride=8), :][:, 0:BASIS] for slot in range(4)]
    for k in range(8):
        fix = exact(given[k % 4], rights[k], ((1,), (0,)))
        fix = exact(lefts[k], fix, ((0,), (0,)))
        fix = fix if k < 4 else -fix
        grid[pl.ds(k, BASIS, stride=8), :] = jnp.concatenate(
            [fix, jnp.zeros((BASIS, 128 - BASIS), jnp.float32)], axis=1)
    fix_rows = to_rows(lambda i: grid[8 * i:8 * i + 8, :], 8)
    for h in range(2):
        for n in range(3):
            fix_own[8 * h:8 * h + 8, 128 * n:128 * n + 128] = fix_rows[3 * h + n]
    start_fixes()
    fix_all[group] = fix_own[...]
    route = routing(links_ref, y, z, core)
    total[...] = jnp.zeros_like(total)
    for d in range(1, SUBS):
        going[d].wait_send()
        pltpu.make_async_remote_copy(
            src_ref=sent.at[peers[d]], dst_ref=got.at[origins[d]], send_sem=send_sem.at[d],
            recv_sem=recv_sem.at[d], device_id={"sub": peers[d]}, device_id_type=MESH).wait_recv()

    loaded(5)
    first = first_ref[...]
    slabs = [jnp.concatenate([got[f, :, 0:768], ninth_layer(got, f)], axis=0) for f in range(FIELDS)]
    lane = lanes_of(16)
    columns = []
    for j in range(BASIS):
        tile, shift = divmod(BASIS * j, 128)
        merged = None
        for f in range(FIELDS):
            piece = slabs[f][:, 128 * tile:128 * tile + 128]
            if shift + BASIS > 128:
                piece = jnp.where(lane >= shift, piece, slabs[f][:, 128 * tile + 128:128 * tile + 256])
            turn = (32 * f - shift) % 128
            piece = pltpu.roll(piece, turn, 1) if turn else piece
            merged = piece if f == 0 else jnp.where(lane >= 32 * f, piece, merged)
        high, low = split(merged)
        columns.append(jnp.concatenate([high, low, high], axis=0))
    for j in range(0, BASIS, 2):
        result = product(first, jnp.concatenate(columns[j:j + 2], axis=1))
        for n in range(min(2, BASIS - j)):
            outer[j + n] = result[:, 128 * n:128 * n + 128]
    loaded(6, 7, 8, 9, 10)

    def step(t, carry):
        def scalar(table, bb, m):
            return middle_ref[t, 32 * table + 4 * bb + m]

        window = [outer[2 * t + m] for m in range(5)]
        values = [w[0:SLAB] for w in window]
        slopes = [w[SLAB:2 * SLAB] for w in window]

        def middle_sum(table, parts, bb):
            e = bb // 4
            out = scalar(table, bb, 0) * parts[e]
            for m in range(1, 4):
                out = out + scalar(table, bb, m) * parts[e + m]
            return out

        def pair_sides(x):
            lane = lanes_of(x.shape[0])
            high = x.astype(jnp.bfloat16)
            wide = high.astype(jnp.float32)
            low = x - wide
            turned = pltpu.roll(wide, 64, 1)
            even = jnp.where(lane < 64, low, turned).astype(jnp.bfloat16)
            odd = jnp.where(lane < 64, turned, low).astype(jnp.bfloat16)
            return jnp.concatenate([high, even], axis=1), jnp.concatenate([high, odd], axis=1)

        def weights(ref):
            lane = lanes_of(SLAB)
            tiles = [ref[:, pl.ds(pl.multiple_of(768 * t + 128 * n, 128), 128)] for n in range(6)]
            parts = []
            for bb in range(8):
                tile, shift = divmod(QUAD * bb, 128)
                part = tiles[tile]
                if shift + QUAD > 128:
                    part = jnp.where(lane >= shift, part, tiles[tile + 1])
                parts.append(pltpu.roll(part, 128 - shift, 1) if shift else part)
            return jnp.concatenate(parts, axis=0)

        s = weights(stiff)
        w = weights(volume)
        def adjoint(parts, table):
            pairs = [split(p) for p in parts]
            sides = [p[0] for p in pairs[:FIELDS]] + [p[1] for p in pairs[:FIELDS]]
            for pair in pairs[FIELDS:]:
                sides.extend(pair)
            wide = product(jnp.concatenate(sides, axis=1), table[...])
            return wide[:, 0:128] + wide[:, 128:256]

        def gradient(table, parts, at):
            even, odd = pair_sides(jnp.concatenate([middle_sum(table, parts, bb) for bb in range(8)], axis=0))
            first, second = product(even, inner_ref[at]), product(odd, inner_ref[at + 1])
            return [first[:, 0:128], first[:, 128:256], second[:, 0:128], second[:, 128:256]], odd

        along, odd = gradient(0, values, 2)
        pressed = w * product(odd, plain_ref[...])
        spill = along[2]
        heads = [None] * 3
        for d in range(2):
            grads, _ = gradient(d, values if d else slopes, 0)
            spill = spill + grads[d]
            heads[d] = adjoint([s * g - pressed if f == d else s * g for f, g in enumerate(grads)], adj_value_ref)
        heads[2] = adjoint([s * g - pressed if f == 2 else s * g for f, g in enumerate(along)] + [w * spill],
                           adj_slope_ref)
        heads = [[h[SLAB * bb:SLAB * bb + SLAB] for bb in range(8)] for h in heads]
        sums = [[None, None] for _ in range(5)]
        for bb in range(8):
            for m in range(4):
                at = bb // 4 + m
                v = scalar(2, bb, m)
                terms = [v * heads[0][bb], scalar(3, bb, m) * heads[1][bb] + v * heads[2][bb]]
                sums[at] = [a if b is None else b + a for a, b in zip(terms, sums[at])]
        for m in range(5):
            total[2 * t + m] += jnp.concatenate(sums[m], axis=0)
        return carry

    lax.fori_loop(0, STEPS // 2, step, 0, unroll=2)
    finish_traces()
    high, low = split(trace_all[...].reshape(64, 384))
    both = (route + pltpu.roll(route, 64, 1)).astype(jnp.bfloat16)
    trace_out[...] = product(both, jnp.concatenate([high, low], axis=0)).reshape(8, 16, 384)
    start_picked()
    trace_in[group] = trace_out[group]
    finish_fixes()
    high, low = split(fix_all[...].reshape(128, 384))
    flipped = route.T.astype(jnp.bfloat16)[0:64]
    fix_out[...] = product(jnp.concatenate([flipped, flipped], axis=1),
                           jnp.concatenate([high, low], axis=0)).reshape(8, 8, 384)
    start_sums()
    fix_in[z] = fix_out[z]
    lax.fori_loop(STEPS // 2, STEPS, step, 0, unroll=2)

    last = last_ref[...]
    lane = lanes_of(16)
    packed = [[jnp.zeros((16, 128), jnp.float32) for _ in range(6)] for _ in range(FIELDS)]
    for j0 in range(0, BASIS, 2):
        some = list(range(j0, min(j0 + 2, BASIS)))
        columns = []
        for j in some:
            high, low = split(total[j])
            columns.append(jnp.concatenate([high, low, high], axis=0))
        result = product(last, jnp.concatenate(columns, axis=1))
        for n, j in enumerate(some):
            piece = result[:, 128 * n:128 * n + 128]
            tile, shift = divmod(BASIS * j, 128)
            for f in range(FIELDS):
                turn = (shift - 32 * f) % 128
                turned = pltpu.roll(piece, turn, 1) if turn else piece
                end = shift + BASIS
                mask = (lane >= shift) & (lane < end)
                packed[f][tile] = jnp.where(mask, turned, packed[f][tile])
                if end > 128:
                    packed[f][tile + 1] = jnp.where(lane < end - 128, turned, packed[f][tile + 1])
    for f in range(FIELDS):
        for n in range(6):
            back[f, :, 128 * n:128 * n + 128] = packed[f][n][0:8]
            back[f, n:n + 1, 768:896] = packed[f][n][8:9]
    going = [None]
    for d in range(1, SUBS):
        copy = pltpu.make_async_remote_copy(
            src_ref=back.at[peers[d]], dst_ref=home.at[me], send_sem=back_send_sem.at[d],
            recv_sem=back_recv_sem.at[d], device_id={"sub": peers[d]}, device_id_type=MESH)
        copy.start()
        going.append(copy)
    home[me] = back[me]
    finish_picked()
    picked = trace_in[0]
    for at in range(1, 8):
        picked = picked + trace_in[at]
    to_matrices([picked[8 * h:8 * h + 8, 128 * n:128 * n + 128] for h in range(2) for n in range(3)], grid)
    jumps = []
    for k in range(8):
        jump = exact(grid[pl.ds(k, BASIS, stride=8), :][:, 0:BASIS], rights[k], ((1,), (1,)))
        jumps.append(exact(lefts[k], jump, ((1,), (0,))))
    for slot in range(4):
        grid[pl.ds(slot, BASIS, stride=8), :] = jnp.concatenate(
            [jumps[slot] - jumps[4 + slot], jnp.zeros((BASIS, 128 - BASIS), jnp.float32)], axis=1)
    jump_rows = jnp.concatenate(to_rows(lambda i: grid[8 * i:8 * i + 8, :], 8), axis=1)
    for slot in range(4):
        jump_ref[slot, 0] = jump_rows[slot:slot + 1, 0:729]
    finish_sums()
    sums = fix_in[0]
    for at in range(1, 8):
        sums = sums + fix_in[at]
    sums = [sums[4 * h:4 * h + 4, 128 * n:128 * n + 128] for h in range(2) for n in range(3)]
    to_matrices(sums, grid)
    lane = lanes_of(BASIS)
    inside = lane < BASIS
    near = jnp.where(inside, grid[pl.ds(2, BASIS, stride=8), :], 0.0)
    far = jnp.where(inside, grid[pl.ds(3, BASIS, stride=8), :], 0.0)
    far = pltpu.roll(far, 62, 1)
    ends = jnp.concatenate(sums, axis=1)
    for d in range(1, SUBS):
        going[d].wait_send()
        pltpu.make_async_remote_copy(
            src_ref=back.at[peers[d]], dst_ref=home.at[origins[d]], send_sem=back_send_sem.at[d],
            recv_sem=back_recv_sem.at[d], device_id={"sub": peers[d]}, device_id_type=MESH).wait_recv()
    x_ref[...] = jnp.zeros((BASIS, BASIS * BASIS), jnp.float32)
    for q in range(SUBS):
        x_ref[6 * q:6 * q + 8, :] += home[q, :, 0:729]
        x_ref[6 * q + 8:6 * q + 9, :] += ninth_layer(home, q)[0:1, 0:729]
    for s in range(2):
        x_ref[26 * s:26 * s + 1, :] += ends[s:s + 1, 0:729]
    x_ref[:, 0:128] += near
    x_ref[:, 640:729] += far[:, 0:89]
    out_ref[0, 0, :, 0, :] = x_ref[...]


def per_device(state, stiff_weight, volume_weight, lagrange, mortar, links):
    vmem = pl.BlockSpec(memory_space=pltpu.VMEM)
    anywhere = pl.BlockSpec(memory_space=pl.ANY)
    constants = constant_tables()
    local = [x.shape[1:] if n < 2 else x.shape for n, x in enumerate(constants)]
    result, jumps = pl.pallas_call(
        operator_kernel,
        name="operator",
        out_shape=(jax.ShapeDtypeStruct((1, 1, BASIS, 1, BASIS * BASIS), jnp.float32),
                   jax.ShapeDtypeStruct(lagrange.shape, jnp.float32)),
        in_specs=[anywhere] * 13,
        out_specs=(vmem, vmem),
        scratch_shapes=[
            pltpu.VMEM((BASIS, BASIS * BASIS), jnp.float32),
            pltpu.VMEM(lagrange.shape, jnp.float32),
            pltpu.VMEM(mortar.shape, jnp.float32),
            pltpu.VMEM((6, 256), jnp.int32),
            pltpu.SMEM((6, 256), jnp.int32),
            *[pltpu.VMEM(shape, jnp.bfloat16) for shape in local[:-1]],
            pltpu.SMEM(local[-1], jnp.float32),
            pltpu.VMEM((SLAB, QUAD * QUAD), jnp.float32),
            pltpu.VMEM((SLAB, QUAD * QUAD), jnp.float32),
            pltpu.VMEM((SUBS, 8, 896), jnp.float32),
            pltpu.VMEM((SUBS, 8, 896), jnp.float32),
            pltpu.VMEM((SUBS, 8, 896), jnp.float32),
            pltpu.VMEM((SUBS, 8, 896), jnp.float32),
            pltpu.VMEM((BASIS, 2 * SLAB, 128), jnp.float32),
            pltpu.VMEM((BASIS, 2 * SLAB, 128), jnp.float32),
            pltpu.VMEM((BASIS * 8, 128), jnp.float32),
            pltpu.VMEM((8, 384), jnp.float32),
            pltpu.VMEM((8, 8, 384), jnp.float32),
            pltpu.VMEM((8, 16, 384), jnp.float32),
            pltpu.VMEM((8, 16, 384), jnp.float32),
            pltpu.VMEM((16, 384), jnp.float32),
            pltpu.VMEM((8, 16, 384), jnp.float32),
            pltpu.VMEM((8, 8, 384), jnp.float32),
            pltpu.VMEM((8, 8, 384), jnp.float32),
            pltpu.SemaphoreType.DMA((11,)),
            pltpu.SemaphoreType.DMA((SUBS,)),
            pltpu.SemaphoreType.DMA((SUBS,)),
            pltpu.SemaphoreType.DMA((SUBS,)),
            pltpu.SemaphoreType.DMA((SUBS,)),
            pltpu.SemaphoreType.DMA((4, 8)),
            pltpu.SemaphoreType.DMA((4, 8)),
        ],
        compiler_params=pltpu.CompilerParams(collective_id=0, has_side_effects=True, vmem_limit_bytes=54 * 10**6),
        cost_estimate=pl.CostEstimate(flops=10**10, bytes_accessed=4 * 10**6, transcendentals=0),
    )(*[pltpu.with_memory_space_constraint(x, pltpu.HBM) for x in (
        jnp.transpose(state, (0, 1, 3, 2, 4)), stiff_weight, volume_weight, lagrange,
        jnp.transpose(mortar, (0, 1, 3, 2, 4)), links.T, *constants)])
    return jnp.transpose(result, (0, 1, 3, 2, 4)), jumps


def solution(mesh):
    return jax.shard_map(
        per_device,
        mesh=mesh,
        in_specs=(
            P("patch", "sub", None, None, None),
            P("patch", None, None),
            P("patch", None, None),
            P("patch", "sub", None, None),
            P("patch", None, None, None, None),
            P(),
        ),
        out_specs=(P("patch", "sub", None, None, None), P("patch", "sub", None, None)),
        check_vma=False,
    )
```

```python
import jax
import jax.numpy as jnp
import numpy as np
from jax import lax
from jax.experimental import pallas as pl
from jax.experimental.pallas import tpu as pltpu
from jax.sharding import PartitionSpec as P

ELEMS = 24
DEGREE = 3
FIELDS = 4
BASIS = 27
QUAD = 96
SUBS = 4
SLAB = QUAD // SUBS
LAYERS = SLAB // 4 + DEGREE
STEPS = 12
MESH = pl.DeviceIdType.MESH

stabilize = 0.25
highest = lax.Precision.HIGHEST
gauss_points_four = [
    -0.8611363115940526,
    -0.3399810435848563,
    0.3399810435848563,
    0.8611363115940526,
]
gauss_weights_four = [
    0.3478548451374538,
    0.6521451548625461,
    0.6521451548625461,
    0.3478548451374538,
]


def spline_tables(elements, degree):
    knot_list = np.concatenate(
        [np.zeros(degree), np.arange(elements + 1.0), np.full(degree, float(elements))]
    )
    gauss_nodes = np.array(gauss_points_four)
    gauss_weights = np.array(gauss_weights_four)
    points = (np.arange(elements)[:, None] + (gauss_nodes[None, :] + 1.0) / 2.0).reshape(-1)
    point_weights = np.tile(gauss_weights / 2.0, elements)
    current = np.where(
        (knot_list[None, :-1] <= points[:, None]) & (points[:, None] < knot_list[None, 1:]),
        1.0,
        0.0,
    )
    previous = current
    for order_k in range(1, degree + 1):
        previous = current
        amount = len(knot_list) - 1 - order_k
        current = np.zeros((points.shape[0], amount))
        for column in range(amount):
            left_span = knot_list[column + order_k] - knot_list[column]
            right_span = knot_list[column + order_k + 1] - knot_list[column + 1]
            if left_span > 0:
                current[:, column] += (points - knot_list[column]) / left_span * previous[:, column]
            if right_span > 0:
                current[:, column] += (
                    (knot_list[column + order_k + 1] - points)
                    / right_span
                    * previous[:, column + 1]
                )
    slope_part = np.zeros(current.shape)
    for column in range(current.shape[1]):
        left_span = knot_list[column + degree] - knot_list[column]
        right_span = knot_list[column + degree + 1] - knot_list[column + 1]
        if left_span > 0:
            slope_part[:, column] += degree / left_span * previous[:, column]
        if right_span > 0:
            slope_part[:, column] -= degree / right_span * previous[:, column + 1]
    return (
        current.astype(np.float32),
        slope_part.astype(np.float32),
        (current * point_weights[:, None]).astype(np.float32),
        (slope_part * point_weights[:, None]).astype(np.float32),
    )


def halves(table):
    high = table.astype(jnp.bfloat16).astype(np.float32)
    low = (table - high).astype(jnp.bfloat16).astype(np.float32)
    return high, low


def constant_tables():
    value, slope, value_w, slope_w = spline_tables(ELEMS, DEGREE)
    first = np.zeros((SUBS, 2 * SLAB, 16), np.float32)
    last = np.zeros((SUBS, 16, 2 * SLAB), np.float32)
    for q in range(SUBS):
        rows = slice(SLAB * q, SLAB * (q + 1))
        cols = slice(6 * q, 6 * q + LAYERS)
        first[q, :SLAB, :LAYERS] = value[rows, cols]
        first[q, SLAB:, :LAYERS] = slope[rows, cols]
        last[q, :LAYERS, :SLAB] = slope_w[rows, cols].T
        last[q, :LAYERS, SLAB:] = value_w[rows, cols].T
    high, low = halves(first)
    first = np.concatenate([high, high, low], axis=2)
    high, low = halves(last)
    last = np.concatenate([high, high, low], axis=2)

    def pair_tables(table):
        high, low = halves(table)
        even = np.zeros((256, 256), np.float32)
        odd = np.zeros((256, 256), np.float32)
        for s in range(2):
            cols = slice(128 * s, 128 * s + QUAD)
            even[32 * s:32 * s + BASIS, cols] = high.T
            even[128 + 32 * s:128 + 32 * s + BASIS, cols] = high.T
            even[192 + 32 * s:192 + 32 * s + BASIS, cols] = low.T
            odd[64 + 32 * s:64 + 32 * s + BASIS, cols] = high.T
            odd[128 + 32 * s:128 + 32 * s + BASIS, cols] = low.T
            odd[192 + 32 * s:192 + 32 * s + BASIS, cols] = high.T
        return even, odd

    value_even, value_odd = pair_tables(value)
    slope_even, slope_odd = pair_tables(slope)
    inner = np.stack([value_even, value_odd, slope_even, slope_odd])
    plain = value_odd[:, 128:]

    def adjoint_table(table, spilled=None):
        high, low = halves(table)
        out = np.zeros((1024, 256), np.float32)
        for f in range(FIELDS):
            scale = -stabilize if f == FIELDS - 1 else 1.0
            rows = slice(128 * f, 128 * f + QUAD)
            out[rows, 32 * f:32 * f + BASIS] = scale * high
            out[rows, 128 + 32 * f:128 + 32 * f + BASIS] = scale * low
            out[512 + 128 * f:512 + 128 * f + QUAD, 32 * f:32 * f + BASIS] = scale * high
        if spilled is None:
            return out
        high, low = halves(spilled)
        more = np.zeros((256, 256), np.float32)
        more[:QUAD, 96:96 + BASIS] = -high
        more[:QUAD, 224:224 + BASIS] = -low
        more[128:128 + QUAD, 96:96 + BASIS] = -high
        return np.concatenate([out, more])

    adjoint_value = adjoint_table(value_w)
    adjoint_slope = adjoint_table(slope_w, value_w)
    middle = np.zeros((STEPS, 128), np.float32)
    for t in range(STEPS):
        for bb in range(8):
            point = 8 * t + bb
            for m in range(4):
                col = 2 * t + bb // 4 + m
                for n, table in enumerate((value, slope, value_w, slope_w)):
                    middle[t, 32 * n + 4 * bb + m] = table[point, col]
    half = lambda x: jnp.asarray(x, jnp.bfloat16)
    return (half(first), half(last), half(inner), half(plain), half(adjoint_value), half(adjoint_slope),
            jnp.asarray(middle, jnp.float32))


def split(x):
    high = x.astype(jnp.bfloat16)
    return high, (x - high.astype(jnp.float32)).astype(jnp.bfloat16)


def product(left, right):
    return jnp.dot(left, right, preferred_element_type=jnp.float32)


def lanes_of(rows):
    return lax.broadcasted_iota(jnp.int32, (rows, 128), 1)


def exact(left, right, dims):
    return lax.dot_general(left, right, (dims, ((), ())), precision=highest, preferred_element_type=jnp.float32)


def to_matrices(tiles, grid):
    for i in range(BASIS):
        tile, shift = divmod(BASIS * i, 128)
        piece = tiles[tile]
        if shift + BASIS > 128:
            piece = jnp.where(lanes_of(piece.shape[0]) >= shift, piece, tiles[tile + 1])
        grid[8 * i:8 * i + piece.shape[0], :] = pltpu.roll(piece, 128 - shift, 1) if shift else piece


def to_rows(row_of, count):
    lane = lanes_of(count)
    tiles = [jnp.zeros((count, 128), jnp.float32) for _ in range(6)]
    for i in range(BASIS):
        tile, shift = divmod(BASIS * i, 128)
        piece = row_of(i)
        piece = pltpu.roll(piece, shift, 1) if shift else piece
        end = shift + BASIS
        tiles[tile] = jnp.where((lane >= shift) & (lane < end), piece, tiles[tile])
        if end > 128:
            tiles[tile + 1] = jnp.where(lane < end - 128, piece, tiles[tile + 1])
    return tiles


def ninth_layer(ref, at):
    first = lax.broadcasted_iota(jnp.int32, (8, 768), 0) == 0
    line = jnp.concatenate([ref[at, n:n + 1, 768:896] for n in range(6)], axis=1)
    return jnp.where(first, line, 0.0)


def routing(links_ref, y, z, core):
    row = lax.broadcasted_iota(jnp.int32, (128, 256), 0)
    col = lax.broadcasted_iota(jnp.int32, (128, 256), 1)
    source = ((row // 32) * 16 + 2 * z + (row // 16) % 2) * 4 + row % 4
    order = jnp.where(col == source, 1.0, 0.0).astype(jnp.bfloat16)
    table = links_ref[...].astype(jnp.float32).astype(jnp.bfloat16)
    found = lax.dot_general(order, table, (((1,), (1,)), ((), ())), preferred_element_type=jnp.float32)
    row = lax.broadcasted_iota(jnp.int32, (128, 1), 0)
    second = (row // 4) % 2 == 1
    patch = jnp.where(second, found[:, 1:2], found[:, 0:1])
    face = jnp.where(second, found[:, 3:4], found[:, 2:3])
    patch = jnp.where(found[:, 4:5] > 0.0, patch, -1.0)
    lane = lanes_of(128)
    row = lax.broadcasted_iota(jnp.int32, (128, 128), 0)
    wanted = (16 * y + 2 * (lane // 8) + core).astype(jnp.float32)
    same = (patch == wanted) & (face == (lane % 4).astype(jnp.float32))
    same = same & ((lane // 4) % 2 == (row // 8) % 2) & (lane < 64)
    return jnp.where(same, 1.0, 0.0)


def masked_mortar(mortar_ref, counts_ref, patch):
    row = lax.broadcasted_iota(jnp.int32, (BASIS, BASIS), 0)
    lefts, rights = [], []
    for s in range(2):
        for slot in range(4):
            at = 4 * patch + slot
            lefts.append(jnp.where(row < counts_ref[4, at], mortar_ref[slot, s, 0], 0.0))
            rights.append(jnp.where(row < counts_ref[5, at], mortar_ref[slot, s, 1], 0.0))
    return lefts, rights


def spread_kernel(x_hbm, lagrange_hbm, mortar_hbm, links_hbm, stiff_hbm, volume_hbm, first_hbm, last_hbm, inner_hbm,
                  plain_hbm, adj_value_hbm, adj_slope_hbm, got_out, trace_own, fix_own, route_out, mortar_ref, stiff,
                  volume, first_ref, last_ref, inner_ref, plain_ref, adj_value_ref, adj_slope_ref, x_ref,
                  lagrange_ref, links_ref, counts_ref, sent, got, grid, load_sem, send_sem, recv_sem):
    me = lax.axis_index("sub")
    load_x = pltpu.make_async_copy(x_hbm.at[0, 0, :, 0, :], x_ref, load_sem.at[0])
    load_x.start()
    rows = pl.ds(pl.multiple_of(me * SLAB, 8), SLAB)
    patch = lax.axis_index("patch")
    y, z, core = patch // 16, (patch // 2) % 8, patch % 2
    peers = [lax.rem(me + d, SUBS) for d in range(SUBS)]
    origins = [lax.rem(me + SUBS - d, SUBS) for d in range(SUBS)]
    barrier = pltpu.get_barrier_semaphore()
    for d in range(1, SUBS):
        pl.semaphore_signal(barrier, inc=1, device_id={"sub": peers[d]}, device_id_type=MESH)
    pairs = [(slot, s, n) for slot in range(4) for s in range(2) for n in range(2)]
    early = [
        [(links_hbm, links_ref)],
        [(links_hbm, counts_ref)],
        [(lagrange_hbm, lagrange_ref)],
        [(mortar_hbm.at[slot, s, :, n, :], mortar_ref.at[slot, s, n]) for slot, s, n in pairs],
    ]
    late = [
        [(stiff_hbm.at[0, rows], stiff), (volume_hbm.at[0, rows], volume)],
        [(first_hbm.at[me], first_ref)],
        [(inner_hbm, inner_ref), (plain_hbm, plain_ref), (adj_value_hbm, adj_value_ref),
         (adj_slope_hbm, adj_slope_ref)],
        [(last_hbm.at[me], last_ref)],
    ]
    early = [pltpu.make_async_copy(a, b, load_sem.at[1 + n]) for n, some in enumerate(early) for a, b in some]
    late = [pltpu.make_async_copy(a, b, load_sem.at[5 + n]) for n, some in enumerate(late) for a, b in some]
    for copy in early + late:
        copy.start()
    load_x.wait()
    sent[...] = jnp.zeros_like(sent)
    for q in range(SUBS):
        sent[q, :, 0:729] = x_ref[6 * q:6 * q + 8, :]
        for n in range(6):
            width = min(128, 729 - 128 * n)
            sent[q, n:n + 1, 768:768 + width] = x_ref[6 * q + 8:6 * q + 9, 128 * n:128 * n + width]
    pl.semaphore_wait(barrier, SUBS - 1)
    going = [None]
    for d in range(1, SUBS):
        copy = pltpu.make_async_remote_copy(
            src_ref=sent.at[peers[d]], dst_ref=got.at[me], send_sem=send_sem.at[d], recv_sem=recv_sem.at[d],
            device_id={"sub": peers[d]}, device_id_type=MESH)
        copy.start()
        going.append(copy)
    got[me] = sent[me]
    trace_rows = [[x_ref[26 * s:26 * s + 1, 128 * n:min(128 * n + 128, 729)] for n in range(6)] for s in range(2)]
    for s in range(2):
        tail = jnp.zeros((1, 768 - 729), jnp.float32)
        trace_rows[s][5] = jnp.concatenate([trace_rows[s][5], tail], axis=1)
    edge = x_ref[:, 0:128]
    trace_rows.append(to_rows(lambda i: edge[i:i + 1, :], 1))
    edge = jnp.concatenate([x_ref[:, 640:729], jnp.zeros((BASIS, 39), jnp.float32)], axis=1)
    edge = pltpu.roll(edge, 128 - 62, 1)
    trace_rows.append(to_rows(lambda i: edge[i:i + 1, :], 1))
    for h in range(2):
        for f in range(4):
            for n in range(3):
                trace_own[4 * h + f:4 * h + f + 1, 128 * n:128 * n + 128] = trace_rows[f][3 * h + n]
    for copy in early:
        copy.wait()
    lefts, rights = masked_mortar(mortar_ref, counts_ref, patch)
    multipliers = jnp.concatenate([lagrange_ref[slot, 0] for slot in range(4)], axis=0)
    multipliers = jnp.concatenate([multipliers, jnp.zeros((4, 768 - 729), jnp.float32)], axis=1)
    to_matrices([multipliers[:, 128 * n:128 * n + 128] for n in range(6)], grid)
    given = [grid[pl.ds(slot, BASIS, stride=8), :][:, 0:BASIS] for slot in range(4)]
    for k in range(8):
        fix = exact(given[k % 4], rights[k], ((1,), (0,)))
        fix = exact(lefts[k], fix, ((0,), (0,)))
        fix = fix if k < 4 else -fix
        grid[pl.ds(k, BASIS, stride=8), :] = jnp.concatenate(
            [fix, jnp.zeros((BASIS, 128 - BASIS), jnp.float32)], axis=1)
    fix_rows = to_rows(lambda i: grid[8 * i:8 * i + 8, :], 8)
    for h in range(2):
        for n in range(3):
            fix_own[8 * h:8 * h + 8, 128 * n:128 * n + 128] = fix_rows[3 * h + n]
    route_out[...] = routing(links_ref, y, z, core)
    for d in range(1, SUBS):
        going[d].wait_send()
        pltpu.make_async_remote_copy(
            src_ref=sent.at[peers[d]], dst_ref=got.at[origins[d]], send_sem=send_sem.at[d],
            recv_sem=recv_sem.at[d], device_id={"sub": peers[d]}, device_id_type=MESH).wait_recv()

    got_out[...] = got[...]
    for copy in late:
        copy.wait()


def operator_kernel(got, trace_own, fix_own, route_ref, mortar_ref, stiff, volume, first_ref, last_ref, inner_ref,
                    plain_ref, adj_value_ref, adj_slope_ref, middle_hbm, links_hbm, out_ref, jump_ref, x_ref,
                    middle_ref, counts_ref, back, home, outer, total, grid, trace_all, trace_out, trace_in, fix_all,
                    fix_out, fix_in, load_sem, back_send_sem, back_recv_sem, face_send_sem, face_recv_sem):
    load_middle = pltpu.make_async_copy(middle_hbm, middle_ref, load_sem.at[0])
    load_counts = pltpu.make_async_copy(links_hbm, counts_ref, load_sem.at[1])
    load_middle.start()
    load_counts.start()
    me = lax.axis_index("sub")
    patch = lax.axis_index("patch")
    y, z, core = patch // 16, (patch // 2) % 8, patch % 2
    group = 2 * y + core
    line = [lax.rem(z + d, 8) for d in range(8)]
    line_from = [lax.rem(z + 8 - d, 8) for d in range(8)]
    plane = [lax.rem(group + d, 8) for d in range(8)]
    plane_from = [lax.rem(group + 8 - d, 8) for d in range(8)]
    line_ids = [{"patch": 16 * y + 2 * at + core} for at in line]
    plane_ids = [{"patch": 16 * (at // 2) + 2 * z + at % 2} for at in plane]

    def exchange(n, source, target, slot, slots_from, ids):
        def one(d, at):
            return pltpu.make_async_remote_copy(
                src_ref=source(d), dst_ref=target.at[at], send_sem=face_send_sem.at[n, d],
                recv_sem=face_recv_sem.at[n, d], device_id=ids[d], device_id_type=MESH)

        def start():
            for d in range(1, 8):
                one(d, slot).start()

        def finish():
            for d in range(1, 8):
                one(d, slot).wait_send()
                one(d, slots_from[d]).wait_recv()

        return start, finish

    peers = [lax.rem(me + d, SUBS) for d in range(SUBS)]
    origins = [lax.rem(me + SUBS - d, SUBS) for d in range(SUBS)]
    barrier = pltpu.get_barrier_semaphore()
    for d in range(1, SUBS):
        pl.semaphore_signal(barrier, inc=1, device_id={"sub": peers[d]}, device_id_type=MESH)
    for d in range(1, 8):
        for ids in (line_ids, plane_ids):
            pl.semaphore_signal(barrier, inc=1, device_id=ids[d], device_id_type=MESH)
    start_traces, finish_traces = exchange(0, lambda d: trace_own, trace_all, z, line_from, line_ids)
    start_picked, finish_picked = exchange(1, lambda d: trace_out.at[plane[d]], trace_in, group, plane_from, plane_ids)
    start_fixes, finish_fixes = exchange(2, lambda d: fix_own, fix_all, group, plane_from, plane_ids)
    start_sums, finish_sums = exchange(3, lambda d: fix_out.at[line[d]], fix_in, z, line_from, line_ids)
    total[...] = jnp.zeros_like(total)
    first = first_ref[...]
    slabs = [jnp.concatenate([got[f, :, 0:768], ninth_layer(got, f)], axis=0) for f in range(FIELDS)]
    lane = lanes_of(16)
    columns = []
    for j in range(BASIS):
        tile, shift = divmod(BASIS * j, 128)
        merged = None
        for f in range(FIELDS):
            piece = slabs[f][:, 128 * tile:128 * tile + 128]
            if shift + BASIS > 128:
                piece = jnp.where(lane >= shift, piece, slabs[f][:, 128 * tile + 128:128 * tile + 256])
            turn = (32 * f - shift) % 128
            piece = pltpu.roll(piece, turn, 1) if turn else piece
            merged = piece if f == 0 else jnp.where(lane >= 32 * f, piece, merged)
        high, low = split(merged)
        columns.append(jnp.concatenate([high, low, high], axis=0))
    for j in range(0, BASIS, 2):
        result = product(first, jnp.concatenate(columns[j:j + 2], axis=1))
        for n in range(min(2, BASIS - j)):
            outer[j + n] = result[:, 128 * n:128 * n + 128]
    load_middle.wait()

    def step(t, carry):
        def scalar(table, bb, m):
            return middle_ref[t, 32 * table + 4 * bb + m]

        window = [outer[2 * t + m] for m in range(5)]
        values = [w[0:SLAB] for w in window]
        slopes = [w[SLAB:2 * SLAB] for w in window]

        def middle_sum(table, parts, bb):
            e = bb // 4
            out = scalar(table, bb, 0) * parts[e]
            for m in range(1, 4):
                out = out + scalar(table, bb, m) * parts[e + m]
            return out

        def pair_sides(x):
            lane = lanes_of(x.shape[0])
            high = x.astype(jnp.bfloat16)
            wide = high.astype(jnp.float32)
            low = x - wide
            turned = pltpu.roll(wide, 64, 1)
            even = jnp.where(lane < 64, low, turned).astype(jnp.bfloat16)
            odd = jnp.where(lane < 64, turned, low).astype(jnp.bfloat16)
            return jnp.concatenate([high, even], axis=1), jnp.concatenate([high, odd], axis=1)

        def weights(ref):
            lane = lanes_of(SLAB)
            tiles = [ref[:, pl.ds(pl.multiple_of(768 * t + 128 * n, 128), 128)] for n in range(6)]
            parts = []
            for bb in range(8):
                tile, shift = divmod(QUAD * bb, 128)
                part = tiles[tile]
                if shift + QUAD > 128:
                    part = jnp.where(lane >= shift, part, tiles[tile + 1])
                parts.append(pltpu.roll(part, 128 - shift, 1) if shift else part)
            return jnp.concatenate(parts, axis=0)

        s = weights(stiff)
        w = weights(volume)
        def adjoint(parts, table):
            pairs = [split(p) for p in parts]
            sides = [p[0] for p in pairs[:FIELDS]] + [p[1] for p in pairs[:FIELDS]]
            for pair in pairs[FIELDS:]:
                sides.extend(pair)
            wide = product(jnp.concatenate(sides, axis=1), table[...])
            return wide[:, 0:128] + wide[:, 128:256]

        def gradient(table, parts, at):
            even, odd = pair_sides(jnp.concatenate([middle_sum(table, parts, bb) for bb in range(8)], axis=0))
            first, second = product(even, inner_ref[at]), product(odd, inner_ref[at + 1])
            return [first[:, 0:128], first[:, 128:256], second[:, 0:128], second[:, 128:256]], odd

        along, odd = gradient(0, values, 2)
        pressed = w * product(odd, plain_ref[...])
        spill = along[2]
        heads = [None] * 3
        for d in range(2):
            grads, _ = gradient(d, values if d else slopes, 0)
            spill = spill + grads[d]
            heads[d] = adjoint([s * g - pressed if f == d else s * g for f, g in enumerate(grads)], adj_value_ref)
        heads[2] = adjoint([s * g - pressed if f == 2 else s * g for f, g in enumerate(along)] + [w * spill],
                           adj_slope_ref)
        heads = [[h[SLAB * bb:SLAB * bb + SLAB] for bb in range(8)] for h in heads]
        sums = [[None, None] for _ in range(5)]
        for bb in range(8):
            for m in range(4):
                at = bb // 4 + m
                v = scalar(2, bb, m)
                terms = [v * heads[0][bb], scalar(3, bb, m) * heads[1][bb] + v * heads[2][bb]]
                sums[at] = [a if b is None else b + a for a, b in zip(terms, sums[at])]
        for m in range(5):
            total[2 * t + m] += jnp.concatenate(sums[m], axis=0)
        return carry

    lax.fori_loop(0, STEPS // 2, step, 0, unroll=2)
    pl.semaphore_wait(barrier, SUBS - 1 + 14)
    start_traces()
    trace_all[z] = trace_own[...]
    start_fixes()
    fix_all[group] = fix_own[...]
    lax.fori_loop(STEPS // 2, STEPS, step, 0, unroll=2)

    last = last_ref[...]
    lane = lanes_of(16)
    packed = [[jnp.zeros((16, 128), jnp.float32) for _ in range(6)] for _ in range(FIELDS)]
    for j0 in range(0, BASIS, 2):
        some = list(range(j0, min(j0 + 2, BASIS)))
        columns = []
        for j in some:
            high, low = split(total[j])
            columns.append(jnp.concatenate([high, low, high], axis=0))
        result = product(last, jnp.concatenate(columns, axis=1))
        for n, j in enumerate(some):
            piece = result[:, 128 * n:128 * n + 128]
            tile, shift = divmod(BASIS * j, 128)
            for f in range(FIELDS):
                turn = (shift - 32 * f) % 128
                turned = pltpu.roll(piece, turn, 1) if turn else piece
                end = shift + BASIS
                mask = (lane >= shift) & (lane < end)
                packed[f][tile] = jnp.where(mask, turned, packed[f][tile])
                if end > 128:
                    packed[f][tile + 1] = jnp.where(lane < end - 128, turned, packed[f][tile + 1])
    for f in range(FIELDS):
        for n in range(6):
            back[f, :, 128 * n:128 * n + 128] = packed[f][n][0:8]
            back[f, n:n + 1, 768:896] = packed[f][n][8:9]
    going = [None]
    for d in range(1, SUBS):
        copy = pltpu.make_async_remote_copy(
            src_ref=back.at[peers[d]], dst_ref=home.at[me], send_sem=back_send_sem.at[d],
            recv_sem=back_recv_sem.at[d], device_id={"sub": peers[d]}, device_id_type=MESH)
        copy.start()
        going.append(copy)
    home[me] = back[me]
    finish_traces()
    high, low = split(trace_all[...].reshape(64, 384))
    both = (route_ref[...] + pltpu.roll(route_ref[...], 64, 1)).astype(jnp.bfloat16)
    trace_out[...] = product(both, jnp.concatenate([high, low], axis=0)).reshape(8, 16, 384)
    start_picked()
    trace_in[group] = trace_out[group]
    finish_fixes()
    high, low = split(fix_all[...].reshape(128, 384))
    flipped = route_ref[...].T.astype(jnp.bfloat16)[0:64]
    fix_out[...] = product(jnp.concatenate([flipped, flipped], axis=1),
                           jnp.concatenate([high, low], axis=0)).reshape(8, 8, 384)
    start_sums()
    fix_in[z] = fix_out[z]
    for d in range(1, SUBS):
        going[d].wait_send()
        pltpu.make_async_remote_copy(
            src_ref=back.at[peers[d]], dst_ref=home.at[origins[d]], send_sem=back_send_sem.at[d],
            recv_sem=back_recv_sem.at[d], device_id={"sub": peers[d]}, device_id_type=MESH).wait_recv()
    x_ref[...] = jnp.zeros((BASIS, BASIS * BASIS), jnp.float32)
    for q in range(SUBS):
        x_ref[6 * q:6 * q + 8, :] += home[q, :, 0:729]
        x_ref[6 * q + 8:6 * q + 9, :] += ninth_layer(home, q)[0:1, 0:729]
    finish_picked()
    picked = trace_in[0]
    for at in range(1, 8):
        picked = picked + trace_in[at]
    to_matrices([picked[8 * h:8 * h + 8, 128 * n:128 * n + 128] for h in range(2) for n in range(3)], grid)
    load_counts.wait()
    lefts, rights = masked_mortar(mortar_ref, counts_ref, patch)
    jumps = []
    for k in range(8):
        jump = exact(grid[pl.ds(k, BASIS, stride=8), :][:, 0:BASIS], rights[k], ((1,), (1,)))
        jumps.append(exact(lefts[k], jump, ((1,), (0,))))
    for slot in range(4):
        grid[pl.ds(slot, BASIS, stride=8), :] = jnp.concatenate(
            [jumps[slot] - jumps[4 + slot], jnp.zeros((BASIS, 128 - BASIS), jnp.float32)], axis=1)
    jump_rows = jnp.concatenate(to_rows(lambda i: grid[8 * i:8 * i + 8, :], 8), axis=1)
    for slot in range(4):
        jump_ref[slot, 0] = jump_rows[slot:slot + 1, 0:729]
    finish_sums()
    sums = fix_in[0]
    for at in range(1, 8):
        sums = sums + fix_in[at]
    sums = [sums[4 * h:4 * h + 4, 128 * n:128 * n + 128] for h in range(2) for n in range(3)]
    to_matrices(sums, grid)
    lane = lanes_of(BASIS)
    inside = lane < BASIS
    near = jnp.where(inside, grid[pl.ds(2, BASIS, stride=8), :], 0.0)
    far = jnp.where(inside, grid[pl.ds(3, BASIS, stride=8), :], 0.0)
    far = pltpu.roll(far, 62, 1)
    ends = jnp.concatenate(sums, axis=1)
    for s in range(2):
        x_ref[26 * s:26 * s + 1, :] += ends[s:s + 1, 0:729]
    x_ref[:, 0:128] += near
    x_ref[:, 640:729] += far[:, 0:89]
    out_ref[0, 0, :, 0, :] = x_ref[...]


def per_device(state, stiff_weight, volume_weight, lagrange, mortar, links):
    vmem = pl.BlockSpec(memory_space=pltpu.VMEM)
    anywhere = pl.BlockSpec(memory_space=pl.ANY)
    f32 = lambda *shape: jax.ShapeDtypeStruct(shape, jnp.float32)
    constants = constant_tables()
    mortar = jnp.transpose(mortar, (0, 1, 3, 2, 4))
    links = links.T
    local = [f32(*(x.shape[1:] if n < 2 else x.shape)) for n, x in enumerate(constants[:-1])]
    local = [jax.ShapeDtypeStruct(x.shape, jnp.bfloat16) for x in local]
    pinned = lambda xs: [pltpu.with_memory_space_constraint(x, pltpu.HBM) for x in xs]
    staged = (f32(SUBS, 8, 896), f32(8, 384), f32(16, 384), f32(128, 128), f32(4, 2, 2, BASIS, BASIS),
              f32(SLAB, QUAD * QUAD), f32(SLAB, QUAD * QUAD), *local)
    spread = pl.pallas_call(
        spread_kernel,
        name="spread",
        out_shape=staged,
        in_specs=[anywhere] * 12,
        out_specs=(vmem,) * len(staged),
        scratch_shapes=[
            pltpu.VMEM((BASIS, BASIS * BASIS), jnp.float32),
            pltpu.VMEM(lagrange.shape, jnp.float32),
            pltpu.VMEM((6, 256), jnp.int32),
            pltpu.SMEM((6, 256), jnp.int32),
            pltpu.VMEM((SUBS, 8, 896), jnp.float32),
            pltpu.VMEM((SUBS, 8, 896), jnp.float32),
            pltpu.VMEM((BASIS * 8, 128), jnp.float32),
            pltpu.SemaphoreType.DMA((9,)),
            pltpu.SemaphoreType.DMA((SUBS,)),
            pltpu.SemaphoreType.DMA((SUBS,)),
        ],
        compiler_params=pltpu.CompilerParams(collective_id=0, has_side_effects=True, vmem_limit_bytes=40 * 10**6),
        cost_estimate=pl.CostEstimate(flops=10**9, bytes_accessed=10**5, transcendentals=0),
    )(*pinned((jnp.transpose(state, (0, 1, 3, 2, 4)), lagrange, mortar, links, stiff_weight, volume_weight,
               *constants[:-1])))
    result, jumps = pl.pallas_call(
        operator_kernel,
        name="operator",
        out_shape=(f32(1, 1, BASIS, 1, BASIS * BASIS), f32(*lagrange.shape)),
        in_specs=[vmem] * 13 + [anywhere] * 2,
        out_specs=(vmem, vmem),
        scratch_shapes=[
            pltpu.VMEM((BASIS, BASIS * BASIS), jnp.float32),
            pltpu.SMEM(constants[-1].shape, jnp.float32),
            pltpu.SMEM((6, 256), jnp.int32),
            pltpu.VMEM((SUBS, 8, 896), jnp.float32),
            pltpu.VMEM((SUBS, 8, 896), jnp.float32),
            pltpu.VMEM((BASIS, 2 * SLAB, 128), jnp.float32),
            pltpu.VMEM((BASIS, 2 * SLAB, 128), jnp.float32),
            pltpu.VMEM((BASIS * 8, 128), jnp.float32),
            pltpu.VMEM((8, 8, 384), jnp.float32),
            pltpu.VMEM((8, 16, 384), jnp.float32),
            pltpu.VMEM((8, 16, 384), jnp.float32),
            pltpu.VMEM((8, 16, 384), jnp.float32),
            pltpu.VMEM((8, 8, 384), jnp.float32),
            pltpu.VMEM((8, 8, 384), jnp.float32),
            pltpu.SemaphoreType.DMA((2,)),
            pltpu.SemaphoreType.DMA((SUBS,)),
            pltpu.SemaphoreType.DMA((SUBS,)),
            pltpu.SemaphoreType.DMA((4, 8)),
            pltpu.SemaphoreType.DMA((4, 8)),
        ],
        compiler_params=pltpu.CompilerParams(collective_id=1, has_side_effects=True, vmem_limit_bytes=40 * 10**6),
        cost_estimate=pl.CostEstimate(flops=10**10, bytes_accessed=4 * 10**6, transcendentals=0),
    )(*spread, *pinned((constants[-1], links)))
    return jnp.transpose(result, (0, 1, 3, 2, 4)), jumps


def solution(mesh):
    return jax.shard_map(
        per_device,
        mesh=mesh,
        in_specs=(
            P("patch", "sub", None, None, None),
            P("patch", None, None),
            P("patch", None, None),
            P("patch", "sub", None, None),
            P("patch", None, None, None, None),
            P(),
        ),
        out_specs=(P("patch", "sub", None, None, None), P("patch", "sub", None, None)),
        check_vma=False,
    )
```

```python
import jax
import jax.numpy as jnp
import numpy as np
from jax import lax
from jax.experimental import pallas as pl
from jax.experimental.pallas import tpu as pltpu
from jax.sharding import PartitionSpec as P

ELEMS = 24
DEGREE = 3
FIELDS = 4
BASIS = 27
QUAD = 96
SUBS = 4
SLAB = QUAD // SUBS
LAYERS = SLAB // 4 + DEGREE
STEPS = 12
MESH = pl.DeviceIdType.MESH

stabilize = 0.25
highest = lax.Precision.HIGHEST
gauss_points_four = [
    -0.8611363115940526,
    -0.3399810435848563,
    0.3399810435848563,
    0.8611363115940526,
]
gauss_weights_four = [
    0.3478548451374538,
    0.6521451548625461,
    0.6521451548625461,
    0.3478548451374538,
]


def spline_tables(elements, degree):
    knot_list = np.concatenate(
        [np.zeros(degree), np.arange(elements + 1.0), np.full(degree, float(elements))]
    )
    gauss_nodes = np.array(gauss_points_four)
    gauss_weights = np.array(gauss_weights_four)
    points = (np.arange(elements)[:, None] + (gauss_nodes[None, :] + 1.0) / 2.0).reshape(-1)
    point_weights = np.tile(gauss_weights / 2.0, elements)
    current = np.where(
        (knot_list[None, :-1] <= points[:, None]) & (points[:, None] < knot_list[None, 1:]),
        1.0,
        0.0,
    )
    previous = current
    for order_k in range(1, degree + 1):
        previous = current
        amount = len(knot_list) - 1 - order_k
        current = np.zeros((points.shape[0], amount))
        for column in range(amount):
            left_span = knot_list[column + order_k] - knot_list[column]
            right_span = knot_list[column + order_k + 1] - knot_list[column + 1]
            if left_span > 0:
                current[:, column] += (points - knot_list[column]) / left_span * previous[:, column]
            if right_span > 0:
                current[:, column] += (
                    (knot_list[column + order_k + 1] - points)
                    / right_span
                    * previous[:, column + 1]
                )
    slope_part = np.zeros(current.shape)
    for column in range(current.shape[1]):
        left_span = knot_list[column + degree] - knot_list[column]
        right_span = knot_list[column + degree + 1] - knot_list[column + 1]
        if left_span > 0:
            slope_part[:, column] += degree / left_span * previous[:, column]
        if right_span > 0:
            slope_part[:, column] -= degree / right_span * previous[:, column + 1]
    return (
        current.astype(np.float32),
        slope_part.astype(np.float32),
        (current * point_weights[:, None]).astype(np.float32),
        (slope_part * point_weights[:, None]).astype(np.float32),
    )


def halves(table):
    high = table.astype(jnp.bfloat16).astype(np.float32)
    low = (table - high).astype(jnp.bfloat16).astype(np.float32)
    return high, low


def constant_tables():
    value, slope, value_w, slope_w = spline_tables(ELEMS, DEGREE)
    first = np.zeros((SUBS, 2 * SLAB, 16), np.float32)
    last = np.zeros((SUBS, 16, 2 * SLAB), np.float32)
    for q in range(SUBS):
        rows = slice(SLAB * q, SLAB * (q + 1))
        cols = slice(6 * q, 6 * q + LAYERS)
        first[q, :SLAB, :LAYERS] = value[rows, cols]
        first[q, SLAB:, :LAYERS] = slope[rows, cols]
        last[q, :LAYERS, :SLAB] = slope_w[rows, cols].T
        last[q, :LAYERS, SLAB:] = value_w[rows, cols].T
    high, low = halves(first)
    first = np.concatenate([high, high, low], axis=2)
    high, low = halves(last)
    last = np.concatenate([high, high, low], axis=2)

    def pair_tables(table):
        high, low = halves(table)
        even = np.zeros((256, 256), np.float32)
        odd = np.zeros((256, 256), np.float32)
        for s in range(2):
            cols = slice(128 * s, 128 * s + QUAD)
            even[32 * s:32 * s + BASIS, cols] = high.T
            even[128 + 32 * s:128 + 32 * s + BASIS, cols] = high.T
            even[192 + 32 * s:192 + 32 * s + BASIS, cols] = low.T
            odd[64 + 32 * s:64 + 32 * s + BASIS, cols] = high.T
            odd[128 + 32 * s:128 + 32 * s + BASIS, cols] = low.T
            odd[192 + 32 * s:192 + 32 * s + BASIS, cols] = high.T
        return even, odd

    value_even, value_odd = pair_tables(value)
    slope_even, slope_odd = pair_tables(slope)
    inner = np.stack([value_even, value_odd, slope_even, slope_odd])
    plain = value_odd[:, 128:]

    def adjoint_table(table, spilled=None):
        high, low = halves(table)
        out = np.zeros((1024, 256), np.float32)
        for f in range(FIELDS):
            scale = -stabilize if f == FIELDS - 1 else 1.0
            rows = slice(128 * f, 128 * f + QUAD)
            out[rows, 32 * f:32 * f + BASIS] = scale * high
            out[rows, 128 + 32 * f:128 + 32 * f + BASIS] = scale * low
            out[512 + 128 * f:512 + 128 * f + QUAD, 32 * f:32 * f + BASIS] = scale * high
        if spilled is None:
            return out
        high, low = halves(spilled)
        more = np.zeros((256, 256), np.float32)
        more[:QUAD, 96:96 + BASIS] = -high
        more[:QUAD, 224:224 + BASIS] = -low
        more[128:128 + QUAD, 96:96 + BASIS] = -high
        return np.concatenate([out, more])

    adjoint_value = adjoint_table(value_w)
    adjoint_slope = adjoint_table(slope_w, value_w)
    middle = np.zeros((STEPS, 128), np.float32)
    for t in range(STEPS):
        for bb in range(8):
            point = 8 * t + bb
            for m in range(4):
                col = 2 * t + bb // 4 + m
                for n, table in enumerate((value, slope, value_w, slope_w)):
                    middle[t, 32 * n + 4 * bb + m] = table[point, col]
    half = lambda x: jnp.asarray(x, jnp.bfloat16)
    return (half(first), half(last), half(inner), half(plain), half(adjoint_value), half(adjoint_slope),
            jnp.asarray(middle, jnp.float32))


def split(x):
    high = x.astype(jnp.bfloat16)
    return high, (x - high.astype(jnp.float32)).astype(jnp.bfloat16)


def product(left, right):
    return jnp.dot(left, right, preferred_element_type=jnp.float32)


def lanes_of(rows):
    return lax.broadcasted_iota(jnp.int32, (rows, 128), 1)


def exact(left, right, dims):
    return lax.dot_general(left, right, (dims, ((), ())), precision=highest, preferred_element_type=jnp.float32)


def to_matrices(tiles, grid):
    for i in range(BASIS):
        tile, shift = divmod(BASIS * i, 128)
        piece = tiles[tile]
        if shift + BASIS > 128:
            piece = jnp.where(lanes_of(piece.shape[0]) >= shift, piece, tiles[tile + 1])
        grid[8 * i:8 * i + piece.shape[0], :] = pltpu.roll(piece, 128 - shift, 1) if shift else piece


def to_rows(row_of, count):
    lane = lanes_of(count)
    tiles = [jnp.zeros((count, 128), jnp.float32) for _ in range(6)]
    for i in range(BASIS):
        tile, shift = divmod(BASIS * i, 128)
        piece = row_of(i)
        piece = pltpu.roll(piece, shift, 1) if shift else piece
        end = shift + BASIS
        tiles[tile] = jnp.where((lane >= shift) & (lane < end), piece, tiles[tile])
        if end > 128:
            tiles[tile + 1] = jnp.where(lane < end - 128, piece, tiles[tile + 1])
    return tiles


def slab_layers(ref, half, at):
    first = lax.broadcasted_iota(jnp.int32, (8, 384), 0) == 0
    line = jnp.concatenate([ref[half, at, n:n + 1, 384:512] for n in range(3)], axis=1)
    return jnp.concatenate([ref[half, at, :, 0:384], jnp.where(first, line, 0.0)], axis=0)


def routing(links_ref, y, z, core):
    row = lax.broadcasted_iota(jnp.int32, (128, 256), 0)
    col = lax.broadcasted_iota(jnp.int32, (128, 256), 1)
    source = ((row // 32) * 16 + 2 * z + (row // 16) % 2) * 4 + row % 4
    order = jnp.where(col == source, 1.0, 0.0).astype(jnp.bfloat16)
    table = links_ref[...].astype(jnp.float32).astype(jnp.bfloat16)
    found = lax.dot_general(order, table, (((1,), (1,)), ((), ())), preferred_element_type=jnp.float32)
    row = lax.broadcasted_iota(jnp.int32, (128, 1), 0)
    second = (row // 4) % 2 == 1
    patch = jnp.where(second, found[:, 1:2], found[:, 0:1])
    face = jnp.where(second, found[:, 3:4], found[:, 2:3])
    patch = jnp.where(found[:, 4:5] > 0.0, patch, -1.0)
    lane = lanes_of(128)
    row = lax.broadcasted_iota(jnp.int32, (128, 128), 0)
    wanted = (16 * y + 2 * (lane // 8) + core).astype(jnp.float32)
    same = (patch == wanted) & (face == (lane % 4).astype(jnp.float32))
    same = same & ((lane // 4) % 2 == (row // 8) % 2) & (lane < 64)
    return jnp.where(same, 1.0, 0.0)


def operator_kernel(x_hbm, stiff_hbm, volume_hbm, lagrange_hbm, mortar_hbm, links_hbm, first_hbm, last_hbm,
                    inner_hbm, plain_hbm, adj_value_hbm, adj_slope_hbm, middle_hbm, out_ref, jump_ref,
                    x_ref, lagrange_ref, mortar_ref, links_ref, counts_ref, first_ref, last_ref, inner_ref,
                    plain_ref, adj_value_ref, adj_slope_ref, middle_ref, stiff, volume, sent, got, back, home, outer, total, grid, trace_own, trace_all,
                    trace_out, trace_in, fix_own, fix_all, fix_out, fix_in, load_sem, send_sem, recv_sem,
                    back_send_sem, back_recv_sem, face_send_sem, face_recv_sem):
    me = lax.axis_index("sub")
    patch = lax.axis_index("patch")
    y, z, core = patch // 16, (patch // 2) % 8, patch % 2
    group = 2 * y + core
    line = [lax.rem(z + d, 8) for d in range(8)]
    line_from = [lax.rem(z + 8 - d, 8) for d in range(8)]
    plane = [lax.rem(group + d, 8) for d in range(8)]
    plane_from = [lax.rem(group + 8 - d, 8) for d in range(8)]
    line_ids = [{"patch": 16 * y + 2 * at + core} for at in line]
    plane_ids = [{"patch": 16 * (at // 2) + 2 * z + at % 2} for at in plane]

    def exchange(n, source, target, slot, slots_from, ids):
        def one(d, at):
            return pltpu.make_async_remote_copy(
                src_ref=source(d), dst_ref=target.at[at], send_sem=face_send_sem.at[n, d],
                recv_sem=face_recv_sem.at[n, d], device_id=ids[d], device_id_type=MESH)

        def start():
            for d in range(1, 8):
                one(d, slot).start()

        def finish():
            for d in range(1, 8):
                one(d, slot).wait_send()
                one(d, slots_from[d]).wait_recv()

        return start, finish

    load_x = pltpu.make_async_copy(x_hbm.at[0, 0, :, 0, :], x_ref, load_sem.at[0])
    load_x.start()
    peers = [lax.rem(me + d, SUBS) for d in range(SUBS)]
    origins = [lax.rem(me + SUBS - d, SUBS) for d in range(SUBS)]
    barrier = pltpu.get_barrier_semaphore()
    for d in range(1, SUBS):
        pl.semaphore_signal(barrier, inc=1, device_id={"sub": peers[d]}, device_id_type=MESH)
    for d in range(1, 8):
        for ids in (line_ids, plane_ids):
            pl.semaphore_signal(barrier, inc=1, device_id=ids[d], device_id_type=MESH)
    rows = pl.ds(pl.multiple_of(me * SLAB, 8), SLAB)
    pairs = [(slot, s, n) for slot in range(4) for s in range(2) for n in range(2)]
    loads = [
        [(links_hbm, links_ref)],
        [(links_hbm, counts_ref)],
        [(lagrange_hbm, lagrange_ref)],
        [(mortar_hbm.at[slot, s, :, n, :], mortar_ref.at[slot, s, n]) for slot, s, n in pairs],
        [(first_hbm.at[me], first_ref)],
        [(middle_hbm, middle_ref)],
        [(inner_hbm, inner_ref), (plain_hbm, plain_ref)],
        [(stiff_hbm.at[0, rows], stiff), (volume_hbm.at[0, rows], volume)],
        [(adj_value_hbm, adj_value_ref), (adj_slope_hbm, adj_slope_ref)],
        [(last_hbm.at[me], last_ref)],
    ]
    loads = [[pltpu.make_async_copy(a, b, load_sem.at[1 + n]) for a, b in some] for n, some in enumerate(loads)]
    for some in loads:
        for copy in some:
            copy.start()

    def loaded(*which):
        for n in which:
            for copy in loads[n]:
                copy.wait()

    load_x.wait()
    sent[...] = jnp.zeros_like(sent)
    for half in range(2):
        for q in range(SUBS):
            width = min(384, 729 - 384 * half)
            sent[half, q, :, 0:width] = x_ref[6 * q:6 * q + 8, 384 * half:384 * half + width]
            for n in range(3):
                lane = 384 * half + 128 * n
                width = min(128, 729 - lane)
                sent[half, q, n:n + 1, 384:384 + width] = x_ref[6 * q + 8:6 * q + 9, lane:lane + width]
    trace_rows = [[x_ref[26 * s:26 * s + 1, 128 * n:min(128 * n + 128, 729)] for n in range(6)] for s in range(2)]
    for s in range(2):
        tail = jnp.zeros((1, 768 - 729), jnp.float32)
        trace_rows[s][5] = jnp.concatenate([trace_rows[s][5], tail], axis=1)
    edge = x_ref[:, 0:128]
    trace_rows.append(to_rows(lambda i: edge[i:i + 1, :], 1))
    edge = jnp.concatenate([x_ref[:, 640:729], jnp.zeros((BASIS, 39), jnp.float32)], axis=1)
    edge = pltpu.roll(edge, 128 - 62, 1)
    trace_rows.append(to_rows(lambda i: edge[i:i + 1, :], 1))
    for h in range(2):
        for f in range(4):
            for n in range(3):
                trace_own[4 * h + f:4 * h + f + 1, 128 * n:128 * n + 128] = trace_rows[f][3 * h + n]
    start_traces, finish_traces = exchange(0, lambda d: trace_own, trace_all, z, line_from, line_ids)
    start_picked, finish_picked = exchange(1, lambda d: trace_out.at[plane[d]], trace_in, group, plane_from, plane_ids)
    start_fixes, finish_fixes = exchange(2, lambda d: fix_own, fix_all, group, plane_from, plane_ids)
    start_sums, finish_sums = exchange(3, lambda d: fix_out.at[line[d]], fix_in, z, line_from, line_ids)
    pl.semaphore_wait(barrier, SUBS - 1 + 14)
    def sub_exchange(half, source, target, send, recv):
        def one(d, at):
            return pltpu.make_async_remote_copy(
                src_ref=source.at[half, peers[d]], dst_ref=target.at[half, at], send_sem=send.at[half, d],
                recv_sem=recv.at[half, d], device_id={"sub": peers[d]}, device_id_type=MESH)

        def start():
            for d in range(1, SUBS):
                one(d, me).start()
            target[half, me] = source[half, me]

        def finish():
            for d in range(1, SUBS):
                one(d, me).wait_send()
                one(d, origins[d]).wait_recv()

        return start, finish

    layers = [sub_exchange(half, sent, got, send_sem, recv_sem) for half in range(2)]
    sums_home = [sub_exchange(half, back, home, back_send_sem, back_recv_sem) for half in range(2)]
    layers[0][0]()
    layers[1][0]()
    start_traces()
    trace_all[z] = trace_own[...]
    loaded(0, 1, 2, 3)
    row = lax.broadcasted_iota(jnp.int32, (BASIS, BASIS), 0)
    lefts, rights = [], []
    for s in range(2):
        for slot in range(4):
            at = 4 * patch + slot
            lefts.append(jnp.where(row < counts_ref[4, at], mortar_ref[slot, s, 0], 0.0))
            rights.append(jnp.where(row < counts_ref[5, at], mortar_ref[slot, s, 1], 0.0))
    multipliers = jnp.concatenate([lagrange_ref[slot, 0] for slot in range(4)], axis=0)
    multipliers = jnp.concatenate([multipliers, jnp.zeros((4, 768 - 729), jnp.float32)], axis=1)
    to_matrices([multipliers[:, 128 * n:128 * n + 128] for n in range(6)], grid)
    given = [grid[pl.ds(slot, BASIS, stride=8), :][:, 0:BASIS] for slot in range(4)]
    for k in range(8):
        fix = exact(given[k % 4], rights[k], ((1,), (0,)))
        fix = exact(lefts[k], fix, ((0,), (0,)))
        fix = fix if k < 4 else -fix
        grid[pl.ds(k, BASIS, stride=8), :] = jnp.concatenate(
            [fix, jnp.zeros((BASIS, 128 - BASIS), jnp.float32)], axis=1)
    fix_rows = to_rows(lambda i: grid[8 * i:8 * i + 8, :], 8)
    for h in range(2):
        for n in range(3):
            fix_own[8 * h:8 * h + 8, 128 * n:128 * n + 128] = fix_rows[3 * h + n]
    start_fixes()
    fix_all[group] = fix_own[...]
    route = routing(links_ref, y, z, core)
    total[...] = jnp.zeros_like(total)
    layers[0][1]()
    loaded(4)
    first = first_ref[...]

    def first_stage(begin, end):
        slabs = [jnp.concatenate([slab_layers(got, half, f) for half in range(1 + (end > 14))], axis=1)
                 for f in range(FIELDS)]
        lane = lanes_of(16)
        columns = []
        for j in range(begin, end):
            tile, shift = divmod(BASIS * j, 128)
            merged = None
            for f in range(FIELDS):
                piece = slabs[f][:, 128 * tile:128 * tile + 128]
                if shift + BASIS > 128:
                    piece = jnp.where(lane >= shift, piece, slabs[f][:, 128 * tile + 128:128 * tile + 256])
                turn = (32 * f - shift) % 128
                piece = pltpu.roll(piece, turn, 1) if turn else piece
                merged = piece if f == 0 else jnp.where(lane >= 32 * f, piece, merged)
            high, low = split(merged)
            columns.append(jnp.concatenate([high, low, high], axis=0))
        for j in range(begin, end, 2):
            result = product(first, jnp.concatenate(columns[j - begin:j - begin + 2], axis=1))
            for n in range(min(2, end - j)):
                outer[j + n] = result[:, 128 * n:128 * n + 128]

    first_stage(0, 14)
    loaded(5, 6, 7, 8, 9)

    def step(t, carry):
        def scalar(table, bb, m):
            return middle_ref[t, 32 * table + 4 * bb + m]

        window = [outer[2 * t + m] for m in range(5)]
        values = [w[0:SLAB] for w in window]
        slopes = [w[SLAB:2 * SLAB] for w in window]

        def middle_sum(table, parts, bb):
            e = bb // 4
            out = scalar(table, bb, 0) * parts[e]
            for m in range(1, 4):
                out = out + scalar(table, bb, m) * parts[e + m]
            return out

        def pair_sides(x):
            lane = lanes_of(x.shape[0])
            high = x.astype(jnp.bfloat16)
            wide = high.astype(jnp.float32)
            low = x - wide
            turned = pltpu.roll(wide, 64, 1)
            even = jnp.where(lane < 64, low, turned).astype(jnp.bfloat16)
            odd = jnp.where(lane < 64, turned, low).astype(jnp.bfloat16)
            return jnp.concatenate([high, even], axis=1), jnp.concatenate([high, odd], axis=1)

        def weights(ref):
            lane = lanes_of(SLAB)
            tiles = [ref[:, pl.ds(pl.multiple_of(768 * t + 128 * n, 128), 128)] for n in range(6)]
            parts = []
            for bb in range(8):
                tile, shift = divmod(QUAD * bb, 128)
                part = tiles[tile]
                if shift + QUAD > 128:
                    part = jnp.where(lane >= shift, part, tiles[tile + 1])
                parts.append(pltpu.roll(part, 128 - shift, 1) if shift else part)
            return jnp.concatenate(parts, axis=0)

        s = weights(stiff)
        w = weights(volume)
        def adjoint(parts, table):
            pairs = [split(p) for p in parts]
            sides = [p[0] for p in pairs[:FIELDS]] + [p[1] for p in pairs[:FIELDS]]
            for pair in pairs[FIELDS:]:
                sides.extend(pair)
            wide = product(jnp.concatenate(sides, axis=1), table[...])
            return wide[:, 0:128] + wide[:, 128:256]

        def gradient(table, parts, at):
            even, odd = pair_sides(jnp.concatenate([middle_sum(table, parts, bb) for bb in range(8)], axis=0))
            first, second = product(even, inner_ref[at]), product(odd, inner_ref[at + 1])
            return [first[:, 0:128], first[:, 128:256], second[:, 0:128], second[:, 128:256]], odd

        along, odd = gradient(0, values, 2)
        pressed = w * product(odd, plain_ref[...])
        spill = along[2]
        heads = [None] * 3
        for d in range(2):
            grads, _ = gradient(d, values if d else slopes, 0)
            spill = spill + grads[d]
            heads[d] = adjoint([s * g - pressed if f == d else s * g for f, g in enumerate(grads)], adj_value_ref)
        heads[2] = adjoint([s * g - pressed if f == 2 else s * g for f, g in enumerate(along)] + [w * spill],
                           adj_slope_ref)
        heads = [[h[SLAB * bb:SLAB * bb + SLAB] for bb in range(8)] for h in heads]
        sums = [[None, None] for _ in range(5)]
        for bb in range(8):
            for m in range(4):
                at = bb // 4 + m
                v = scalar(2, bb, m)
                terms = [v * heads[0][bb], scalar(3, bb, m) * heads[1][bb] + v * heads[2][bb]]
                sums[at] = [a if b is None else b + a for a, b in zip(terms, sums[at])]
        for m in range(5):
            total[2 * t + m] += jnp.concatenate(sums[m], axis=0)
        return carry

    last = last_ref[...]

    def last_stage(half):
        lane = lanes_of(16)
        packed = [[jnp.zeros((16, 128), jnp.float32) for _ in range(3)] for _ in range(FIELDS)]
        begin, end = (0, 15) if half == 0 else (14, BASIS)
        for j0 in range(begin, end, 2):
            some = list(range(j0, min(j0 + 2, end)))
            columns = []
            for j in some:
                high, low = split(total[j])
                columns.append(jnp.concatenate([high, low, high], axis=0))
            result = product(last, jnp.concatenate(columns, axis=1))
            for n, j in enumerate(some):
                piece = result[:, 128 * n:128 * n + 128]
                tile, shift = divmod(BASIS * j, 128)
                stop = shift + BASIS
                at = tile - 3 * half
                for f in range(FIELDS):
                    turn = (shift - 32 * f) % 128
                    turned = pltpu.roll(piece, turn, 1) if turn else piece
                    if 0 <= at < 3:
                        packed[f][at] = jnp.where((lane >= shift) & (lane < stop), turned, packed[f][at])
                    if stop > 128 and 0 <= at + 1 < 3:
                        packed[f][at + 1] = jnp.where(lane < stop - 128, turned, packed[f][at + 1])
        for f in range(FIELDS):
            for n in range(3):
                back[half, f, :, 128 * n:128 * n + 128] = packed[f][n][0:8]
                back[half, f, n:n + 1, 384:512] = packed[f][n][8:9]
        sums_home[half][0]()

    lax.fori_loop(0, 4, step, 0, unroll=4)
    layers[1][1]()
    first_stage(14, BASIS)
    finish_traces()
    high, low = split(trace_all[...].reshape(64, 384))
    both = (route + pltpu.roll(route, 64, 1)).astype(jnp.bfloat16)
    trace_out[...] = product(both, jnp.concatenate([high, low], axis=0)).reshape(8, 16, 384)
    start_picked()
    trace_in[group] = trace_out[group]
    finish_fixes()
    high, low = split(fix_all[...].reshape(128, 384))
    flipped = route.T.astype(jnp.bfloat16)[0:64]
    fix_out[...] = product(jnp.concatenate([flipped, flipped], axis=1),
                           jnp.concatenate([high, low], axis=0)).reshape(8, 8, 384)
    start_sums()
    fix_in[z] = fix_out[z]
    lax.fori_loop(4, 8, step, 0, unroll=4)
    last_stage(0)
    lax.fori_loop(8, STEPS, step, 0, unroll=4)
    last_stage(1)
    finish_picked()
    picked = trace_in[0]
    for at in range(1, 8):
        picked = picked + trace_in[at]
    to_matrices([picked[8 * h:8 * h + 8, 128 * n:128 * n + 128] for h in range(2) for n in range(3)], grid)
    jumps = []
    for k in range(8):
        jump = exact(grid[pl.ds(k, BASIS, stride=8), :][:, 0:BASIS], rights[k], ((1,), (1,)))
        jumps.append(exact(lefts[k], jump, ((1,), (0,))))
    for slot in range(4):
        grid[pl.ds(slot, BASIS, stride=8), :] = jnp.concatenate(
            [jumps[slot] - jumps[4 + slot], jnp.zeros((BASIS, 128 - BASIS), jnp.float32)], axis=1)
    jump_rows = jnp.concatenate(to_rows(lambda i: grid[8 * i:8 * i + 8, :], 8), axis=1)
    for slot in range(4):
        jump_ref[slot, 0] = jump_rows[slot:slot + 1, 0:729]
    finish_sums()
    sums = fix_in[0]
    for at in range(1, 8):
        sums = sums + fix_in[at]
    sums = [sums[4 * h:4 * h + 4, 128 * n:128 * n + 128] for h in range(2) for n in range(3)]
    to_matrices(sums, grid)
    lane = lanes_of(BASIS)
    inside = lane < BASIS
    near = jnp.where(inside, grid[pl.ds(2, BASIS, stride=8), :], 0.0)
    far = jnp.where(inside, grid[pl.ds(3, BASIS, stride=8), :], 0.0)
    far = pltpu.roll(far, 62, 1)
    ends = jnp.concatenate(sums, axis=1)
    sums_home[0][1]()
    sums_home[1][1]()
    x_ref[...] = jnp.zeros((BASIS, BASIS * BASIS), jnp.float32)
    for q in range(SUBS):
        layers_q = jnp.concatenate([slab_layers(home, half, q) for half in range(2)], axis=1)
        x_ref[6 * q:6 * q + LAYERS, :] += layers_q[0:LAYERS, 0:729]
    for s in range(2):
        x_ref[26 * s:26 * s + 1, :] += ends[s:s + 1, 0:729]
    x_ref[:, 0:128] += near
    x_ref[:, 640:729] += far[:, 0:89]
    out_ref[0, 0, :, 0, :] = x_ref[...]


def store_kernel(result, jumps, result_hbm, jumps_hbm, sems):
    copies = [pltpu.make_async_copy(result, result_hbm, sems.at[0]), pltpu.make_async_copy(jumps, jumps_hbm, sems.at[1])]
    for copy in copies:
        copy.start()
    for copy in copies:
        copy.wait()


def per_device(state, stiff_weight, volume_weight, lagrange, mortar, links):
    vmem = pl.BlockSpec(memory_space=pltpu.VMEM)
    anywhere = pl.BlockSpec(memory_space=pl.ANY)
    constants = constant_tables()
    local = [x.shape[1:] if n < 2 else x.shape for n, x in enumerate(constants)]
    result, jumps = pl.pallas_call(
        operator_kernel,
        name="operator",
        out_shape=(jax.ShapeDtypeStruct((1, 1, BASIS, 1, BASIS * BASIS), jnp.float32),
                   jax.ShapeDtypeStruct(lagrange.shape, jnp.float32)),
        in_specs=[anywhere] * 13,
        out_specs=(vmem, vmem),
        scratch_shapes=[
            pltpu.VMEM((BASIS, BASIS * BASIS), jnp.float32),
            pltpu.VMEM(lagrange.shape, jnp.float32),
            pltpu.VMEM(mortar.shape, jnp.float32),
            pltpu.VMEM((6, 256), jnp.int32),
            pltpu.SMEM((6, 256), jnp.int32),
            *[pltpu.VMEM(shape, jnp.bfloat16) for shape in local[:-1]],
            pltpu.SMEM(local[-1], jnp.float32),
            pltpu.VMEM((SLAB, QUAD * QUAD), jnp.float32),
            pltpu.VMEM((SLAB, QUAD * QUAD), jnp.float32),
            pltpu.VMEM((2, SUBS, 8, 512), jnp.float32),
            pltpu.VMEM((2, SUBS, 8, 512), jnp.float32),
            pltpu.VMEM((2, SUBS, 8, 512), jnp.float32),
            pltpu.VMEM((2, SUBS, 8, 512), jnp.float32),
            pltpu.VMEM((BASIS, 2 * SLAB, 128), jnp.float32),
            pltpu.VMEM((BASIS, 2 * SLAB, 128), jnp.float32),
            pltpu.VMEM((BASIS * 8, 128), jnp.float32),
            pltpu.VMEM((8, 384), jnp.float32),
            pltpu.VMEM((8, 8, 384), jnp.float32),
            pltpu.VMEM((8, 16, 384), jnp.float32),
            pltpu.VMEM((8, 16, 384), jnp.float32),
            pltpu.VMEM((16, 384), jnp.float32),
            pltpu.VMEM((8, 16, 384), jnp.float32),
            pltpu.VMEM((8, 8, 384), jnp.float32),
            pltpu.VMEM((8, 8, 384), jnp.float32),
            pltpu.SemaphoreType.DMA((11,)),
            pltpu.SemaphoreType.DMA((2, SUBS)),
            pltpu.SemaphoreType.DMA((2, SUBS)),
            pltpu.SemaphoreType.DMA((2, SUBS)),
            pltpu.SemaphoreType.DMA((2, SUBS)),
            pltpu.SemaphoreType.DMA((4, 8)),
            pltpu.SemaphoreType.DMA((4, 8)),
        ],
        compiler_params=pltpu.CompilerParams(collective_id=0, has_side_effects=True, vmem_limit_bytes=54 * 10**6),
        cost_estimate=pl.CostEstimate(flops=10**10, bytes_accessed=4 * 10**6, transcendentals=0),
    )(*[pltpu.with_memory_space_constraint(x, pltpu.HBM) for x in (
        jnp.transpose(state, (0, 1, 3, 2, 4)), stiff_weight, volume_weight, lagrange,
        jnp.transpose(mortar, (0, 1, 3, 2, 4)), links.T, *constants)])
    result, jumps = pl.pallas_call(
        store_kernel,
        name="store",
        out_shape=(jax.ShapeDtypeStruct(result.shape, jnp.float32), jax.ShapeDtypeStruct(jumps.shape, jnp.float32)),
        in_specs=[vmem, vmem],
        out_specs=(anywhere, anywhere),
        scratch_shapes=[pltpu.SemaphoreType.DMA((2,))],
        compiler_params=pltpu.CompilerParams(vmem_limit_bytes=2 * 10**6),
    )(result, jumps)
    return jnp.transpose(result, (0, 1, 3, 2, 4)), jumps


def solution(mesh):
    return jax.shard_map(
        per_device,
        mesh=mesh,
        in_specs=(
            P("patch", "sub", None, None, None),
            P("patch", None, None),
            P("patch", None, None),
            P("patch", "sub", None, None),
            P("patch", None, None, None, None),
            P(),
        ),
        out_specs=(P("patch", "sub", None, None, None), P("patch", "sub", None, None)),
        check_vma=False,
    )
```

```python
import jax
import jax.numpy as jnp
import numpy as np
from jax import lax
from jax.experimental import pallas as pl
from jax.experimental.pallas import tpu as pltpu
from jax.sharding import PartitionSpec as P

ELEMS = 24
DEGREE = 3
FIELDS = 4
BASIS = 27
QUAD = 96
SUBS = 4
SLAB = QUAD // SUBS
LAYERS = SLAB // 4 + DEGREE
STEPS = 12
MESH = pl.DeviceIdType.MESH

stabilize = 0.25
highest = lax.Precision.HIGHEST
gauss_points_four = [
    -0.8611363115940526,
    -0.3399810435848563,
    0.3399810435848563,
    0.8611363115940526,
]
gauss_weights_four = [
    0.3478548451374538,
    0.6521451548625461,
    0.6521451548625461,
    0.3478548451374538,
]


def spline_tables(elements, degree):
    knot_list = np.concatenate(
        [np.zeros(degree), np.arange(elements + 1.0), np.full(degree, float(elements))]
    )
    gauss_nodes = np.array(gauss_points_four)
    gauss_weights = np.array(gauss_weights_four)
    points = (np.arange(elements)[:, None] + (gauss_nodes[None, :] + 1.0) / 2.0).reshape(-1)
    point_weights = np.tile(gauss_weights / 2.0, elements)
    current = np.where(
        (knot_list[None, :-1] <= points[:, None]) & (points[:, None] < knot_list[None, 1:]),
        1.0,
        0.0,
    )
    previous = current
    for order_k in range(1, degree + 1):
        previous = current
        amount = len(knot_list) - 1 - order_k
        current = np.zeros((points.shape[0], amount))
        for column in range(amount):
            left_span = knot_list[column + order_k] - knot_list[column]
            right_span = knot_list[column + order_k + 1] - knot_list[column + 1]
            if left_span > 0:
                current[:, column] += (points - knot_list[column]) / left_span * previous[:, column]
            if right_span > 0:
                current[:, column] += (
                    (knot_list[column + order_k + 1] - points)
                    / right_span
                    * previous[:, column + 1]
                )
    slope_part = np.zeros(current.shape)
    for column in range(current.shape[1]):
        left_span = knot_list[column + degree] - knot_list[column]
        right_span = knot_list[column + degree + 1] - knot_list[column + 1]
        if left_span > 0:
            slope_part[:, column] += degree / left_span * previous[:, column]
        if right_span > 0:
            slope_part[:, column] -= degree / right_span * previous[:, column + 1]
    return (
        current.astype(np.float32),
        slope_part.astype(np.float32),
        (current * point_weights[:, None]).astype(np.float32),
        (slope_part * point_weights[:, None]).astype(np.float32),
    )


def halves(table):
    high = table.astype(jnp.bfloat16).astype(np.float32)
    low = (table - high).astype(jnp.bfloat16).astype(np.float32)
    return high, low


def constant_tables():
    value, slope, value_w, slope_w = spline_tables(ELEMS, DEGREE)
    first = np.zeros((SUBS, 2 * SLAB, 16), np.float32)
    last = np.zeros((SUBS, 16, 2 * SLAB), np.float32)
    for q in range(SUBS):
        rows = slice(SLAB * q, SLAB * (q + 1))
        cols = slice(6 * q, 6 * q + LAYERS)
        first[q, :SLAB, :LAYERS] = value[rows, cols]
        first[q, SLAB:, :LAYERS] = slope[rows, cols]
        last[q, :LAYERS, :SLAB] = slope_w[rows, cols].T
        last[q, :LAYERS, SLAB:] = value_w[rows, cols].T
    high, low = halves(first)
    first = np.concatenate([high, high, low], axis=2)
    high, low = halves(last)
    last = np.concatenate([high, high, low], axis=2)

    def pair_tables(table):
        high, low = halves(table)
        even = np.zeros((256, 256), np.float32)
        odd = np.zeros((256, 256), np.float32)
        for s in range(2):
            cols = slice(128 * s, 128 * s + QUAD)
            even[32 * s:32 * s + BASIS, cols] = high.T
            even[128 + 32 * s:128 + 32 * s + BASIS, cols] = high.T
            even[192 + 32 * s:192 + 32 * s + BASIS, cols] = low.T
            odd[64 + 32 * s:64 + 32 * s + BASIS, cols] = high.T
            odd[128 + 32 * s:128 + 32 * s + BASIS, cols] = low.T
            odd[192 + 32 * s:192 + 32 * s + BASIS, cols] = high.T
        return even, odd

    value_even, value_odd = pair_tables(value)
    slope_even, slope_odd = pair_tables(slope)
    inner = np.stack([value_even, value_odd, slope_even, slope_odd])
    plain = value_odd[:, 128:]

    def adjoint_table(table, spilled=None):
        high, low = halves(table)
        out = np.zeros((1024, 256), np.float32)
        for f in range(FIELDS):
            scale = -stabilize if f == FIELDS - 1 else 1.0
            rows = slice(128 * f, 128 * f + QUAD)
            out[rows, 32 * f:32 * f + BASIS] = scale * high
            out[rows, 128 + 32 * f:128 + 32 * f + BASIS] = scale * low
            out[512 + 128 * f:512 + 128 * f + QUAD, 32 * f:32 * f + BASIS] = scale * high
        if spilled is None:
            return out
        high, low = halves(spilled)
        more = np.zeros((256, 256), np.float32)
        more[:QUAD, 96:96 + BASIS] = -high
        more[:QUAD, 224:224 + BASIS] = -low
        more[128:128 + QUAD, 96:96 + BASIS] = -high
        return np.concatenate([out, more])

    adjoint_value = adjoint_table(value_w)
    adjoint_slope = adjoint_table(slope_w, value_w)
    middle = np.zeros((STEPS, 128), np.float32)
    for t in range(STEPS):
        for bb in range(8):
            point = 8 * t + bb
            for m in range(4):
                col = 2 * t + bb // 4 + m
                for n, table in enumerate((value, slope, value_w, slope_w)):
                    middle[t, 32 * n + 4 * bb + m] = table[point, col]
    half = lambda x: jnp.asarray(x, jnp.bfloat16)
    return (half(first), half(last), half(inner), half(plain), half(adjoint_value), half(adjoint_slope),
            jnp.asarray(middle, jnp.float32))


def split(x):
    high = x.astype(jnp.bfloat16)
    return high, (x - high.astype(jnp.float32)).astype(jnp.bfloat16)


def product(left, right):
    return jnp.dot(left, right, preferred_element_type=jnp.float32)


def lanes_of(rows):
    return lax.broadcasted_iota(jnp.int32, (rows, 128), 1)


def exact(left, right, dims):
    return lax.dot_general(left, right, (dims, ((), ())), precision=highest, preferred_element_type=jnp.float32)


def to_matrices(tiles, grid):
    for i in range(BASIS):
        tile, shift = divmod(BASIS * i, 128)
        piece = tiles[tile]
        if shift + BASIS > 128:
            piece = jnp.where(lanes_of(piece.shape[0]) >= shift, piece, tiles[tile + 1])
        grid[8 * i:8 * i + piece.shape[0], :] = pltpu.roll(piece, 128 - shift, 1) if shift else piece


def to_rows(row_of, count):
    lane = lanes_of(count)
    tiles = [jnp.zeros((count, 128), jnp.float32) for _ in range(6)]
    for i in range(BASIS):
        tile, shift = divmod(BASIS * i, 128)
        piece = row_of(i)
        piece = pltpu.roll(piece, shift, 1) if shift else piece
        end = shift + BASIS
        tiles[tile] = jnp.where((lane >= shift) & (lane < end), piece, tiles[tile])
        if end > 128:
            tiles[tile + 1] = jnp.where(lane < end - 128, piece, tiles[tile + 1])
    return tiles


def slab_layers(ref, half, at):
    first = lax.broadcasted_iota(jnp.int32, (8, 384), 0) == 0
    line = jnp.concatenate([ref[half, at, n:n + 1, 384:512] for n in range(3)], axis=1)
    return jnp.concatenate([ref[half, at, :, 0:384], jnp.where(first, line, 0.0)], axis=0)


def routing(links_ref, y, z, core):
    row = lax.broadcasted_iota(jnp.int32, (128, 256), 0)
    col = lax.broadcasted_iota(jnp.int32, (128, 256), 1)
    source = ((row // 32) * 16 + 2 * z + (row // 16) % 2) * 4 + row % 4
    order = jnp.where(col == source, 1.0, 0.0).astype(jnp.bfloat16)
    table = links_ref[...].astype(jnp.float32).astype(jnp.bfloat16)
    found = lax.dot_general(order, table, (((1,), (1,)), ((), ())), preferred_element_type=jnp.float32)
    row = lax.broadcasted_iota(jnp.int32, (128, 1), 0)
    second = (row // 4) % 2 == 1
    patch = jnp.where(second, found[:, 1:2], found[:, 0:1])
    face = jnp.where(second, found[:, 3:4], found[:, 2:3])
    patch = jnp.where(found[:, 4:5] > 0.0, patch, -1.0)
    lane = lanes_of(128)
    row = lax.broadcasted_iota(jnp.int32, (128, 128), 0)
    wanted = (16 * y + 2 * (lane // 8) + core).astype(jnp.float32)
    same = (patch == wanted) & (face == (lane % 4).astype(jnp.float32))
    same = same & ((lane // 4) % 2 == (row // 8) % 2) & (lane < 64)
    return jnp.where(same, 1.0, 0.0)


def operator_kernel(x_hbm, stiff_hbm, volume_hbm, lagrange_hbm, mortar_hbm, links_hbm, first_hbm, last_hbm,
                    inner_hbm, plain_hbm, adj_value_hbm, adj_slope_hbm, middle_hbm, out_ref, jump_ref,
                    x_ref, lagrange_ref, mortar_ref, links_ref, counts_ref, first_ref, last_ref, inner_ref,
                    plain_ref, adj_value_ref, adj_slope_ref, middle_ref, stiff, volume, sent, got, back, home, outer, total, picks, grid, trace_own, trace_all,
                    trace_out, trace_in, fix_own, fix_all, fix_out, fix_in, load_sem, send_sem, recv_sem,
                    back_send_sem, back_recv_sem, face_send_sem, face_recv_sem):
    load_x = pltpu.make_async_copy(x_hbm.at[0, 0, :, 0, :], x_ref, load_sem.at[0])
    load_x.start()
    me = lax.axis_index("sub")
    patch = lax.axis_index("patch")
    y, z, core = patch // 16, (patch // 2) % 8, patch % 2
    group = 2 * y + core
    line = [lax.rem(z + d, 8) for d in range(8)]
    line_from = [lax.rem(z + 8 - d, 8) for d in range(8)]
    plane = [lax.rem(group + d, 8) for d in range(8)]
    plane_from = [lax.rem(group + 8 - d, 8) for d in range(8)]
    line_ids = [{"patch": 16 * y + 2 * at + core} for at in line]
    plane_ids = [{"patch": 16 * (at // 2) + 2 * z + at % 2} for at in plane]

    def exchange(n, source, target, slot, slots_from, ids):
        def one(d, at):
            return pltpu.make_async_remote_copy(
                src_ref=source(d), dst_ref=target.at[at], send_sem=face_send_sem.at[n, d],
                recv_sem=face_recv_sem.at[n, d], device_id=ids[d], device_id_type=MESH)

        def start():
            for d in range(1, 8):
                one(d, slot).start()

        def finish():
            for d in range(1, 8):
                one(d, slot).wait_send()
                one(d, slots_from[d]).wait_recv()

        return start, finish

    peers = [lax.rem(me + d, SUBS) for d in range(SUBS)]
    origins = [lax.rem(me + SUBS - d, SUBS) for d in range(SUBS)]
    barrier = pltpu.get_barrier_semaphore()
    for d in (4, 3, 5, 2, 6, 1, 7):
        pl.semaphore_signal(barrier, inc=1, device_id=line_ids[d], device_id_type=MESH)
    for d in range(1, SUBS):
        pl.semaphore_signal(barrier, inc=1, device_id={"sub": peers[d]}, device_id_type=MESH)
    for d in range(1, 8):
        pl.semaphore_signal(barrier, inc=1, device_id=plane_ids[d], device_id_type=MESH)
    rows = pl.ds(pl.multiple_of(me * SLAB, 8), SLAB)
    pairs = [(slot, s, n) for slot in range(4) for s in range(2) for n in range(2)]
    loads = [
        [(links_hbm, links_ref)],
        [(links_hbm, counts_ref)],
        [(lagrange_hbm, lagrange_ref)],
        [(mortar_hbm.at[slot, s, :, n, :], mortar_ref.at[slot, s, n]) for slot, s, n in pairs],
        [(first_hbm.at[me], first_ref)],
        [(middle_hbm, middle_ref)],
        [(inner_hbm, inner_ref), (plain_hbm, plain_ref)],
        [(stiff_hbm.at[0, rows], stiff), (volume_hbm.at[0, rows], volume)],
        [(adj_value_hbm, adj_value_ref), (adj_slope_hbm, adj_slope_ref)],
        [(last_hbm.at[me], last_ref)],
    ]
    loads = [[pltpu.make_async_copy(a, b, load_sem.at[1 + n]) for a, b in some] for n, some in enumerate(loads)]
    for some in loads:
        for copy in some:
            copy.start()

    def loaded(*which):
        for n in which:
            for copy in loads[n]:
                copy.wait()

    load_x.wait()
    sent[...] = jnp.zeros_like(sent)
    for half in range(2):
        for q in range(SUBS):
            width = min(384, 729 - 384 * half)
            sent[half, q, :, 0:width] = x_ref[6 * q:6 * q + 8, 384 * half:384 * half + width]
            for n in range(3):
                lane = 384 * half + 128 * n
                width = min(128, 729 - lane)
                sent[half, q, n:n + 1, 384:384 + width] = x_ref[6 * q + 8:6 * q + 9, lane:lane + width]
    trace_rows = [[x_ref[26 * s:26 * s + 1, 128 * n:min(128 * n + 128, 729)] for n in range(6)] for s in range(2)]
    for s in range(2):
        tail = jnp.zeros((1, 768 - 729), jnp.float32)
        trace_rows[s][5] = jnp.concatenate([trace_rows[s][5], tail], axis=1)
    edge = x_ref[:, 0:128]
    trace_rows.append(to_rows(lambda i: edge[i:i + 1, :], 1))
    edge = jnp.concatenate([x_ref[:, 640:729], jnp.zeros((BASIS, 39), jnp.float32)], axis=1)
    edge = pltpu.roll(edge, 128 - 62, 1)
    trace_rows.append(to_rows(lambda i: edge[i:i + 1, :], 1))
    for h in range(2):
        for f in range(4):
            for n in range(3):
                trace_own[4 * h + f:4 * h + f + 1, 128 * n:128 * n + 128] = trace_rows[f][3 * h + n]
    start_traces, finish_traces = exchange(0, lambda d: trace_own, trace_all, z, line_from, line_ids)
    start_picked, finish_picked = exchange(1, lambda d: trace_out.at[plane[d]], trace_in, group, plane_from, plane_ids)
    start_fixes, finish_fixes = exchange(2, lambda d: fix_own, fix_all, group, plane_from, plane_ids)
    start_sums, finish_sums = exchange(3, lambda d: fix_out.at[line[d]], fix_in, z, line_from, line_ids)
    pl.semaphore_wait(barrier, SUBS - 1 + 14)
    def sub_exchange(half, source, target, send, recv):
        def one(d, at):
            return pltpu.make_async_remote_copy(
                src_ref=source.at[half, peers[d]], dst_ref=target.at[half, at], send_sem=send.at[half, d],
                recv_sem=recv.at[half, d], device_id={"sub": peers[d]}, device_id_type=MESH)

        def start():
            for d in range(1, SUBS):
                one(d, me).start()
            target[half, me] = source[half, me]

        def finish():
            for d in range(1, SUBS):
                one(d, me).wait_send()
                one(d, origins[d]).wait_recv()

        return start, finish

    layers = [sub_exchange(half, sent, got, send_sem, recv_sem) for half in range(2)]
    sums_home = [sub_exchange(half, back, home, back_send_sem, back_recv_sem) for half in range(2)]
    layers[0][0]()
    layers[1][0]()
    start_traces()
    trace_all[z] = trace_own[...]
    loaded(0, 1, 2, 3)
    row = lax.broadcasted_iota(jnp.int32, (BASIS, BASIS), 0)
    lefts, rights = [], []
    for s in range(2):
        for slot in range(4):
            at = 4 * patch + slot
            lefts.append(jnp.where(row < counts_ref[4, at], mortar_ref[slot, s, 0], 0.0))
            rights.append(jnp.where(row < counts_ref[5, at], mortar_ref[slot, s, 1], 0.0))
    multipliers = jnp.concatenate([lagrange_ref[slot, 0] for slot in range(4)], axis=0)
    multipliers = jnp.concatenate([multipliers, jnp.zeros((4, 768 - 729), jnp.float32)], axis=1)
    to_matrices([multipliers[:, 128 * n:128 * n + 128] for n in range(6)], grid)
    given = [grid[pl.ds(slot, BASIS, stride=8), :][:, 0:BASIS] for slot in range(4)]
    for k in range(8):
        fix = exact(given[k % 4], rights[k], ((1,), (0,)))
        fix = exact(lefts[k], fix, ((0,), (0,)))
        fix = fix if k < 4 else -fix
        grid[pl.ds(k, BASIS, stride=8), :] = jnp.concatenate(
            [fix, jnp.zeros((BASIS, 128 - BASIS), jnp.float32)], axis=1)
    fix_rows = to_rows(lambda i: grid[8 * i:8 * i + 8, :], 8)
    for h in range(2):
        for n in range(3):
            fix_own[8 * h:8 * h + 8, 128 * n:128 * n + 128] = fix_rows[3 * h + n]
    start_fixes()
    fix_all[group] = fix_own[...]
    route = routing(links_ref, y, z, core)
    picks[0] = (route + pltpu.roll(route, 64, 1)).astype(jnp.bfloat16)
    flipped = route.T.astype(jnp.bfloat16)[0:64]
    flipped = jnp.concatenate([flipped, flipped], axis=1)
    picks[1] = jnp.concatenate([flipped[:, 0:128], flipped[:, 128:256]], axis=0)
    total[...] = jnp.zeros_like(total)
    layers[0][1]()
    loaded(4)
    first = first_ref[...]

    def first_stage(begin, end):
        slabs = [jnp.concatenate([slab_layers(got, half, f) for half in range(1 + (end > 14))], axis=1)
                 for f in range(FIELDS)]
        lane = lanes_of(16)
        columns = []
        for j in range(begin, end):
            tile, shift = divmod(BASIS * j, 128)
            merged = None
            for f in range(FIELDS):
                piece = slabs[f][:, 128 * tile:128 * tile + 128]
                if shift + BASIS > 128:
                    piece = jnp.where(lane >= shift, piece, slabs[f][:, 128 * tile + 128:128 * tile + 256])
                turn = (32 * f - shift) % 128
                piece = pltpu.roll(piece, turn, 1) if turn else piece
                merged = piece if f == 0 else jnp.where(lane >= 32 * f, piece, merged)
            high, low = split(merged)
            columns.append(jnp.concatenate([high, low, high], axis=0))
        for j in range(begin, end, 2):
            result = product(first, jnp.concatenate(columns[j - begin:j - begin + 2], axis=1))
            for n in range(min(2, end - j)):
                outer[j + n] = result[:, 128 * n:128 * n + 128]

    first_stage(0, 14)
    loaded(5, 6, 7, 8, 9)

    def step(t, carry):
        def scalar(table, bb, m):
            return middle_ref[t, 32 * table + 4 * bb + m]

        window = [outer[2 * t + m] for m in range(5)]
        values = [w[0:SLAB] for w in window]
        slopes = [w[SLAB:2 * SLAB] for w in window]

        def middle_sum(table, parts, bb):
            e = bb // 4
            out = scalar(table, bb, 0) * parts[e]
            for m in range(1, 4):
                out = out + scalar(table, bb, m) * parts[e + m]
            return out

        def pair_sides(x):
            lane = lanes_of(x.shape[0])
            high = x.astype(jnp.bfloat16)
            wide = high.astype(jnp.float32)
            low = x - wide
            turned = pltpu.roll(wide, 64, 1)
            even = jnp.where(lane < 64, low, turned).astype(jnp.bfloat16)
            odd = jnp.where(lane < 64, turned, low).astype(jnp.bfloat16)
            return jnp.concatenate([high, even], axis=1), jnp.concatenate([high, odd], axis=1)

        def weights(ref):
            lane = lanes_of(SLAB)
            tiles = [ref[:, pl.ds(pl.multiple_of(768 * t + 128 * n, 128), 128)] for n in range(6)]
            parts = []
            for bb in range(8):
                tile, shift = divmod(QUAD * bb, 128)
                part = tiles[tile]
                if shift + QUAD > 128:
                    part = jnp.where(lane >= shift, part, tiles[tile + 1])
                parts.append(pltpu.roll(part, 128 - shift, 1) if shift else part)
            return jnp.concatenate(parts, axis=0)

        s = weights(stiff)
        w = weights(volume)
        def adjoint(parts, table):
            pairs = [split(p) for p in parts]
            sides = [p[0] for p in pairs[:FIELDS]] + [p[1] for p in pairs[:FIELDS]]
            for pair in pairs[FIELDS:]:
                sides.extend(pair)
            wide = product(jnp.concatenate(sides, axis=1), table[...])
            return wide[:, 0:128] + wide[:, 128:256]

        def gradient(table, parts, at):
            even, odd = pair_sides(jnp.concatenate([middle_sum(table, parts, bb) for bb in range(8)], axis=0))
            first, second = product(even, inner_ref[at]), product(odd, inner_ref[at + 1])
            return [first[:, 0:128], first[:, 128:256], second[:, 0:128], second[:, 128:256]], odd

        along, odd = gradient(0, values, 2)
        pressed = w * product(odd, plain_ref[...])
        spill = along[2]
        heads = [None] * 3
        for d in range(2):
            grads, _ = gradient(d, values if d else slopes, 0)
            spill = spill + grads[d]
            heads[d] = adjoint([s * g - pressed if f == d else s * g for f, g in enumerate(grads)], adj_value_ref)
        heads[2] = adjoint([s * g - pressed if f == 2 else s * g for f, g in enumerate(along)] + [w * spill],
                           adj_slope_ref)
        heads = [[h[SLAB * bb:SLAB * bb + SLAB] for bb in range(8)] for h in heads]
        sums = [[None, None] for _ in range(5)]
        for bb in range(8):
            for m in range(4):
                at = bb // 4 + m
                v = scalar(2, bb, m)
                terms = [v * heads[0][bb], scalar(3, bb, m) * heads[1][bb] + v * heads[2][bb]]
                sums[at] = [a if b is None else b + a for a, b in zip(terms, sums[at])]
        for m in range(5):
            total[2 * t + m] += jnp.concatenate(sums[m], axis=0)
        return carry

    last = last_ref[...]

    def last_stage(half):
        lane = lanes_of(16)
        packed = [[jnp.zeros((16, 128), jnp.float32) for _ in range(3)] for _ in range(FIELDS)]
        begin, end = (0, 15) if half == 0 else (14, BASIS)
        for j0 in range(begin, end, 2):
            some = list(range(j0, min(j0 + 2, end)))
            columns = []
            for j in some:
                high, low = split(total[j])
                columns.append(jnp.concatenate([high, low, high], axis=0))
            result = product(last, jnp.concatenate(columns, axis=1))
            for n, j in enumerate(some):
                piece = result[:, 128 * n:128 * n + 128]
                tile, shift = divmod(BASIS * j, 128)
                stop = shift + BASIS
                at = tile - 3 * half
                for f in range(FIELDS):
                    turn = (shift - 32 * f) % 128
                    turned = pltpu.roll(piece, turn, 1) if turn else piece
                    if 0 <= at < 3:
                        packed[f][at] = jnp.where((lane >= shift) & (lane < stop), turned, packed[f][at])
                    if stop > 128 and 0 <= at + 1 < 3:
                        packed[f][at + 1] = jnp.where(lane < stop - 128, turned, packed[f][at + 1])
        for f in range(FIELDS):
            for n in range(3):
                back[half, f, :, 128 * n:128 * n + 128] = packed[f][n][0:8]
                back[half, f, n:n + 1, 384:512] = packed[f][n][8:9]
        sums_home[half][0]()

    lax.fori_loop(0, 4, step, 0, unroll=4)
    layers[1][1]()
    finish_traces()
    high, low = split(trace_all[...].reshape(64, 384))
    trace_out[...] = product(picks[0], jnp.concatenate([high, low], axis=0)).reshape(8, 16, 384)
    start_picked()
    trace_in[group] = trace_out[group]
    finish_fixes()
    high, low = split(fix_all[...].reshape(128, 384))
    fix_out[...] = product(jnp.concatenate([picks[1, 0:64], picks[1, 64:128]], axis=1),
                           jnp.concatenate([high, low], axis=0)).reshape(8, 8, 384)
    start_sums()
    fix_in[z] = fix_out[z]
    first_stage(14, BASIS)
    lax.fori_loop(4, 8, step, 0, unroll=4)
    last_stage(0)
    lax.fori_loop(8, STEPS, step, 0, unroll=4)
    last_stage(1)
    finish_picked()
    picked = trace_in[0]
    for at in range(1, 8):
        picked = picked + trace_in[at]
    to_matrices([picked[8 * h:8 * h + 8, 128 * n:128 * n + 128] for h in range(2) for n in range(3)], grid)
    jumps = []
    for k in range(8):
        jump = exact(grid[pl.ds(k, BASIS, stride=8), :][:, 0:BASIS], rights[k], ((1,), (1,)))
        jumps.append(exact(lefts[k], jump, ((1,), (0,))))
    for slot in range(4):
        grid[pl.ds(slot, BASIS, stride=8), :] = jnp.concatenate(
            [jumps[slot] - jumps[4 + slot], jnp.zeros((BASIS, 128 - BASIS), jnp.float32)], axis=1)
    jump_rows = jnp.concatenate(to_rows(lambda i: grid[8 * i:8 * i + 8, :], 8), axis=1)
    for slot in range(4):
        jump_ref[slot, 0] = jump_rows[slot:slot + 1, 0:729]
    finish_sums()
    sums = fix_in[0]
    for at in range(1, 8):
        sums = sums + fix_in[at]
    sums = [sums[4 * h:4 * h + 4, 128 * n:128 * n + 128] for h in range(2) for n in range(3)]
    to_matrices(sums, grid)
    lane = lanes_of(BASIS)
    inside = lane < BASIS
    near = jnp.where(inside, grid[pl.ds(2, BASIS, stride=8), :], 0.0)
    far = jnp.where(inside, grid[pl.ds(3, BASIS, stride=8), :], 0.0)
    far = pltpu.roll(far, 62, 1)
    ends = jnp.concatenate(sums, axis=1)
    sums_home[0][1]()
    sums_home[1][1]()
    x_ref[...] = jnp.zeros((BASIS, BASIS * BASIS), jnp.float32)
    for q in range(SUBS):
        layers_q = jnp.concatenate([slab_layers(home, half, q) for half in range(2)], axis=1)
        x_ref[6 * q:6 * q + LAYERS, :] += layers_q[0:LAYERS, 0:729]
    for s in range(2):
        x_ref[26 * s:26 * s + 1, :] += ends[s:s + 1, 0:729]
    x_ref[:, 0:128] += near
    x_ref[:, 640:729] += far[:, 0:89]
    out_ref[0, 0, :, 0, :] = x_ref[...]


def store_kernel(result, jumps, result_hbm, jumps_hbm, sems):
    copies = [pltpu.make_async_copy(result, result_hbm, sems.at[0]), pltpu.make_async_copy(jumps, jumps_hbm, sems.at[1])]
    for copy in copies:
        copy.start()
    for copy in copies:
        copy.wait()


def per_device(state, stiff_weight, volume_weight, lagrange, mortar, links):
    vmem = pl.BlockSpec(memory_space=pltpu.VMEM)
    anywhere = pl.BlockSpec(memory_space=pl.ANY)
    constants = constant_tables()
    local = [x.shape[1:] if n < 2 else x.shape for n, x in enumerate(constants)]
    result, jumps = pl.pallas_call(
        operator_kernel,
        name="operator",
        out_shape=(jax.ShapeDtypeStruct((1, 1, BASIS, 1, BASIS * BASIS), jnp.float32),
                   jax.ShapeDtypeStruct(lagrange.shape, jnp.float32)),
        in_specs=[anywhere] * 13,
        out_specs=(vmem, vmem),
        scratch_shapes=[
            pltpu.VMEM((BASIS, BASIS * BASIS), jnp.float32),
            pltpu.VMEM(lagrange.shape, jnp.float32),
            pltpu.VMEM(mortar.shape, jnp.float32),
            pltpu.VMEM((6, 256), jnp.int32),
            pltpu.SMEM((6, 256), jnp.int32),
            *[pltpu.VMEM(shape, jnp.bfloat16) for shape in local[:-1]],
            pltpu.SMEM(local[-1], jnp.float32),
            pltpu.VMEM((SLAB, QUAD * QUAD), jnp.float32),
            pltpu.VMEM((SLAB, QUAD * QUAD), jnp.float32),
            pltpu.VMEM((2, SUBS, 8, 512), jnp.float32),
            pltpu.VMEM((2, SUBS, 8, 512), jnp.float32),
            pltpu.VMEM((2, SUBS, 8, 512), jnp.float32),
            pltpu.VMEM((2, SUBS, 8, 512), jnp.float32),
            pltpu.VMEM((BASIS, 2 * SLAB, 128), jnp.float32),
            pltpu.VMEM((BASIS, 2 * SLAB, 128), jnp.float32),
            pltpu.VMEM((2, 128, 128), jnp.bfloat16),
            pltpu.VMEM((BASIS * 8, 128), jnp.float32),
            pltpu.VMEM((8, 384), jnp.float32),
            pltpu.VMEM((8, 8, 384), jnp.float32),
            pltpu.VMEM((8, 16, 384), jnp.float32),
            pltpu.VMEM((8, 16, 384), jnp.float32),
            pltpu.VMEM((16, 384), jnp.float32),
            pltpu.VMEM((8, 16, 384), jnp.float32),
            pltpu.VMEM((8, 8, 384), jnp.float32),
            pltpu.VMEM((8, 8, 384), jnp.float32),
            pltpu.SemaphoreType.DMA((11,)),
            pltpu.SemaphoreType.DMA((2, SUBS)),
            pltpu.SemaphoreType.DMA((2, SUBS)),
            pltpu.SemaphoreType.DMA((2, SUBS)),
            pltpu.SemaphoreType.DMA((2, SUBS)),
            pltpu.SemaphoreType.DMA((4, 8)),
            pltpu.SemaphoreType.DMA((4, 8)),
        ],
        compiler_params=pltpu.CompilerParams(collective_id=0, has_side_effects=True, vmem_limit_bytes=54 * 10**6),
        cost_estimate=pl.CostEstimate(flops=10**10, bytes_accessed=4 * 10**6, transcendentals=0),
    )(*[pltpu.with_memory_space_constraint(x, pltpu.HBM) for x in (
        jnp.transpose(state, (0, 1, 3, 2, 4)), stiff_weight, volume_weight, lagrange,
        jnp.transpose(mortar, (0, 1, 3, 2, 4)), links.T, *constants)])
    result, jumps = pl.pallas_call(
        store_kernel,
        name="store",
        out_shape=(jax.ShapeDtypeStruct(result.shape, jnp.float32), jax.ShapeDtypeStruct(jumps.shape, jnp.float32)),
        in_specs=[vmem, vmem],
        out_specs=(anywhere, anywhere),
        scratch_shapes=[pltpu.SemaphoreType.DMA((2,))],
        compiler_params=pltpu.CompilerParams(vmem_limit_bytes=2 * 10**6),
    )(result, jumps)
    return jnp.transpose(result, (0, 1, 3, 2, 4)), jumps


def solution(mesh):
    return jax.shard_map(
        per_device,
        mesh=mesh,
        in_specs=(
            P("patch", "sub", None, None, None),
            P("patch", None, None),
            P("patch", None, None),
            P("patch", "sub", None, None),
            P("patch", None, None, None, None),
            P(),
        ),
        out_specs=(P("patch", "sub", None, None, None), P("patch", "sub", None, None)),
        check_vma=False,
    )
```

```python
import jax
import jax.numpy as jnp
import numpy as np
from jax import lax
from jax.experimental import pallas as pl
from jax.experimental.pallas import tpu as pltpu
from jax.sharding import PartitionSpec as P

ELEMS = 24
DEGREE = 3
FIELDS = 4
BASIS = 27
QUAD = 96
SUBS = 4
SLAB = QUAD // SUBS
LAYERS = SLAB // 4 + DEGREE
STEPS = 12
MESH = pl.DeviceIdType.MESH

stabilize = 0.25
highest = lax.Precision.HIGHEST
gauss_points_four = [
    -0.8611363115940526,
    -0.3399810435848563,
    0.3399810435848563,
    0.8611363115940526,
]
gauss_weights_four = [
    0.3478548451374538,
    0.6521451548625461,
    0.6521451548625461,
    0.3478548451374538,
]


def spline_tables(elements, degree):
    knot_list = np.concatenate(
        [np.zeros(degree), np.arange(elements + 1.0), np.full(degree, float(elements))]
    )
    gauss_nodes = np.array(gauss_points_four)
    gauss_weights = np.array(gauss_weights_four)
    points = (np.arange(elements)[:, None] + (gauss_nodes[None, :] + 1.0) / 2.0).reshape(-1)
    point_weights = np.tile(gauss_weights / 2.0, elements)
    current = np.where(
        (knot_list[None, :-1] <= points[:, None]) & (points[:, None] < knot_list[None, 1:]),
        1.0,
        0.0,
    )
    previous = current
    for order_k in range(1, degree + 1):
        previous = current
        amount = len(knot_list) - 1 - order_k
        current = np.zeros((points.shape[0], amount))
        for column in range(amount):
            left_span = knot_list[column + order_k] - knot_list[column]
            right_span = knot_list[column + order_k + 1] - knot_list[column + 1]
            if left_span > 0:
                current[:, column] += (points - knot_list[column]) / left_span * previous[:, column]
            if right_span > 0:
                current[:, column] += (
                    (knot_list[column + order_k + 1] - points)
                    / right_span
                    * previous[:, column + 1]
                )
    slope_part = np.zeros(current.shape)
    for column in range(current.shape[1]):
        left_span = knot_list[column + degree] - knot_list[column]
        right_span = knot_list[column + degree + 1] - knot_list[column + 1]
        if left_span > 0:
            slope_part[:, column] += degree / left_span * previous[:, column]
        if right_span > 0:
            slope_part[:, column] -= degree / right_span * previous[:, column + 1]
    return (
        current.astype(np.float32),
        slope_part.astype(np.float32),
        (current * point_weights[:, None]).astype(np.float32),
        (slope_part * point_weights[:, None]).astype(np.float32),
    )


def halves(table):
    high = table.astype(jnp.bfloat16).astype(np.float32)
    low = (table - high).astype(jnp.bfloat16).astype(np.float32)
    return high, low


def constant_tables():
    value, slope, value_w, slope_w = spline_tables(ELEMS, DEGREE)
    first = np.zeros((SUBS, 2 * SLAB, 16), np.float32)
    last = np.zeros((SUBS, 16, 2 * SLAB), np.float32)
    for q in range(SUBS):
        rows = slice(SLAB * q, SLAB * (q + 1))
        cols = slice(6 * q, 6 * q + LAYERS)
        first[q, :SLAB, :LAYERS] = value[rows, cols]
        first[q, SLAB:, :LAYERS] = slope[rows, cols]
        last[q, :LAYERS, :SLAB] = slope_w[rows, cols].T
        last[q, :LAYERS, SLAB:] = value_w[rows, cols].T
    high, low = halves(first)
    first = np.concatenate([high, high, low], axis=2)
    high, low = halves(last)
    last = np.concatenate([high, high, low], axis=2)

    def pair_tables(table):
        high, low = halves(table)
        even = np.zeros((256, 256), np.float32)
        odd = np.zeros((256, 256), np.float32)
        for s in range(2):
            cols = slice(128 * s, 128 * s + QUAD)
            even[32 * s:32 * s + BASIS, cols] = high.T
            even[128 + 32 * s:128 + 32 * s + BASIS, cols] = high.T
            even[192 + 32 * s:192 + 32 * s + BASIS, cols] = low.T
            odd[64 + 32 * s:64 + 32 * s + BASIS, cols] = high.T
            odd[128 + 32 * s:128 + 32 * s + BASIS, cols] = low.T
            odd[192 + 32 * s:192 + 32 * s + BASIS, cols] = high.T
        return even, odd

    value_even, value_odd = pair_tables(value)
    slope_even, slope_odd = pair_tables(slope)
    inner = np.stack([value_even, value_odd, slope_even, slope_odd])
    plain = value_odd[:, 128:]

    def adjoint_table(table, spilled=None):
        high, low = halves(table)
        out = np.zeros((1024, 256), np.float32)
        for f in range(FIELDS):
            scale = -stabilize if f == FIELDS - 1 else 1.0
            rows = slice(128 * f, 128 * f + QUAD)
            out[rows, 32 * f:32 * f + BASIS] = scale * high
            out[rows, 128 + 32 * f:128 + 32 * f + BASIS] = scale * low
            out[512 + 128 * f:512 + 128 * f + QUAD, 32 * f:32 * f + BASIS] = scale * high
        if spilled is None:
            return out
        high, low = halves(spilled)
        more = np.zeros((256, 256), np.float32)
        more[:QUAD, 96:96 + BASIS] = -high
        more[:QUAD, 224:224 + BASIS] = -low
        more[128:128 + QUAD, 96:96 + BASIS] = -high
        return np.concatenate([out, more])

    adjoint_value = adjoint_table(value_w)
    adjoint_slope = adjoint_table(slope_w, value_w)
    middle = np.zeros((STEPS, 128), np.float32)
    for t in range(STEPS):
        for bb in range(8):
            point = 8 * t + bb
            for m in range(4):
                col = 2 * t + bb // 4 + m
                for n, table in enumerate((value, slope, value_w, slope_w)):
                    middle[t, 32 * n + 4 * bb + m] = table[point, col]
    half = lambda x: jnp.asarray(x, jnp.bfloat16)
    return (half(first), half(last), half(inner), half(plain), half(adjoint_value), half(adjoint_slope),
            jnp.asarray(middle, jnp.float32))


def split(x):
    high = x.astype(jnp.bfloat16)
    return high, (x - high.astype(jnp.float32)).astype(jnp.bfloat16)


def product(left, right):
    return jnp.dot(left, right, preferred_element_type=jnp.float32)


def lanes_of(rows):
    return lax.broadcasted_iota(jnp.int32, (rows, 128), 1)


def exact(left, right, dims):
    return lax.dot_general(left, right, (dims, ((), ())), precision=highest, preferred_element_type=jnp.float32)


def to_matrices(tiles, grid):
    for i in range(BASIS):
        tile, shift = divmod(BASIS * i, 128)
        piece = tiles[tile]
        if shift + BASIS > 128:
            piece = jnp.where(lanes_of(piece.shape[0]) >= shift, piece, tiles[tile + 1])
        grid[8 * i:8 * i + piece.shape[0], :] = pltpu.roll(piece, 128 - shift, 1) if shift else piece


def to_rows(row_of, count):
    lane = lanes_of(count)
    tiles = [jnp.zeros((count, 128), jnp.float32) for _ in range(6)]
    for i in range(BASIS):
        tile, shift = divmod(BASIS * i, 128)
        piece = row_of(i)
        piece = pltpu.roll(piece, shift, 1) if shift else piece
        end = shift + BASIS
        tiles[tile] = jnp.where((lane >= shift) & (lane < end), piece, tiles[tile])
        if end > 128:
            tiles[tile + 1] = jnp.where(lane < end - 128, piece, tiles[tile + 1])
    return tiles


def slab_layers(ref, half, at):
    first = lax.broadcasted_iota(jnp.int32, (8, 384), 0) == 0
    line = jnp.concatenate([ref[half, at, n:n + 1, 384:512] for n in range(3)], axis=1)
    return jnp.concatenate([ref[half, at, :, 0:384], jnp.where(first, line, 0.0)], axis=0)


def routing(links_ref, y, z, core):
    row = lax.broadcasted_iota(jnp.int32, (128, 256), 0)
    col = lax.broadcasted_iota(jnp.int32, (128, 256), 1)
    source = ((row // 32) * 16 + 2 * z + (row // 16) % 2) * 4 + row % 4
    order = jnp.where(col == source, 1.0, 0.0).astype(jnp.bfloat16)
    table = links_ref[...].astype(jnp.float32).astype(jnp.bfloat16)
    found = lax.dot_general(order, table, (((1,), (1,)), ((), ())), preferred_element_type=jnp.float32)
    row = lax.broadcasted_iota(jnp.int32, (128, 1), 0)
    second = (row // 4) % 2 == 1
    patch = jnp.where(second, found[:, 1:2], found[:, 0:1])
    face = jnp.where(second, found[:, 3:4], found[:, 2:3])
    patch = jnp.where(found[:, 4:5] > 0.0, patch, -1.0)
    lane = lanes_of(128)
    row = lax.broadcasted_iota(jnp.int32, (128, 128), 0)
    wanted = (16 * y + 2 * (lane // 8) + core).astype(jnp.float32)
    same = (patch == wanted) & (face == (lane % 4).astype(jnp.float32))
    same = same & ((lane // 4) % 2 == (row // 8) % 2) & (lane < 64)
    return jnp.where(same, 1.0, 0.0)


def operator_kernel(x_hbm, stiff_hbm, volume_hbm, lagrange_hbm, mortar_hbm, links_hbm, first_hbm, last_hbm,
                    inner_hbm, plain_hbm, adj_value_hbm, adj_slope_hbm, middle_hbm, out_ref, jump_ref,
                    x_ref, lagrange_ref, mortar_ref, links_ref, counts_ref, first_ref, last_ref, inner_ref,
                    plain_ref, adj_value_ref, adj_slope_ref, middle_ref, stiff, volume, sent, got, back, home, outer, total, grid, trace_own, trace_all,
                    trace_out, trace_in, fix_own, fix_all, fix_out, fix_in, load_sem, send_sem, recv_sem,
                    back_send_sem, back_recv_sem, face_send_sem, face_recv_sem):
    load_x = pltpu.make_async_copy(x_hbm.at[0, 0, :, 0, :], x_ref, load_sem.at[0])
    load_x.start()
    me = lax.axis_index("sub")
    patch = lax.axis_index("patch")
    y, z, core = patch // 16, (patch // 2) % 8, patch % 2
    group = 2 * y + core
    line = [lax.rem(z + d, 8) for d in range(8)]
    line_from = [lax.rem(z + 8 - d, 8) for d in range(8)]
    plane = [lax.rem(group + d, 8) for d in range(8)]
    plane_from = [lax.rem(group + 8 - d, 8) for d in range(8)]
    line_ids = [{"patch": 16 * y + 2 * at + core} for at in line]
    plane_ids = [{"patch": 16 * (at // 2) + 2 * z + at % 2} for at in plane]

    def exchange(n, source, target, slot, slots_from, ids):
        def one(d, at):
            return pltpu.make_async_remote_copy(
                src_ref=source(d), dst_ref=target.at[at], send_sem=face_send_sem.at[n, d],
                recv_sem=face_recv_sem.at[n, d], device_id=ids[d], device_id_type=MESH)

        def start():
            for d in (4, 3, 5, 2, 6, 1, 7):
                one(d, slot).start()

        def finish():
            for d in range(1, 8):
                one(d, slot).wait_send()
                one(d, slots_from[d]).wait_recv()

        return start, finish

    peers = [lax.rem(me + d, SUBS) for d in range(SUBS)]
    origins = [lax.rem(me + SUBS - d, SUBS) for d in range(SUBS)]
    barrier = pltpu.get_barrier_semaphore()
    for d in range(1, SUBS):
        pl.semaphore_signal(barrier, inc=1, device_id={"sub": peers[d]}, device_id_type=MESH)
    for d in range(1, 8):
        for ids in (line_ids, plane_ids):
            pl.semaphore_signal(barrier, inc=1, device_id=ids[d], device_id_type=MESH)
    rows = pl.ds(pl.multiple_of(me * SLAB, 8), SLAB)
    pairs = [(slot, s, n) for slot in range(4) for s in range(2) for n in range(2)]
    loads = [
        [(links_hbm, links_ref)],
        [(links_hbm, counts_ref)],
        [(lagrange_hbm, lagrange_ref)],
        [(mortar_hbm.at[slot, s, :, n, :], mortar_ref.at[slot, s, n]) for slot, s, n in pairs],
        [(first_hbm.at[me], first_ref)],
        [(middle_hbm, middle_ref)],
        [(inner_hbm, inner_ref), (plain_hbm, plain_ref)],
        [(stiff_hbm.at[0, rows], stiff), (volume_hbm.at[0, rows], volume)],
        [(adj_value_hbm, adj_value_ref), (adj_slope_hbm, adj_slope_ref)],
        [(last_hbm.at[me], last_ref)],
    ]
    loads = [[pltpu.make_async_copy(a, b, load_sem.at[1 + n]) for a, b in some] for n, some in enumerate(loads)]
    for some in loads:
        for copy in some:
            copy.start()

    def loaded(*which):
        for n in which:
            for copy in loads[n]:
                copy.wait()

    load_x.wait()
    sent[...] = jnp.zeros_like(sent)
    for half in range(2):
        for q in range(SUBS):
            width = min(384, 729 - 384 * half)
            sent[half, q, :, 0:width] = x_ref[6 * q:6 * q + 8, 384 * half:384 * half + width]
            for n in range(3):
                lane = 384 * half + 128 * n
                width = min(128, 729 - lane)
                sent[half, q, n:n + 1, 384:384 + width] = x_ref[6 * q + 8:6 * q + 9, lane:lane + width]
    trace_rows = [[x_ref[26 * s:26 * s + 1, 128 * n:min(128 * n + 128, 729)] for n in range(6)] for s in range(2)]
    for s in range(2):
        tail = jnp.zeros((1, 768 - 729), jnp.float32)
        trace_rows[s][5] = jnp.concatenate([trace_rows[s][5], tail], axis=1)
    edge = x_ref[:, 0:128]
    trace_rows.append(to_rows(lambda i: edge[i:i + 1, :], 1))
    edge = jnp.concatenate([x_ref[:, 640:729], jnp.zeros((BASIS, 39), jnp.float32)], axis=1)
    edge = pltpu.roll(edge, 128 - 62, 1)
    trace_rows.append(to_rows(lambda i: edge[i:i + 1, :], 1))
    for h in range(2):
        for f in range(4):
            for n in range(3):
                trace_own[4 * h + f:4 * h + f + 1, 128 * n:128 * n + 128] = trace_rows[f][3 * h + n]
    start_traces, finish_traces = exchange(0, lambda d: trace_own, trace_all, z, line_from, line_ids)
    start_picked, finish_picked = exchange(1, lambda d: trace_out.at[plane[d]], trace_in, group, plane_from, plane_ids)
    start_fixes, finish_fixes = exchange(2, lambda d: fix_own, fix_all, group, plane_from, plane_ids)
    start_sums, finish_sums = exchange(3, lambda d: fix_out.at[line[d]], fix_in, z, line_from, line_ids)
    pl.semaphore_wait(barrier, SUBS - 1 + 14)
    def sub_exchange(half, source, target, send, recv):
        def one(d, at):
            return pltpu.make_async_remote_copy(
                src_ref=source.at[half, peers[d]], dst_ref=target.at[half, at], send_sem=send.at[half, d],
                recv_sem=recv.at[half, d], device_id={"sub": peers[d]}, device_id_type=MESH)

        def start():
            for d in (2, 1, 3):
                one(d, me).start()
            target[half, me] = source[half, me]

        def finish():
            for d in range(1, SUBS):
                one(d, me).wait_send()
                one(d, origins[d]).wait_recv()

        return start, finish

    layers = [sub_exchange(half, sent, got, send_sem, recv_sem) for half in range(2)]
    sums_home = [sub_exchange(half, back, home, back_send_sem, back_recv_sem) for half in range(2)]
    layers[0][0]()
    layers[1][0]()
    start_traces()
    trace_all[z] = trace_own[...]
    loaded(0, 1, 2, 3)
    row = lax.broadcasted_iota(jnp.int32, (BASIS, BASIS), 0)
    lefts, rights = [], []
    for s in range(2):
        for slot in range(4):
            at = 4 * patch + slot
            lefts.append(jnp.where(row < counts_ref[4, at], mortar_ref[slot, s, 0], 0.0))
            rights.append(jnp.where(row < counts_ref[5, at], mortar_ref[slot, s, 1], 0.0))
    multipliers = jnp.concatenate([lagrange_ref[slot, 0] for slot in range(4)], axis=0)
    multipliers = jnp.concatenate([multipliers, jnp.zeros((4, 768 - 729), jnp.float32)], axis=1)
    to_matrices([multipliers[:, 128 * n:128 * n + 128] for n in range(6)], grid)
    given = [grid[pl.ds(slot, BASIS, stride=8), :][:, 0:BASIS] for slot in range(4)]
    for k in range(8):
        fix = exact(given[k % 4], rights[k], ((1,), (0,)))
        fix = exact(lefts[k], fix, ((0,), (0,)))
        fix = fix if k < 4 else -fix
        grid[pl.ds(k, BASIS, stride=8), :] = jnp.concatenate(
            [fix, jnp.zeros((BASIS, 128 - BASIS), jnp.float32)], axis=1)
    fix_rows = to_rows(lambda i: grid[8 * i:8 * i + 8, :], 8)
    for h in range(2):
        for n in range(3):
            fix_own[8 * h:8 * h + 8, 128 * n:128 * n + 128] = fix_rows[3 * h + n]
    start_fixes()
    fix_all[group] = fix_own[...]
    route = routing(links_ref, y, z, core)
    total[...] = jnp.zeros_like(total)
    layers[0][1]()
    loaded(4)
    first = first_ref[...]

    def first_stage(begin, end):
        slabs = [jnp.concatenate([slab_layers(got, half, f) for half in range(1 + (end > 14))], axis=1)
                 for f in range(FIELDS)]
        lane = lanes_of(16)
        columns = []
        for j in range(begin, end):
            tile, shift = divmod(BASIS * j, 128)
            merged = None
            for f in range(FIELDS):
                piece = slabs[f][:, 128 * tile:128 * tile + 128]
                if shift + BASIS > 128:
                    piece = jnp.where(lane >= shift, piece, slabs[f][:, 128 * tile + 128:128 * tile + 256])
                turn = (32 * f - shift) % 128
                piece = pltpu.roll(piece, turn, 1) if turn else piece
                merged = piece if f == 0 else jnp.where(lane >= 32 * f, piece, merged)
            high, low = split(merged)
            columns.append(jnp.concatenate([high, low, high], axis=0))
        for j in range(begin, end, 2):
            result = product(first, jnp.concatenate(columns[j - begin:j - begin + 2], axis=1))
            for n in range(min(2, end - j)):
                outer[j + n] = result[:, 128 * n:128 * n + 128]

    first_stage(0, 14)
    loaded(5, 6, 7, 8, 9)

    def step(t, carry):
        def scalar(table, bb, m):
            return middle_ref[t, 32 * table + 4 * bb + m]

        window = [outer[2 * t + m] for m in range(5)]
        values = [w[0:SLAB] for w in window]
        slopes = [w[SLAB:2 * SLAB] for w in window]

        def middle_sum(table, parts, bb):
            e = bb // 4
            out = scalar(table, bb, 0) * parts[e]
            for m in range(1, 4):
                out = out + scalar(table, bb, m) * parts[e + m]
            return out

        def pair_sides(x):
            lane = lanes_of(x.shape[0])
            high = x.astype(jnp.bfloat16)
            wide = high.astype(jnp.float32)
            low = x - wide
            turned = pltpu.roll(wide, 64, 1)
            even = jnp.where(lane < 64, low, turned).astype(jnp.bfloat16)
            odd = jnp.where(lane < 64, turned, low).astype(jnp.bfloat16)
            return jnp.concatenate([high, even], axis=1), jnp.concatenate([high, odd], axis=1)

        def weights(ref):
            lane = lanes_of(SLAB)
            tiles = [ref[:, pl.ds(pl.multiple_of(768 * t + 128 * n, 128), 128)] for n in range(6)]
            parts = []
            for bb in range(8):
                tile, shift = divmod(QUAD * bb, 128)
                part = tiles[tile]
                if shift + QUAD > 128:
                    part = jnp.where(lane >= shift, part, tiles[tile + 1])
                parts.append(pltpu.roll(part, 128 - shift, 1) if shift else part)
            return jnp.concatenate(parts, axis=0)

        s = weights(stiff)
        w = weights(volume)
        def adjoint(parts, table):
            pairs = [split(p) for p in parts]
            sides = [p[0] for p in pairs[:FIELDS]] + [p[1] for p in pairs[:FIELDS]]
            for pair in pairs[FIELDS:]:
                sides.extend(pair)
            wide = product(jnp.concatenate(sides, axis=1), table[...])
            return wide[:, 0:128] + wide[:, 128:256]

        def gradient(table, parts, at):
            even, odd = pair_sides(jnp.concatenate([middle_sum(table, parts, bb) for bb in range(8)], axis=0))
            first, second = product(even, inner_ref[at]), product(odd, inner_ref[at + 1])
            return [first[:, 0:128], first[:, 128:256], second[:, 0:128], second[:, 128:256]], odd

        along, odd = gradient(0, values, 2)
        pressed = w * product(odd, plain_ref[...])
        spill = along[2]
        heads = [None] * 3
        for d in range(2):
            grads, _ = gradient(d, values if d else slopes, 0)
            spill = spill + grads[d]
            heads[d] = adjoint([s * g - pressed if f == d else s * g for f, g in enumerate(grads)], adj_value_ref)
        heads[2] = adjoint([s * g - pressed if f == 2 else s * g for f, g in enumerate(along)] + [w * spill],
                           adj_slope_ref)
        heads = [[h[SLAB * bb:SLAB * bb + SLAB] for bb in range(8)] for h in heads]
        sums = [[None, None] for _ in range(5)]
        for bb in range(8):
            for m in range(4):
                at = bb // 4 + m
                v = scalar(2, bb, m)
                terms = [v * heads[0][bb], scalar(3, bb, m) * heads[1][bb] + v * heads[2][bb]]
                sums[at] = [a if b is None else b + a for a, b in zip(terms, sums[at])]
        for m in range(5):
            total[2 * t + m] += jnp.concatenate(sums[m], axis=0)
        return carry

    last = last_ref[...]

    def last_stage(half):
        lane = lanes_of(16)
        packed = [[jnp.zeros((16, 128), jnp.float32) for _ in range(3)] for _ in range(FIELDS)]
        begin, end = (0, 15) if half == 0 else (14, BASIS)
        for j0 in range(begin, end, 2):
            some = list(range(j0, min(j0 + 2, end)))
            columns = []
            for j in some:
                high, low = split(total[j])
                columns.append(jnp.concatenate([high, low, high], axis=0))
            result = product(last, jnp.concatenate(columns, axis=1))
            for n, j in enumerate(some):
                piece = result[:, 128 * n:128 * n + 128]
                tile, shift = divmod(BASIS * j, 128)
                stop = shift + BASIS
                at = tile - 3 * half
                for f in range(FIELDS):
                    turn = (shift - 32 * f) % 128
                    turned = pltpu.roll(piece, turn, 1) if turn else piece
                    if 0 <= at < 3:
                        packed[f][at] = jnp.where((lane >= shift) & (lane < stop), turned, packed[f][at])
                    if stop > 128 and 0 <= at + 1 < 3:
                        packed[f][at + 1] = jnp.where(lane < stop - 128, turned, packed[f][at + 1])
        for f in range(FIELDS):
            for n in range(3):
                back[half, f, :, 128 * n:128 * n + 128] = packed[f][n][0:8]
                back[half, f, n:n + 1, 384:512] = packed[f][n][8:9]
        sums_home[half][0]()

    lax.fori_loop(0, 4, step, 0, unroll=4)
    layers[1][1]()
    first_stage(14, BASIS)
    finish_traces()
    high, low = split(trace_all[...].reshape(64, 384))
    both = (route + pltpu.roll(route, 64, 1)).astype(jnp.bfloat16)
    trace_out[...] = product(both, jnp.concatenate([high, low], axis=0)).reshape(8, 16, 384)
    start_picked()
    trace_in[group] = trace_out[group]
    finish_fixes()
    high, low = split(fix_all[...].reshape(128, 384))
    flipped = route.T.astype(jnp.bfloat16)[0:64]
    fix_out[...] = product(jnp.concatenate([flipped, flipped], axis=1),
                           jnp.concatenate([high, low], axis=0)).reshape(8, 8, 384)
    start_sums()
    fix_in[z] = fix_out[z]
    lax.fori_loop(4, 8, step, 0, unroll=4)
    last_stage(0)
    lax.fori_loop(8, STEPS, step, 0, unroll=4)
    last_stage(1)
    finish_picked()
    picked = trace_in[0]
    for at in range(1, 8):
        picked = picked + trace_in[at]
    to_matrices([picked[8 * h:8 * h + 8, 128 * n:128 * n + 128] for h in range(2) for n in range(3)], grid)
    jumps = []
    for k in range(8):
        jump = exact(grid[pl.ds(k, BASIS, stride=8), :][:, 0:BASIS], rights[k], ((1,), (1,)))
        jumps.append(exact(lefts[k], jump, ((1,), (0,))))
    for slot in range(4):
        grid[pl.ds(slot, BASIS, stride=8), :] = jnp.concatenate(
            [jumps[slot] - jumps[4 + slot], jnp.zeros((BASIS, 128 - BASIS), jnp.float32)], axis=1)
    jump_rows = jnp.concatenate(to_rows(lambda i: grid[8 * i:8 * i + 8, :], 8), axis=1)
    for slot in range(4):
        jump_ref[slot, 0] = jump_rows[slot:slot + 1, 0:729]
    finish_sums()
    sums = fix_in[0]
    for at in range(1, 8):
        sums = sums + fix_in[at]
    sums = [sums[4 * h:4 * h + 4, 128 * n:128 * n + 128] for h in range(2) for n in range(3)]
    to_matrices(sums, grid)
    lane = lanes_of(BASIS)
    inside = lane < BASIS
    near = jnp.where(inside, grid[pl.ds(2, BASIS, stride=8), :], 0.0)
    far = jnp.where(inside, grid[pl.ds(3, BASIS, stride=8), :], 0.0)
    far = pltpu.roll(far, 62, 1)
    ends = jnp.concatenate(sums, axis=1)
    sums_home[0][1]()
    sums_home[1][1]()
    x_ref[...] = jnp.zeros((BASIS, BASIS * BASIS), jnp.float32)
    for q in range(SUBS):
        layers_q = jnp.concatenate([slab_layers(home, half, q) for half in range(2)], axis=1)
        x_ref[6 * q:6 * q + LAYERS, :] += layers_q[0:LAYERS, 0:729]
    for s in range(2):
        x_ref[26 * s:26 * s + 1, :] += ends[s:s + 1, 0:729]
    x_ref[:, 0:128] += near
    x_ref[:, 640:729] += far[:, 0:89]
    out_ref[0, 0, :, 0, :] = x_ref[...]


def store_kernel(result, jumps, result_hbm, jumps_hbm, sems):
    copies = [pltpu.make_async_copy(result, result_hbm, sems.at[0]), pltpu.make_async_copy(jumps, jumps_hbm, sems.at[1])]
    for copy in copies:
        copy.start()
    for copy in copies:
        copy.wait()


def per_device(state, stiff_weight, volume_weight, lagrange, mortar, links):
    vmem = pl.BlockSpec(memory_space=pltpu.VMEM)
    anywhere = pl.BlockSpec(memory_space=pl.ANY)
    constants = constant_tables()
    local = [x.shape[1:] if n < 2 else x.shape for n, x in enumerate(constants)]
    result, jumps = pl.pallas_call(
        operator_kernel,
        name="operator",
        out_shape=(jax.ShapeDtypeStruct((1, 1, BASIS, 1, BASIS * BASIS), jnp.float32),
                   jax.ShapeDtypeStruct(lagrange.shape, jnp.float32)),
        in_specs=[anywhere] * 13,
        out_specs=(vmem, vmem),
        scratch_shapes=[
            pltpu.VMEM((BASIS, BASIS * BASIS), jnp.float32),
            pltpu.VMEM(lagrange.shape, jnp.float32),
            pltpu.VMEM(mortar.shape, jnp.float32),
            pltpu.VMEM((6, 256), jnp.int32),
            pltpu.SMEM((6, 256), jnp.int32),
            *[pltpu.VMEM(shape, jnp.bfloat16) for shape in local[:-1]],
            pltpu.SMEM(local[-1], jnp.float32),
            pltpu.VMEM((SLAB, QUAD * QUAD), jnp.float32),
            pltpu.VMEM((SLAB, QUAD * QUAD), jnp.float32),
            pltpu.VMEM((2, SUBS, 8, 512), jnp.float32),
            pltpu.VMEM((2, SUBS, 8, 512), jnp.float32),
            pltpu.VMEM((2, SUBS, 8, 512), jnp.float32),
            pltpu.VMEM((2, SUBS, 8, 512), jnp.float32),
            pltpu.VMEM((BASIS, 2 * SLAB, 128), jnp.float32),
            pltpu.VMEM((BASIS, 2 * SLAB, 128), jnp.float32),
            pltpu.VMEM((BASIS * 8, 128), jnp.float32),
            pltpu.VMEM((8, 384), jnp.float32),
            pltpu.VMEM((8, 8, 384), jnp.float32),
            pltpu.VMEM((8, 16, 384), jnp.float32),
            pltpu.VMEM((8, 16, 384), jnp.float32),
            pltpu.VMEM((16, 384), jnp.float32),
            pltpu.VMEM((8, 16, 384), jnp.float32),
            pltpu.VMEM((8, 8, 384), jnp.float32),
            pltpu.VMEM((8, 8, 384), jnp.float32),
            pltpu.SemaphoreType.DMA((11,)),
            pltpu.SemaphoreType.DMA((2, SUBS)),
            pltpu.SemaphoreType.DMA((2, SUBS)),
            pltpu.SemaphoreType.DMA((2, SUBS)),
            pltpu.SemaphoreType.DMA((2, SUBS)),
            pltpu.SemaphoreType.DMA((4, 8)),
            pltpu.SemaphoreType.DMA((4, 8)),
        ],
        compiler_params=pltpu.CompilerParams(collective_id=0, has_side_effects=True, vmem_limit_bytes=54 * 10**6),
        cost_estimate=pl.CostEstimate(flops=10**10, bytes_accessed=4 * 10**6, transcendentals=0),
    )(*[pltpu.with_memory_space_constraint(x, pltpu.HBM) for x in (
        jnp.transpose(state, (0, 1, 3, 2, 4)), stiff_weight, volume_weight, lagrange,
        jnp.transpose(mortar, (0, 1, 3, 2, 4)), links.T, *constants)])
    result, jumps = pl.pallas_call(
        store_kernel,
        name="store",
        out_shape=(jax.ShapeDtypeStruct(result.shape, jnp.float32), jax.ShapeDtypeStruct(jumps.shape, jnp.float32)),
        in_specs=[vmem, vmem],
        out_specs=(anywhere, anywhere),
        scratch_shapes=[pltpu.SemaphoreType.DMA((2,))],
        compiler_params=pltpu.CompilerParams(vmem_limit_bytes=2 * 10**6),
    )(result, jumps)
    return jnp.transpose(result, (0, 1, 3, 2, 4)), jumps


def solution(mesh):
    return jax.shard_map(
        per_device,
        mesh=mesh,
        in_specs=(
            P("patch", "sub", None, None, None),
            P("patch", None, None),
            P("patch", None, None),
            P("patch", "sub", None, None),
            P("patch", None, None, None, None),
            P(),
        ),
        out_specs=(P("patch", "sub", None, None, None), P("patch", "sub", None, None)),
        check_vma=False,
    )
```

```python
import jax
import jax.numpy as jnp
import numpy as np
from jax import lax
from jax.experimental import pallas as pl
from jax.experimental.pallas import tpu as pltpu
from jax.sharding import PartitionSpec as P

ELEMS = 24
DEGREE = 3
FIELDS = 4
BASIS = 27
QUAD = 96
SUBS = 4
SLAB = QUAD // SUBS
LAYERS = SLAB // 4 + DEGREE
STEPS = 12
MESH = pl.DeviceIdType.MESH

stabilize = 0.25
highest = lax.Precision.HIGHEST
gauss_points_four = [
    -0.8611363115940526,
    -0.3399810435848563,
    0.3399810435848563,
    0.8611363115940526,
]
gauss_weights_four = [
    0.3478548451374538,
    0.6521451548625461,
    0.6521451548625461,
    0.3478548451374538,
]


def spline_tables(elements, degree):
    knot_list = np.concatenate(
        [np.zeros(degree), np.arange(elements + 1.0), np.full(degree, float(elements))]
    )
    gauss_nodes = np.array(gauss_points_four)
    gauss_weights = np.array(gauss_weights_four)
    points = (np.arange(elements)[:, None] + (gauss_nodes[None, :] + 1.0) / 2.0).reshape(-1)
    point_weights = np.tile(gauss_weights / 2.0, elements)
    current = np.where(
        (knot_list[None, :-1] <= points[:, None]) & (points[:, None] < knot_list[None, 1:]),
        1.0,
        0.0,
    )
    previous = current
    for order_k in range(1, degree + 1):
        previous = current
        amount = len(knot_list) - 1 - order_k
        current = np.zeros((points.shape[0], amount))
        for column in range(amount):
            left_span = knot_list[column + order_k] - knot_list[column]
            right_span = knot_list[column + order_k + 1] - knot_list[column + 1]
            if left_span > 0:
                current[:, column] += (points - knot_list[column]) / left_span * previous[:, column]
            if right_span > 0:
                current[:, column] += (
                    (knot_list[column + order_k + 1] - points)
                    / right_span
                    * previous[:, column + 1]
                )
    slope_part = np.zeros(current.shape)
    for column in range(current.shape[1]):
        left_span = knot_list[column + degree] - knot_list[column]
        right_span = knot_list[column + degree + 1] - knot_list[column + 1]
        if left_span > 0:
            slope_part[:, column] += degree / left_span * previous[:, column]
        if right_span > 0:
            slope_part[:, column] -= degree / right_span * previous[:, column + 1]
    return (
        current.astype(np.float32),
        slope_part.astype(np.float32),
        (current * point_weights[:, None]).astype(np.float32),
        (slope_part * point_weights[:, None]).astype(np.float32),
    )


def halves(table):
    high = table.astype(jnp.bfloat16).astype(np.float32)
    low = (table - high).astype(jnp.bfloat16).astype(np.float32)
    return high, low


def constant_tables():
    value, slope, value_w, slope_w = spline_tables(ELEMS, DEGREE)
    first = np.zeros((SUBS, 2 * SLAB, 16), np.float32)
    last = np.zeros((SUBS, 16, 2 * SLAB), np.float32)
    for q in range(SUBS):
        rows = slice(SLAB * q, SLAB * (q + 1))
        cols = slice(6 * q, 6 * q + LAYERS)
        first[q, :SLAB, :LAYERS] = value[rows, cols]
        first[q, SLAB:, :LAYERS] = slope[rows, cols]
        last[q, :LAYERS, :SLAB] = slope_w[rows, cols].T
        last[q, :LAYERS, SLAB:] = value_w[rows, cols].T
    high, low = halves(first)
    first = np.concatenate([high, high, low], axis=2)
    high, low = halves(last)
    last = np.concatenate([high, high, low], axis=2)

    def pair_tables(table):
        high, low = halves(table)
        even = np.zeros((256, 256), np.float32)
        odd = np.zeros((256, 256), np.float32)
        for s in range(2):
            cols = slice(128 * s, 128 * s + QUAD)
            even[32 * s:32 * s + BASIS, cols] = high.T
            even[128 + 32 * s:128 + 32 * s + BASIS, cols] = high.T
            even[192 + 32 * s:192 + 32 * s + BASIS, cols] = low.T
            odd[64 + 32 * s:64 + 32 * s + BASIS, cols] = high.T
            odd[128 + 32 * s:128 + 32 * s + BASIS, cols] = low.T
            odd[192 + 32 * s:192 + 32 * s + BASIS, cols] = high.T
        return even, odd

    value_even, value_odd = pair_tables(value)
    slope_even, slope_odd = pair_tables(slope)
    inner = np.stack([value_even, value_odd, slope_even, slope_odd])
    plain = value_odd[:, 128:]

    def adjoint_table(table, spilled=None):
        high, low = halves(table)
        out = np.zeros((1024, 256), np.float32)
        for f in range(FIELDS):
            scale = -stabilize if f == FIELDS - 1 else 1.0
            rows = slice(128 * f, 128 * f + QUAD)
            out[rows, 32 * f:32 * f + BASIS] = scale * high
            out[rows, 128 + 32 * f:128 + 32 * f + BASIS] = scale * low
            out[512 + 128 * f:512 + 128 * f + QUAD, 32 * f:32 * f + BASIS] = scale * high
        if spilled is None:
            return out
        high, low = halves(spilled)
        more = np.zeros((256, 256), np.float32)
        more[:QUAD, 96:96 + BASIS] = -high
        more[:QUAD, 224:224 + BASIS] = -low
        more[128:128 + QUAD, 96:96 + BASIS] = -high
        return np.concatenate([out, more])

    adjoint_value = adjoint_table(value_w)
    adjoint_slope = adjoint_table(slope_w, value_w)
    middle = np.zeros((STEPS, 128), np.float32)
    for t in range(STEPS):
        for bb in range(8):
            point = 8 * t + bb
            for m in range(4):
                col = 2 * t + bb // 4 + m
                for n, table in enumerate((value, slope, value_w, slope_w)):
                    middle[t, 32 * n + 4 * bb + m] = table[point, col]
    half = lambda x: jnp.asarray(x, jnp.bfloat16)
    return (half(first), half(last), half(inner), half(plain), half(adjoint_value), half(adjoint_slope),
            jnp.asarray(middle, jnp.float32))


def split(x):
    high = x.astype(jnp.bfloat16)
    return high, (x - high.astype(jnp.float32)).astype(jnp.bfloat16)


def product(left, right):
    return jnp.dot(left, right, preferred_element_type=jnp.float32)


def lanes_of(rows):
    return lax.broadcasted_iota(jnp.int32, (rows, 128), 1)


def exact(left, right, dims):
    return lax.dot_general(left, right, (dims, ((), ())), precision=highest, preferred_element_type=jnp.float32)


def to_matrices(tiles, grid):
    for i in range(BASIS):
        tile, shift = divmod(BASIS * i, 128)
        piece = tiles[tile]
        if shift + BASIS > 128:
            piece = jnp.where(lanes_of(piece.shape[0]) >= shift, piece, tiles[tile + 1])
        grid[8 * i:8 * i + piece.shape[0], :] = pltpu.roll(piece, 128 - shift, 1) if shift else piece


def to_rows(row_of, count):
    lane = lanes_of(count)
    tiles = [jnp.zeros((count, 128), jnp.float32) for _ in range(6)]
    for i in range(BASIS):
        tile, shift = divmod(BASIS * i, 128)
        piece = row_of(i)
        piece = pltpu.roll(piece, shift, 1) if shift else piece
        end = shift + BASIS
        tiles[tile] = jnp.where((lane >= shift) & (lane < end), piece, tiles[tile])
        if end > 128:
            tiles[tile + 1] = jnp.where(lane < end - 128, piece, tiles[tile + 1])
    return tiles


def slab_layers(ref, half, at):
    first = lax.broadcasted_iota(jnp.int32, (8, 384), 0) == 0
    line = jnp.concatenate([ref[half, at, n:n + 1, 384:512] for n in range(3)], axis=1)
    return jnp.concatenate([ref[half, at, :, 0:384], jnp.where(first, line, 0.0)], axis=0)


def routing(links_ref, y, z, core):
    row = lax.broadcasted_iota(jnp.int32, (128, 256), 0)
    col = lax.broadcasted_iota(jnp.int32, (128, 256), 1)
    source = ((row // 32) * 16 + 2 * z + (row // 16) % 2) * 4 + row % 4
    order = jnp.where(col == source, 1.0, 0.0).astype(jnp.bfloat16)
    table = links_ref[...].astype(jnp.float32).astype(jnp.bfloat16)
    found = lax.dot_general(order, table, (((1,), (1,)), ((), ())), preferred_element_type=jnp.float32)
    row = lax.broadcasted_iota(jnp.int32, (128, 1), 0)
    second = (row // 4) % 2 == 1
    patch = jnp.where(second, found[:, 1:2], found[:, 0:1])
    face = jnp.where(second, found[:, 3:4], found[:, 2:3])
    patch = jnp.where(found[:, 4:5] > 0.0, patch, -1.0)
    lane = lanes_of(128)
    row = lax.broadcasted_iota(jnp.int32, (128, 128), 0)
    wanted = (16 * y + 2 * (lane // 8) + core).astype(jnp.float32)
    same = (patch == wanted) & (face == (lane % 4).astype(jnp.float32))
    same = same & ((lane // 4) % 2 == (row // 8) % 2) & (lane < 64)
    return jnp.where(same, 1.0, 0.0)


def operator_kernel(x_hbm, stiff_hbm, volume_hbm, lagrange_hbm, mortar_hbm, links_hbm, first_hbm, last_hbm,
                    inner_hbm, plain_hbm, adj_value_hbm, adj_slope_hbm, middle_hbm, out_ref, jump_ref,
                    x_ref, lagrange_ref, mortar_ref, links_ref, counts_ref, first_ref, last_ref, inner_ref,
                    plain_ref, adj_value_ref, adj_slope_ref, middle_ref, stiff, volume, sent, got, back, home, outer, total, grid, trace_own, trace_all,
                    trace_out, trace_in, fix_own, fix_all, fix_out, fix_in, load_sem, send_sem, recv_sem,
                    back_send_sem, back_recv_sem, face_send_sem, face_recv_sem):
    load_x = pltpu.make_async_copy(x_hbm.at[0, 0, :, 0, :], x_ref, load_sem.at[0])
    load_x.start()
    me = lax.axis_index("sub")
    patch = lax.axis_index("patch")
    y, z, core = patch // 16, (patch // 2) % 8, patch % 2
    group = 2 * y + core
    line = [lax.rem(z + d, 8) for d in range(8)]
    line_from = [lax.rem(z + 8 - d, 8) for d in range(8)]
    plane = [lax.rem(group + d, 8) for d in range(8)]
    plane_from = [lax.rem(group + 8 - d, 8) for d in range(8)]
    line_ids = [{"patch": 16 * y + 2 * at + core} for at in line]
    plane_ids = [{"patch": 16 * (at // 2) + 2 * z + at % 2} for at in plane]

    def exchange(n, source, target, slot, slots_from, ids):
        def one(d, at):
            return pltpu.make_async_remote_copy(
                src_ref=source(d), dst_ref=target.at[at], send_sem=face_send_sem.at[n, d],
                recv_sem=face_recv_sem.at[n, d], device_id=ids[d], device_id_type=MESH)

        def start():
            for d in (4, 3, 5, 2, 6, 1, 7):
                one(d, slot).start()

        def finish():
            for d in range(1, 8):
                one(d, slot).wait_send()
                one(d, slots_from[d]).wait_recv()

        return start, finish

    peers = [lax.rem(me + d, SUBS) for d in range(SUBS)]
    origins = [lax.rem(me + SUBS - d, SUBS) for d in range(SUBS)]
    barrier = pltpu.get_barrier_semaphore()
    for d in range(1, SUBS):
        pl.semaphore_signal(barrier, inc=1, device_id={"sub": peers[d]}, device_id_type=MESH)
    for d in range(1, 8):
        for ids in (line_ids, plane_ids):
            pl.semaphore_signal(barrier, inc=1, device_id=ids[d], device_id_type=MESH)
    rows = pl.ds(pl.multiple_of(me * SLAB, 8), SLAB)
    pairs = [(slot, s, n) for slot in range(4) for s in range(2) for n in range(2)]
    loads = [
        [(links_hbm, links_ref)],
        [(links_hbm, counts_ref)],
        [(lagrange_hbm, lagrange_ref)],
        [(mortar_hbm.at[slot, s, :, n, :], mortar_ref.at[slot, s, n]) for slot, s, n in pairs],
        [(first_hbm.at[me], first_ref)],
        [(middle_hbm, middle_ref)],
        [(inner_hbm, inner_ref), (plain_hbm, plain_ref)],
        [(stiff_hbm.at[0, rows], stiff), (volume_hbm.at[0, rows], volume)],
        [(adj_value_hbm, adj_value_ref), (adj_slope_hbm, adj_slope_ref)],
        [(last_hbm.at[me], last_ref)],
    ]
    loads = [[pltpu.make_async_copy(a, b, load_sem.at[1 + n]) for a, b in some] for n, some in enumerate(loads)]
    for some in loads:
        for copy in some:
            copy.start()

    def loaded(*which):
        for n in which:
            for copy in loads[n]:
                copy.wait()

    load_x.wait()
    sent[...] = jnp.zeros_like(sent)
    for half in range(2):
        for q in range(SUBS):
            width = min(384, 729 - 384 * half)
            sent[half, q, :, 0:width] = x_ref[6 * q:6 * q + 8, 384 * half:384 * half + width]
            for n in range(3):
                lane = 384 * half + 128 * n
                width = min(128, 729 - lane)
                sent[half, q, n:n + 1, 384:384 + width] = x_ref[6 * q + 8:6 * q + 9, lane:lane + width]
    trace_rows = [[x_ref[26 * s:26 * s + 1, 128 * n:min(128 * n + 128, 729)] for n in range(6)] for s in range(2)]
    for s in range(2):
        tail = jnp.zeros((1, 768 - 729), jnp.float32)
        trace_rows[s][5] = jnp.concatenate([trace_rows[s][5], tail], axis=1)
    edge = x_ref[:, 0:128]
    trace_rows.append(to_rows(lambda i: edge[i:i + 1, :], 1))
    edge = jnp.concatenate([x_ref[:, 640:729], jnp.zeros((BASIS, 39), jnp.float32)], axis=1)
    edge = pltpu.roll(edge, 128 - 62, 1)
    trace_rows.append(to_rows(lambda i: edge[i:i + 1, :], 1))
    for h in range(2):
        for f in range(4):
            for n in range(3):
                trace_own[4 * h + f:4 * h + f + 1, 128 * n:128 * n + 128] = trace_rows[f][3 * h + n]
    start_traces, finish_traces = exchange(0, lambda d: trace_own, trace_all, z, line_from, line_ids)
    start_picked, finish_picked = exchange(1, lambda d: trace_out.at[plane[d]], trace_in, group, plane_from, plane_ids)
    start_fixes, finish_fixes = exchange(2, lambda d: fix_own, fix_all, group, plane_from, plane_ids)
    start_sums, finish_sums = exchange(3, lambda d: fix_out.at[line[d]], fix_in, z, line_from, line_ids)
    pl.semaphore_wait(barrier, SUBS - 1 + 14)
    def sub_exchange(half, source, target, send, recv):
        def one(d, at):
            return pltpu.make_async_remote_copy(
                src_ref=source.at[half, peers[d]], dst_ref=target.at[half, at], send_sem=send.at[half, d],
                recv_sem=recv.at[half, d], device_id={"sub": peers[d]}, device_id_type=MESH)

        def start():
            for d in (2, 1, 3):
                one(d, me).start()
            target[half, me] = source[half, me]

        def finish():
            for d in range(1, SUBS):
                one(d, me).wait_send()
                one(d, origins[d]).wait_recv()

        return start, finish

    layers = [sub_exchange(half, sent, got, send_sem, recv_sem) for half in range(2)]
    sums_home = [sub_exchange(half, back, home, back_send_sem, back_recv_sem) for half in range(2)]
    layers[0][0]()
    layers[1][0]()
    start_traces()
    trace_all[z] = trace_own[...]
    loaded(0, 1, 2, 3)
    row = lax.broadcasted_iota(jnp.int32, (BASIS, BASIS), 0)
    lefts, rights = [], []
    for s in range(2):
        for slot in range(4):
            at = 4 * patch + slot
            lefts.append(jnp.where(row < counts_ref[4, at], mortar_ref[slot, s, 0], 0.0))
            rights.append(jnp.where(row < counts_ref[5, at], mortar_ref[slot, s, 1], 0.0))
    multipliers = jnp.concatenate([lagrange_ref[slot, 0] for slot in range(4)], axis=0)
    multipliers = jnp.concatenate([multipliers, jnp.zeros((4, 768 - 729), jnp.float32)], axis=1)
    to_matrices([multipliers[:, 128 * n:128 * n + 128] for n in range(6)], grid)
    given = [grid[pl.ds(slot, BASIS, stride=8), :][:, 0:BASIS] for slot in range(4)]
    for k in range(8):
        fix = exact(given[k % 4], rights[k], ((1,), (0,)))
        fix = exact(lefts[k], fix, ((0,), (0,)))
        fix = fix if k < 4 else -fix
        grid[pl.ds(k, BASIS, stride=8), :] = jnp.concatenate(
            [fix, jnp.zeros((BASIS, 128 - BASIS), jnp.float32)], axis=1)
    fix_rows = to_rows(lambda i: grid[8 * i:8 * i + 8, :], 8)
    for h in range(2):
        for n in range(3):
            fix_own[8 * h:8 * h + 8, 128 * n:128 * n + 128] = fix_rows[3 * h + n]
    start_fixes()
    fix_all[group] = fix_own[...]
    route = routing(links_ref, y, z, core)
    total[...] = jnp.zeros_like(total)
    layers[0][1]()
    loaded(4)
    first = first_ref[...]

    def first_stage(begin, end):
        slabs = [jnp.concatenate([slab_layers(got, half, f) for half in range(1 + (end > 14))], axis=1)
                 for f in range(FIELDS)]
        lane = lanes_of(16)
        columns = []
        for j in range(begin, end):
            tile, shift = divmod(BASIS * j, 128)
            merged = None
            for f in range(FIELDS):
                piece = slabs[f][:, 128 * tile:128 * tile + 128]
                if shift + BASIS > 128:
                    piece = jnp.where(lane >= shift, piece, slabs[f][:, 128 * tile + 128:128 * tile + 256])
                turn = (32 * f - shift) % 128
                piece = pltpu.roll(piece, turn, 1) if turn else piece
                merged = piece if f == 0 else jnp.where(lane >= 32 * f, piece, merged)
            high, low = split(merged)
            columns.append(jnp.concatenate([high, low, high], axis=0))
        for j in range(begin, end, 2):
            result = product(first, jnp.concatenate(columns[j - begin:j - begin + 2], axis=1))
            for n in range(min(2, end - j)):
                outer[j + n] = result[:, 128 * n:128 * n + 128]

    first_stage(0, 14)
    loaded(5, 6, 7, 8, 9)

    def step(t, carry):
        def scalar(table, bb, m):
            return middle_ref[t, 32 * table + 4 * bb + m]

        window = [outer[2 * t + m] for m in range(5)]
        values = [w[0:SLAB] for w in window]
        slopes = [w[SLAB:2 * SLAB] for w in window]

        def middle_sum(table, parts, bb):
            e = bb // 4
            out = scalar(table, bb, 0) * parts[e]
            for m in range(1, 4):
                out = out + scalar(table, bb, m) * parts[e + m]
            return out

        def pair_sides(x):
            lane = lanes_of(x.shape[0])
            high = x.astype(jnp.bfloat16)
            wide = high.astype(jnp.float32)
            low = x - wide
            turned = pltpu.roll(wide, 64, 1)
            even = jnp.where(lane < 64, low, turned).astype(jnp.bfloat16)
            odd = jnp.where(lane < 64, turned, low).astype(jnp.bfloat16)
            return jnp.concatenate([high, even], axis=1), jnp.concatenate([high, odd], axis=1)

        def weights(ref):
            lane = lanes_of(SLAB)
            tiles = [ref[:, pl.ds(pl.multiple_of(768 * t + 128 * n, 128), 128)] for n in range(6)]
            parts = []
            for bb in range(8):
                tile, shift = divmod(QUAD * bb, 128)
                part = tiles[tile]
                if shift + QUAD > 128:
                    part = jnp.where(lane >= shift, part, tiles[tile + 1])
                parts.append(pltpu.roll(part, 128 - shift, 1) if shift else part)
            return jnp.concatenate(parts, axis=0)

        s = weights(stiff)
        w = weights(volume)
        def adjoint(parts, table):
            pairs = [split(p) for p in parts]
            sides = [p[0] for p in pairs[:FIELDS]] + [p[1] for p in pairs[:FIELDS]]
            for pair in pairs[FIELDS:]:
                sides.extend(pair)
            wide = product(jnp.concatenate(sides, axis=1), table[...])
            return wide[:, 0:128] + wide[:, 128:256]

        def gradient(table, parts, at):
            even, odd = pair_sides(jnp.concatenate([middle_sum(table, parts, bb) for bb in range(8)], axis=0))
            first, second = product(even, inner_ref[at]), product(odd, inner_ref[at + 1])
            return [first[:, 0:128], first[:, 128:256], second[:, 0:128], second[:, 128:256]], odd

        along, odd = gradient(0, values, 2)
        pressed = w * product(odd, plain_ref[...])
        spill = along[2]
        heads = [None] * 3
        for d in range(2):
            grads, _ = gradient(d, values if d else slopes, 0)
            spill = spill + grads[d]
            heads[d] = adjoint([s * g - pressed if f == d else s * g for f, g in enumerate(grads)], adj_value_ref)
        heads[2] = adjoint([s * g - pressed if f == 2 else s * g for f, g in enumerate(along)] + [w * spill],
                           adj_slope_ref)
        heads = [[h[SLAB * bb:SLAB * bb + SLAB] for bb in range(8)] for h in heads]
        sums = [[None, None] for _ in range(5)]
        for bb in range(8):
            for m in range(4):
                at = bb // 4 + m
                v = scalar(2, bb, m)
                terms = [v * heads[0][bb], scalar(3, bb, m) * heads[1][bb] + v * heads[2][bb]]
                sums[at] = [a if b is None else b + a for a, b in zip(terms, sums[at])]
        for m in range(5):
            total[2 * t + m] += jnp.concatenate(sums[m], axis=0)
        return carry

    last = last_ref[...]

    def last_stage(half):
        lane = lanes_of(16)
        packed = [[jnp.zeros((16, 128), jnp.float32) for _ in range(3)] for _ in range(FIELDS)]
        begin, end = (0, 15) if half == 0 else (14, BASIS)
        for j0 in range(begin, end, 2):
            some = list(range(j0, min(j0 + 2, end)))
            columns = []
            for j in some:
                high, low = split(total[j])
                columns.append(jnp.concatenate([high, low, high], axis=0))
            result = product(last, jnp.concatenate(columns, axis=1))
            for n, j in enumerate(some):
                piece = result[:, 128 * n:128 * n + 128]
                tile, shift = divmod(BASIS * j, 128)
                stop = shift + BASIS
                at = tile - 3 * half
                for f in range(FIELDS):
                    turn = (shift - 32 * f) % 128
                    turned = pltpu.roll(piece, turn, 1) if turn else piece
                    if 0 <= at < 3:
                        packed[f][at] = jnp.where((lane >= shift) & (lane < stop), turned, packed[f][at])
                    if stop > 128 and 0 <= at + 1 < 3:
                        packed[f][at + 1] = jnp.where(lane < stop - 128, turned, packed[f][at + 1])
        for f in range(FIELDS):
            for n in range(3):
                back[half, f, :, 128 * n:128 * n + 128] = packed[f][n][0:8]
                back[half, f, n:n + 1, 384:512] = packed[f][n][8:9]
        sums_home[half][0]()

    lax.fori_loop(0, 4, step, 0, unroll=4)
    layers[1][1]()
    first_stage(14, BASIS)
    finish_traces()
    high, low = split(trace_all[...].reshape(64, 384))
    both = (route + pltpu.roll(route, 64, 1)).astype(jnp.bfloat16)
    trace_out[...] = product(both, jnp.concatenate([high, low], axis=0)).reshape(8, 16, 384)
    start_picked()
    trace_in[group] = trace_out[group]
    finish_fixes()
    high, low = split(fix_all[...].reshape(128, 384))
    flipped = route.T.astype(jnp.bfloat16)[0:64]
    fix_out[...] = product(jnp.concatenate([flipped, flipped], axis=1),
                           jnp.concatenate([high, low], axis=0)).reshape(8, 8, 384)
    start_sums()
    fix_in[z] = fix_out[z]
    lax.fori_loop(4, 8, step, 0, unroll=4)
    last_stage(0)
    lax.fori_loop(8, STEPS, step, 0, unroll=4)
    last_stage(1)
    finish_picked()
    picked = trace_in[0]
    for at in range(1, 8):
        picked = picked + trace_in[at]
    to_matrices([picked[8 * h:8 * h + 8, 128 * n:128 * n + 128] for h in range(2) for n in range(3)], grid)
    jumps = []
    for k in range(8):
        jump = exact(grid[pl.ds(k, BASIS, stride=8), :][:, 0:BASIS], rights[k], ((1,), (1,)))
        jumps.append(exact(lefts[k], jump, ((1,), (0,))))
    for slot in range(4):
        grid[pl.ds(slot, BASIS, stride=8), :] = jnp.concatenate(
            [jumps[slot] - jumps[4 + slot], jnp.zeros((BASIS, 128 - BASIS), jnp.float32)], axis=1)
    jump_rows = jnp.concatenate(to_rows(lambda i: grid[8 * i:8 * i + 8, :], 8), axis=1)
    for slot in range(4):
        jump_ref[slot, 0] = jump_rows[slot:slot + 1, 0:729]
    finish_sums()
    sums = fix_in[0]
    for at in range(1, 8):
        sums = sums + fix_in[at]
    sums = [sums[4 * h:4 * h + 4, 128 * n:128 * n + 128] for h in range(2) for n in range(3)]
    to_matrices(sums, grid)
    lane = lanes_of(BASIS)
    inside = lane < BASIS
    near = jnp.where(inside, grid[pl.ds(2, BASIS, stride=8), :], 0.0)
    far = jnp.where(inside, grid[pl.ds(3, BASIS, stride=8), :], 0.0)
    far = pltpu.roll(far, 62, 1)
    ends = jnp.concatenate(sums, axis=1)
    sums_home[0][1]()
    sums_home[1][1]()
    x_ref[...] = jnp.zeros((BASIS, BASIS * BASIS), jnp.float32)
    for q in range(SUBS):
        layers_q = jnp.concatenate([slab_layers(home, half, q) for half in range(2)], axis=1)
        x_ref[6 * q:6 * q + LAYERS, :] += layers_q[0:LAYERS, 0:729]
    for s in range(2):
        x_ref[26 * s:26 * s + 1, :] += ends[s:s + 1, 0:729]
    x_ref[:, 0:128] += near
    x_ref[:, 640:729] += far[:, 0:89]
    out_ref[...] = x_ref[...]


def store_kernel(result, jumps, result_hbm, jumps_hbm, sems):
    copies = [pltpu.make_async_copy(result, result_hbm.at[0, 0, :, 0, :], sems.at[0]), pltpu.make_async_copy(jumps, jumps_hbm, sems.at[1])]
    for copy in copies:
        copy.start()
    for copy in copies:
        copy.wait()


def per_device(state, stiff_weight, volume_weight, lagrange, mortar, links):
    vmem = pl.BlockSpec(memory_space=pltpu.VMEM)
    anywhere = pl.BlockSpec(memory_space=pl.ANY)
    constants = constant_tables()
    local = [x.shape[1:] if n < 2 else x.shape for n, x in enumerate(constants)]
    result, jumps = pl.pallas_call(
        operator_kernel,
        name="operator",
        out_shape=(jax.ShapeDtypeStruct((BASIS, BASIS * BASIS), jnp.float32),
                   jax.ShapeDtypeStruct(lagrange.shape, jnp.float32)),
        in_specs=[anywhere] * 13,
        out_specs=(vmem, vmem),
        scratch_shapes=[
            pltpu.VMEM((BASIS, BASIS * BASIS), jnp.float32),
            pltpu.VMEM(lagrange.shape, jnp.float32),
            pltpu.VMEM(mortar.shape, jnp.float32),
            pltpu.VMEM((6, 256), jnp.int32),
            pltpu.SMEM((6, 256), jnp.int32),
            *[pltpu.VMEM(shape, jnp.bfloat16) for shape in local[:-1]],
            pltpu.SMEM(local[-1], jnp.float32),
            pltpu.VMEM((SLAB, QUAD * QUAD), jnp.float32),
            pltpu.VMEM((SLAB, QUAD * QUAD), jnp.float32),
            pltpu.VMEM((2, SUBS, 8, 512), jnp.float32),
            pltpu.VMEM((2, SUBS, 8, 512), jnp.float32),
            pltpu.VMEM((2, SUBS, 8, 512), jnp.float32),
            pltpu.VMEM((2, SUBS, 8, 512), jnp.float32),
            pltpu.VMEM((BASIS, 2 * SLAB, 128), jnp.float32),
            pltpu.VMEM((BASIS, 2 * SLAB, 128), jnp.float32),
            pltpu.VMEM((256, 128), jnp.float32),
            pltpu.VMEM((8, 384), jnp.float32),
            pltpu.VMEM((8, 8, 384), jnp.float32),
            pltpu.VMEM((8, 16, 384), jnp.float32),
            pltpu.VMEM((8, 16, 384), jnp.float32),
            pltpu.VMEM((16, 384), jnp.float32),
            pltpu.VMEM((8, 16, 384), jnp.float32),
            pltpu.VMEM((8, 8, 384), jnp.float32),
            pltpu.VMEM((8, 8, 384), jnp.float32),
            pltpu.SemaphoreType.DMA((11,)),
            pltpu.SemaphoreType.DMA((2, SUBS)),
            pltpu.SemaphoreType.DMA((2, SUBS)),
            pltpu.SemaphoreType.DMA((2, SUBS)),
            pltpu.SemaphoreType.DMA((2, SUBS)),
            pltpu.SemaphoreType.DMA((4, 8)),
            pltpu.SemaphoreType.DMA((4, 8)),
        ],
        compiler_params=pltpu.CompilerParams(collective_id=0, has_side_effects=True, vmem_limit_bytes=54 * 10**6),
        cost_estimate=pl.CostEstimate(flops=10**10, bytes_accessed=4 * 10**6, transcendentals=0),
    )(*[pltpu.with_memory_space_constraint(x, pltpu.HBM) for x in (
        jnp.transpose(state, (0, 1, 3, 2, 4)), stiff_weight, volume_weight, lagrange,
        jnp.transpose(mortar, (0, 1, 3, 2, 4)), links.T, *constants)])
    result, jumps = pl.pallas_call(
        store_kernel,
        name="store",
        out_shape=(jax.ShapeDtypeStruct((1, 1, BASIS, 1, BASIS * BASIS), jnp.float32), jax.ShapeDtypeStruct(jumps.shape, jnp.float32)),
        in_specs=[vmem, vmem],
        out_specs=(anywhere, anywhere),
        scratch_shapes=[pltpu.SemaphoreType.DMA((2,))],
        compiler_params=pltpu.CompilerParams(vmem_limit_bytes=2 * 10**6),
    )(result, jumps)
    return jnp.transpose(result, (0, 1, 3, 2, 4)), jumps


def solution(mesh):
    return jax.shard_map(
        per_device,
        mesh=mesh,
        in_specs=(
            P("patch", "sub", None, None, None),
            P("patch", None, None),
            P("patch", None, None),
            P("patch", "sub", None, None),
            P("patch", None, None, None, None),
            P(),
        ),
        out_specs=(P("patch", "sub", None, None, None), P("patch", "sub", None, None)),
        check_vma=False,
    )
```
